256 devices in a mesh: groups: 2 (over y), mesh: 16 (over z), edge: 8 (over x, core).
Axes of the slice: x: 4, y: 2, z: 16, core: 2. Of those that a mesh axis runs over, the one named last changes fastest.
The devices are a block of a 4x16x16 slice.
Arguments:
- grid_input: bfloat16 [131072, 474], P(('groups', 'mesh', 'edge')), parts along dimension 0, may hold values from -6 to 6
- mesh_position: bfloat16 [3, 2048], P(None, ('mesh', 'edge')), may hold values from -1 to 1
- encoder_senders: int32 [262144], P(('mesh', 'edge')), may hold values from 0 to 65535, as said below
- encoder_receivers: int32 [262144], P(('mesh', 'edge')), may hold values from 0 to 2047, as said below
- encoder_features: bfloat16 [4, 262144], P(None, ('mesh', 'edge')), may hold values from -6 to 6
- encoder_counts: int32 [128], P(('mesh', 'edge')), may hold values from 1 to 16, as said below
- mesh_senders: int32 [32768], P(('mesh', 'edge')), may hold values from 0 to 2047, as said below
- mesh_receivers: int32 [32768], P(('mesh', 'edge')), may hold values from 0 to 2047, as said below
- mesh_features: bfloat16 [4, 32768], P(None, ('mesh', 'edge')), may hold values from -6 to 6
- cotangent: bfloat16 [4096, 512], P(('groups', 'mesh', 'edge')), parts along dimension 0, may hold values from -6 to 6
- grid_first: bfloat16 [474, 512], replicated, may hold values from -0.25 to 0.25
- grid_second: bfloat16 [512, 512], replicated, may hold values from -0.25 to 0.25
- encoder_inner: bfloat16 [512, 512], replicated, may hold values from -0.25 to 0.25
- encoder_geometry: bfloat16 [4, 512], replicated, may hold values from -3 to 3
- encoder_outer: bfloat16 [512, 512], replicated, may hold values from -0.25 to 0.25
- node_first: bfloat16 [512, 512], replicated, may hold values from -0.25 to 0.25
- node_position: bfloat16 [3, 512], replicated, may hold values from -3.5 to 3.5
- node_second: bfloat16 [512, 512], replicated, may hold values from -0.25 to 0.25
- edge_sender: bfloat16 [512, 512], replicated, may hold values from -0.25 to 0.25
- edge_receiver: bfloat16 [512, 512], replicated, may hold values from -0.25 to 0.25
- edge_geometry: bfloat16 [4, 512], replicated, may hold values from -3 to 3
- edge_outer: bfloat16 [512, 512], replicated, may hold values from -0.25 to 0.25
- update_message: bfloat16 [512, 512], replicated, may hold values from -0.25 to 0.25
- update_state: bfloat16 [512, 512], replicated, may hold values from -0.25 to 0.25
- update_outer: bfloat16 [512, 512], replicated, may hold values from -0.25 to 0.25
Outputs:
- mesh_output: bfloat16 [4096, 512], P(('groups', 'mesh', 'edge')), parts along dimension 0
- mesh_gradient: float32 [4096, 512], P(('groups', 'mesh', 'edge')), parts along dimension 0
The draws below stay inside these ranges and needn't reach their ends.
There are 2 independent parts, one for each index of `groups`. The reference program is written for one: setup_inputs(seed, part) draws one part's arguments, and reference() takes and returns one part's arrays. A program takes and returns all parts, laid end to end along the dimension named above; an argument that names none is the same for every part. Nothing has to cross between parts.
Inputs may be any that keep to these rules, and one draw needn't show every extreme that they name: `encoder_senders`: an encoder edge slot of a device with mesh index b has its sender in band b: from b * 4096 to (b + 1) * 4096 - 1. `encoder_receivers`: an encoder edge slot of a device with mesh index b has its receiver among the mesh nodes b * 128 to (b + 1) * 128 - 1. `encoder_counts`: slots in blocks at or beyond a device's count carry no edge. For every mesh index, one device of the edge axis has all 16 blocks live. `mesh_receivers`: A multimesh edge of a device with mesh index b has its receiver among the mesh nodes b * 128 to (b + 1) * 128 - 1. `mesh_senders`: A multimesh edge of a device with mesh index b has its sender either among the mesh nodes b * 128 to (b + 1) * 128 - 1, or at a node n with n mod 16 below 4.
All inputs are finite; a program needn't handle non-finite values.
Results may differ from the reference program's by a relative error of at most 0.039.
Values may be sent and summed in bfloat16 or wider, within the bound.
A program may use at most 128 MiB of HBM per device.

```python
import jax
import jax.numpy as jnp
from jax import lax

CHANNELS = 474
LATENT = 512
MESH_DEV = 16
COARSE_DEV = 4
BLOCK = 128
G2M_BLOCKS = 16
M2M_BLOCKS = 2
OWNERS = 128
GRID = 65536
BAND = 4096
MESH = 2048
SHARD = 128
G2M_EDGES = 262144
M2M_EDGES = 32768
N_MESH = 16
N_EDGE = 8


def slot_band(total, per_device):
    return jnp.arange(total, dtype=jnp.int32) // per_device // N_EDGE


def draw_encoder_senders(key, part):
    band_number = slot_band(G2M_EDGES, G2M_BLOCKS * BLOCK)
    offsets = jax.random.randint(jax.random.fold_in(key, 11), (G2M_EDGES,), 0, BAND)
    return (band_number * BAND + offsets).astype(jnp.int32)


def draw_encoder_receivers(key, part):
    band_number = slot_band(G2M_EDGES, G2M_BLOCKS * BLOCK)
    offsets = jax.random.randint(jax.random.fold_in(key, 12), (G2M_EDGES,), 0, SHARD)
    return (band_number * SHARD + offsets).astype(jnp.int32)


def draw_encoder_counts(key, part):
    busiest = jax.random.randint(jax.random.fold_in(key, 13), (N_MESH,), 0, N_EDGE)
    lowest = max(G2M_BLOCKS // 4, 1)
    highest = max(3 * G2M_BLOCKS // 8, lowest)
    lighter = jax.random.randint(jax.random.fold_in(key, 14), (OWNERS,), lowest, highest + 1)
    devices = jnp.arange(OWNERS, dtype=jnp.int32)
    heavy = devices % N_EDGE == busiest[devices // N_EDGE]
    return jnp.where(heavy, G2M_BLOCKS, lighter).astype(jnp.int32)


def draw_mesh_receivers(key, part):
    band_number = slot_band(M2M_EDGES, M2M_BLOCKS * BLOCK)
    offsets = jax.random.randint(jax.random.fold_in(key, 15), (M2M_EDGES,), 0, SHARD)
    return (band_number * SHARD + offsets).astype(jnp.int32)


def draw_mesh_senders(key, part):
    band_number = slot_band(M2M_EDGES, M2M_BLOCKS * BLOCK)
    nearby = band_number * SHARD + jax.random.randint(jax.random.fold_in(key, 16), (M2M_EDGES,), 0, SHARD)
    owners = jax.random.randint(jax.random.fold_in(key, 17), (M2M_EDGES,), 0, OWNERS)
    coarse = owners * MESH_DEV + jax.random.randint(jax.random.fold_in(key, 18), (M2M_EDGES,), 0, COARSE_DEV)
    faraway = jax.random.randint(jax.random.fold_in(key, 19), (M2M_EDGES,), 0, 4) == 0
    return jnp.where(faraway, coarse, nearby).astype(jnp.int32)


def block_scale(rng, shape, pieces, least, high):
    loudness = 1.0
    for position, blocks in pieces:
        draws = jax.random.uniform(jax.random.fold_in(jax.random.fold_in(rng, 6), position), (blocks,), jnp.float32, least / len(pieces), high / len(pieces))
        loudness = loudness * jnp.repeat(jnp.exp(draws), shape[position] // blocks).reshape((-1,) + (1,) * (len(shape) - 1 - position))
    return loudness


def gaussian(rng, dims, scale, most, shards=(), kind=jnp.bfloat16):
    entries = scale * jax.random.normal(rng, dims, jnp.float32)
    if shards:
        entries = entries * block_scale(rng, dims, shards, -0.22, 0.18)
    return jnp.clip(entries, -most, most).astype(kind)


def setup_inputs(seed: int = 0, part: int = 0) -> dict:
    key_of = jax.random.split(jax.random.key(seed), 26)
    part_keys = jax.random.split(jax.random.fold_in(key_of[25], part), 26)
    return {
        "grid_input": gaussian(part_keys[0], (GRID, CHANNELS), 1.0, 6.0, ((0, 128),)),
        "mesh_position": jnp.clip(jax.random.uniform(key_of[1], (3, MESH), jnp.float32, -1.0, 1.0) * block_scale(key_of[1], (3, MESH), ((1, 128),), -0.4, 0.0), -1.0, 1.0).astype(jnp.bfloat16),
        "encoder_senders": draw_encoder_senders(jax.random.fold_in(key_of[25], 71), part),
        "encoder_receivers": draw_encoder_receivers(jax.random.fold_in(key_of[25], 71), part),
        "encoder_features": gaussian(key_of[4], (4, G2M_EDGES), 1.0, 6.0, ((1, 128),)),
        "encoder_counts": draw_encoder_counts(jax.random.fold_in(key_of[25], 71), part),
        "mesh_senders": draw_mesh_senders(jax.random.fold_in(key_of[25], 71), part),
        "mesh_receivers": draw_mesh_receivers(jax.random.fold_in(key_of[25], 71), part),
        "mesh_features": gaussian(key_of[8], (4, M2M_EDGES), 1.0, 6.0, ((1, 128),)),
        "cotangent": gaussian(part_keys[9], (MESH, LATENT), 1.0, 6.0, ((0, 128),)),
        "grid_first": gaussian(key_of[10], (CHANNELS, LATENT), CHANNELS ** -0.5, 0.25),
        "grid_second": gaussian(key_of[11], (LATENT, LATENT), LATENT ** -0.5, 0.25),
        "encoder_inner": gaussian(key_of[12], (LATENT, LATENT), LATENT ** -0.5, 0.25),
        "encoder_geometry": gaussian(key_of[13], (4, LATENT), 4 ** -0.5, 3.0),
        "encoder_outer": gaussian(key_of[14], (LATENT, LATENT), LATENT ** -0.5, 0.25),
        "node_first": gaussian(key_of[15], (LATENT, LATENT), LATENT ** -0.5, 0.25),
        "node_position": gaussian(key_of[16], (3, LATENT), 3 ** -0.5, 3.5),
        "node_second": gaussian(key_of[17], (LATENT, LATENT), LATENT ** -0.5, 0.25),
        "edge_sender": gaussian(key_of[18], (LATENT, LATENT), LATENT ** -0.5, 0.25),
        "edge_receiver": gaussian(key_of[19], (LATENT, LATENT), LATENT ** -0.5, 0.25),
        "edge_geometry": gaussian(key_of[20], (4, LATENT), 4 ** -0.5, 3.0),
        "edge_outer": gaussian(key_of[21], (LATENT, LATENT), LATENT ** -0.5, 0.25),
        "update_message": gaussian(key_of[22], (LATENT, LATENT), LATENT ** -0.5, 0.25),
        "update_state": gaussian(key_of[23], (LATENT, LATENT), LATENT ** -0.5, 0.25),
        "update_outer": gaussian(key_of[24], (LATENT, LATENT), LATENT ** -0.5, 0.25),
    }


def product(left, right):
    return jnp.dot(left, right, preferred_element_type=jnp.float32)

def layer_norm(values):
    centred = values - lax.optimization_barrier(jnp.mean(values, axis=-1, keepdims=True))
    variance = lax.optimization_barrier(jnp.mean(centred * centred, axis=-1, keepdims=True))
    return centred * lax.rsqrt(variance + 1e-05)

def silu_grad(values):
    sigma = jax.nn.sigmoid(values)
    return sigma * (1.0 + values * (1.0 - sigma))

def reference(grid_input, mesh_position, encoder_senders, encoder_receivers, encoder_features, encoder_counts, mesh_senders, mesh_receivers, mesh_features, cotangent, grid_first, grid_second, encoder_inner, encoder_geometry, encoder_outer, node_first, node_position, node_second, edge_sender, edge_receiver, edge_geometry, edge_outer, update_message, update_state, update_outer):
    grid_hidden = jax.nn.silu(product(grid_input, grid_first)).astype(jnp.bfloat16)
    grid_latent = layer_norm(product(grid_hidden, grid_second)).astype(jnp.bfloat16)
    per_device = G2M_BLOCKS * BLOCK
    slots = jnp.arange(G2M_EDGES, dtype=jnp.int32)
    owner = slots // per_device
    block_number = slots % per_device // BLOCK
    live = (block_number < encoder_counts[owner]).astype(jnp.float32)
    enc_pre = product(grid_latent[encoder_senders], encoder_inner) + product(encoder_features.T, encoder_geometry)
    enc_act = jax.nn.silu(enc_pre).astype(jnp.bfloat16)
    enc_message = product(enc_act, encoder_outer) * live[:, None]
    enc_sum = jnp.zeros((MESH, LATENT), jnp.float32).at[encoder_receivers].add(enc_message)
    node_hidden = jax.nn.silu(product(enc_sum.astype(jnp.bfloat16), node_first) + product(mesh_position.T, node_position)).astype(jnp.bfloat16)
    mesh_latent = layer_norm(product(node_hidden, node_second)).astype(jnp.bfloat16)
    proc_pre = product(mesh_latent[mesh_senders], edge_sender) + product(mesh_latent[mesh_receivers], edge_receiver) + product(mesh_features.T, edge_geometry)
    proc_act = jax.nn.silu(proc_pre).astype(jnp.bfloat16)
    proc_message = product(proc_act, edge_outer)
    proc_sum = jnp.zeros((MESH, LATENT), jnp.float32).at[mesh_receivers].add(proc_message).astype(jnp.bfloat16)
    update_pre = product(proc_sum, update_message) + product(mesh_latent, update_state)
    update_act = jax.nn.silu(update_pre).astype(jnp.bfloat16)
    mesh_output = (mesh_latent.astype(jnp.float32) + product(update_act, update_outer)).astype(jnp.bfloat16)
    grad_pre = (product(cotangent, update_outer.T) * silu_grad(update_pre)).astype(jnp.bfloat16)
    grad_sum = product(grad_pre, update_message.T).astype(jnp.bfloat16)
    grad_node = cotangent.astype(jnp.float32) + product(grad_pre, update_state.T)
    grad_edge = (product(grad_sum[mesh_receivers], edge_outer.T) * silu_grad(proc_pre)).astype(jnp.bfloat16)
    mesh_gradient = grad_node.at[mesh_senders].add(product(grad_edge, edge_sender.T))
    mesh_gradient = mesh_gradient.at[mesh_receivers].add(product(grad_edge, edge_receiver.T))
    return (mesh_output, mesh_gradient)
```

```python
import functools

import jax
import jax.numpy as jnp
from jax import lax
from jax.experimental import pallas as pl
from jax.experimental.pallas import tpu as pltpu
from jax.sharding import PartitionSpec as P

BLOCK = 128
CHUNK_ROWS = 8
WINDOW = 256
COARSE = 4
MESH = pl.DeviceIdType.MESH
F32 = jnp.float32
BF16 = jnp.bfloat16
I32 = jnp.int32


def bits(size):
    return size.bit_length() - 1


def nn(left, right):
    return jnp.dot(left, right, preferred_element_type=F32)


def nt(left, right):
    return lax.dot_general(left, right, (((1,), (1,)), ((), ())), preferred_element_type=F32)


def tn(left, right):
    return lax.dot_general(left, right, (((0,), (0,)), ((), ())), preferred_element_type=F32)


def tt(left, right):
    return lax.dot_general(left, right, (((0,), (1,)), ((), ())), preferred_element_type=F32)


def sigmoid(values):
    return 0.5 + 0.5 * jnp.tanh(0.5 * values)


def layer_norm(values):
    centred = values - jnp.mean(values, axis=-1, keepdims=True)
    variance = jnp.mean(centred * centred, axis=-1, keepdims=True)
    return centred * lax.rsqrt(variance + 1e-05)


def iota(shape, dim):
    return lax.broadcasted_iota(I32, shape, dim)


def one_hot(hits):
    return jnp.where(hits, 1.0, 0.0).astype(BF16)


def greet(axis, count):
    me = lax.axis_index(axis)
    barrier = pltpu.get_barrier_semaphore()

    def signal(k, carry):
        pl.semaphore_signal(
            barrier, inc=1, device_id={axis: lax.rem(me + k, count)}, device_id_type=MESH
        )
        return carry

    lax.fori_loop(1, count, signal, 0)


def each_peer(axis, count, action):
    me = lax.axis_index(axis)

    def step(k, carry):
        action(me, lax.rem(me + k, count))
        return carry

    lax.fori_loop(1, count, step, 0)


def embed_kernel(
    n_edge,
    count,
    senders,
    receivers,
    features,
    grid_input,
    first,
    second,
    inner,
    packed_all,
    features_all,
    projected,
    rows_v,
    first_v,
    second_v,
    inner_v,
    load_sem,
    send_a,
    send_b,
    recv_a,
    recv_b,
):
    me = lax.axis_index("edge")
    band = lax.axis_index("mesh")
    loads = [
        pltpu.make_async_copy(src, dst, load_sem.at[k])
        for k, (src, dst) in enumerate(
            [(grid_input, rows_v), (first, first_v), (second, second_v), (inner, inner_v)]
        )
    ]
    for load in loads:
        load.start()
    greet("edge", n_edge)
    blocks = senders.shape[0]
    rows = grid_input.shape[0]
    shard = packed_shard(n_edge)
    low = senders[...] - band * (rows * n_edge)
    near = receivers[...] - band * shard
    live = iota((blocks, BLOCK), 0) < count[0]
    packed_all[me] = jnp.where(live, low * shard + near, -1)
    features_all[me] = features[...]
    pl.semaphore_wait(pltpu.get_barrier_semaphore(), n_edge - 1)

    def copy_packed(owner, peer, sem):
        return pltpu.make_async_remote_copy(
            src_ref=packed_all.at[owner],
            dst_ref=packed_all.at[owner],
            send_sem=send_a.at[sem],
            recv_sem=recv_a.at[owner],
            device_id={"edge": peer},
            device_id_type=MESH,
        )

    def copy_features(owner, peer, sem):
        return pltpu.make_async_remote_copy(
            src_ref=features,
            dst_ref=features_all.at[owner],
            send_sem=send_b.at[sem],
            recv_sem=recv_b.at[owner],
            device_id={"edge": peer},
            device_id_type=MESH,
        )

    def send(own, peer):
        copy_packed(own, peer, peer).start()
        copy_features(own, peer, peer).start()

    each_peer("edge", n_edge, send)
    loads[0].wait()
    loads[1].wait()
    hidden = nn(rows_v[...], first_v[...])
    hidden = (hidden * sigmoid(hidden)).astype(BF16)
    loads[2].wait()
    latent = layer_norm(nn(hidden, second_v[...])).astype(BF16)
    loads[3].wait()
    projected[...] = tt(inner_v[...], latent).astype(BF16)

    def arrive(own, peer):
        copy_packed(own, peer, peer).wait_send()
        copy_features(own, peer, peer).wait_send()
        copy_packed(peer, peer, peer).wait_recv()
        copy_features(peer, peer, peer).wait_recv()

    each_peer("edge", n_edge, arrive)


def packed_shard(n_edge):
    return 16 * n_edge


def encode_kernel(
    n_edge,
    shard,
    packed,
    features,
    projected,
    geometry,
    partial,
    position,
    bounds_v,
    bounds,
    queue,
    geometry_v,
    total,
    sem,
):
    me = lax.axis_index("edge")
    blocks = packed.shape[0]
    per_device = blocks // n_edge
    grid_rows = projected.shape[1]
    width = projected.shape[0]
    shift = bits(shard)
    row_bits = bits(grid_rows)
    index = packed[...]
    own = (index >> (shift + row_bits)) == me
    own_b = one_hot(own)
    upper = one_hot(iota((BLOCK, BLOCK), 0) < iota((BLOCK, BLOCK), 1))
    before = one_hot(iota((blocks, blocks), 0) < iota((blocks, blocks), 1))
    lower = one_hot(iota((blocks, blocks), 0) > iota((blocks, blocks), 1))
    ones = jnp.ones((BLOCK, BLOCK), BF16)
    rank = nn(own_b, upper)
    per_block = nn(own_b, ones)
    base = nn(lower, per_block.astype(BF16))
    position[...] = jnp.where(own, (rank + base).astype(I32), -1)
    totals = nt(jnp.ones((8, BLOCK), BF16), own_b)
    starts = nn(totals.astype(BF16), before)
    stops = starts + totals
    bounds_v[...] = jnp.where(iota((8, blocks), 0) == 0, starts, stops).astype(I32)
    copy = pltpu.make_async_copy(bounds_v, bounds, sem)
    copy.start()
    queue[...] = jnp.zeros_like(queue)
    total[...] = jnp.zeros_like(total)
    geometry_v[...] = jnp.zeros_like(geometry_v)
    geometry_v[0:4, :] = geometry[...].astype(F32)
    copy.wait()
    chunk = CHUNK_ROWS * BLOCK
    per_chunk = per_device // CHUNK_ROWS

    def sort_chunk(c, carry):
        first = bounds[0, c * CHUNK_ROWS]
        last = bounds[1, c * CHUNK_ROWS + CHUNK_ROWS - 1]

        @pl.when(last > first)
        def _():
            device = lax.div(c, per_chunk)
            lane = pl.multiple_of(lax.rem(c, per_chunk) * chunk, chunk)
            row = pl.multiple_of(c * CHUNK_ROWS, CHUNK_ROWS)
            code = packed[pl.ds(row, CHUNK_ROWS), :]
            where = position[pl.ds(row, CHUNK_ROWS), :]
            code_row = jnp.concatenate([code[k : k + 1, :] for k in range(CHUNK_ROWS)], axis=1)
            where_row = jnp.concatenate([where[k : k + 1, :] for k in range(CHUNK_ROWS)], axis=1)
            sender = (code_row >> shift) & (grid_rows - 1)
            parts = features[device, :, pl.ds(lane, chunk)].astype(F32)
            parts = jnp.concatenate([parts, jnp.zeros_like(parts)], axis=0)
            place = iota((8, chunk), 0)
            high = (sender >> 7).astype(F32)
            rest = (sender & 127).astype(F32)
            target = ((code_row & (shard - 1)) + 1).astype(F32)
            parts = jnp.where(place == 4, high, parts)
            parts = jnp.where(place == 5, rest, parts)
            parts = jnp.where(place == 6, target, parts)
            parts = parts.astype(BF16)
            start = lax.div(first, BLOCK) * BLOCK

            def fill(w, inner_carry):
                offset = pl.multiple_of(start + w * WINDOW, BLOCK)
                slots = iota((WINDOW, chunk), 0)
                hits = one_hot(slots == where_row - offset)
                queue[:, pl.ds(offset, WINDOW)] += nt(parts, hits)
                return inner_carry

            lax.fori_loop(0, lax.div(last - start + WINDOW - 1, WINDOW), fill, 0)

        return carry

    lax.fori_loop(0, n_edge * per_chunk, sort_chunk, 0)
    found = bounds[1, blocks - 1]

    def encode(j, carry):
        offset = pl.multiple_of(j * WINDOW, WINDOW)
        parts = queue[:, pl.ds(offset, WINDOW)]
        sender = (parts[4:5, :] * 128.0 + parts[5:6, :]).astype(I32)
        target = parts[6:7, :].astype(I32)
        picks = one_hot(iota((grid_rows, WINDOW), 0) == sender)
        goes = one_hot(iota((shard, WINDOW), 0) + 1 == target)
        pre = nn(projected[...], picks)
        pre = pre + tn(geometry_v[...].astype(BF16), parts.astype(BF16))
        act = (pre * sigmoid(pre)).astype(BF16)
        total[...] += nt(goes, act)
        return carry

    lax.fori_loop(0, lax.div(found + WINDOW - 1, WINDOW), encode, 0)
    partial[...] = total[...].astype(BF16)


def step_of(place):
    return jnp.where((place & 1) == 1, (place + 1) >> 1, -(place >> 1))


def place_of(step, n_mesh):
    step = step & (n_mesh - 1)
    return jnp.where(
        step == 0, 0, jnp.where(step <= n_mesh // 2, 2 * step - 1, 2 * (n_mesh - step))
    )


def process_kernel(
    n_mesh,
    n_edge,
    partial,
    mesh_position,
    senders,
    receivers,
    features,
    cotangent,
    node_position,
    geometry,
    w_encoder_outer,
    w_node_first,
    w_node_second,
    w_edge_sender,
    w_edge_receiver,
    w_edge_outer,
    w_update_message,
    w_update_state,
    w_update_outer,
    output,
    gradient,
    encoder_outer,
    node_first,
    node_second,
    edge_sender,
    edge_receiver,
    edge_outer,
    update_message,
    update_state,
    update_outer,
    padded,
    small,
    enc_land,
    latents,
    coarse_own,
    coarse_land,
    coarse,
    send_pick,
    recv_pick,
    send_drop,
    recv_drop,
    edge_term,
    slope,
    proc_send,
    proc_land,
    grads,
    back_band,
    back_band_land,
    back_coarse,
    back_coarse_land,
    back_far,
    back_far_land,
    tail,
    load_sem,
    send_sem,
    recv_sem,
    far_send,
    far_recv,
    relay_send,
    relay_recv,
    final_send,
    final_recv,
):
    me = lax.axis_index("edge")
    band = lax.axis_index("mesh")
    own_rows = cotangent.shape[0]
    shard = own_rows * n_edge
    groups = n_mesh * COARSE // own_rows
    per_group = own_rows // COARSE
    edges = senders.shape[1]
    far_rows = n_mesh * COARSE
    loads = [
        pltpu.make_async_copy(src, dst, load_sem.at[k])
        for k, (src, dst) in enumerate(
            [
                (w_encoder_outer, encoder_outer),
                (w_node_first, node_first),
                (w_node_second, node_second),
                (w_edge_sender, edge_sender),
                (w_edge_receiver, edge_receiver),
                (w_edge_outer, edge_outer),
                (w_update_message, update_message),
                (w_update_state, update_state),
                (w_update_outer, update_outer),
            ]
        )
    ]
    for load in loads:
        load.start()
    greet("edge", n_edge)
    greet("mesh", n_mesh)

    padded[...] = jnp.zeros_like(padded)
    padded[0:3, 0:own_rows] = mesh_position[...].astype(F32)
    place_columns = padded[...].T
    position_term = jnp.zeros((own_rows, node_position.shape[1]), F32)
    for k in range(3):
        position_term += (
            place_columns[0:own_rows, k : k + 1] * node_position[k : k + 1, :].astype(F32)
        )

    pl.semaphore_wait(pltpu.get_barrier_semaphore(), n_edge - 1 + n_mesh - 1)

    def to_peer(phase, src, dst, sem, land):
        def copy(peer):
            return pltpu.make_async_remote_copy(
                src_ref=src(peer),
                dst_ref=dst,
                send_sem=send_sem.at[phase, sem(peer)],
                recv_sem=recv_sem.at[phase, land],
                device_id={"edge": peer},
                device_id_type=MESH,
            )

        return copy

    def start_all(phase, src, dst):
        each_peer(
            "edge",
            n_edge,
            lambda own, peer: to_peer(phase, src, dst.at[own], lambda p: p, own)(peer).start(),
        )

    def wait_all(phase, src, dst):
        def finish(own, peer):
            to_peer(phase, src, dst.at[own], lambda p: p, own)(peer).wait_send()
            to_peer(phase, src, dst.at[peer], lambda p: p, peer)(peer).wait_recv()

        each_peer("edge", n_edge, finish)

    def rows_of(ref):
        return lambda peer: ref.at[pl.ds(pl.multiple_of(peer * own_rows, own_rows), own_rows), :]

    own_slice = pl.ds(pl.multiple_of(me * own_rows, own_rows), own_rows)
    start_all(0, rows_of(partial), enc_land)
    enc_land[me] = partial[own_slice, :]

    sender = senders[...]
    local = sender - band * shard
    owner_band = sender >> bits(shard)
    owner_edge = (sender >> bits(own_rows)) & (n_edge - 1)
    far_place = place_of(owner_band - band, n_mesh)
    far = shard + owner_edge * far_rows + far_place * COARSE + (sender & (COARSE - 1))
    pick = jnp.where(owner_band == band, local, far)
    receiver = receivers[...] - band * shard
    table_rows = shard + n_edge * far_rows
    send_drop[...] = one_hot(iota((table_rows, edges), 0) == pick)
    recv_drop[...] = one_hot(iota((shard, edges), 0) == receiver)
    pick_columns = jnp.broadcast_to(pick.astype(F32), (128, edges)).T.astype(I32)
    recv_columns = jnp.broadcast_to(receiver.astype(F32), (128, edges)).T.astype(I32)
    lanes = iota((edges, 128), 1)
    for k in range(table_rows // 128):
        send_pick[:, k * 128 : (k + 1) * 128] = one_hot(lanes + k * 128 == pick_columns)
    for k in range(shard // 128):
        recv_pick[:, k * 128 : (k + 1) * 128] = one_hot(lanes + k * 128 == recv_columns)
    small[...] = jnp.zeros_like(small)
    small[0:4, 0:edges] = features[...].astype(F32)
    width = geometry.shape[1]
    padded_geometry = jnp.concatenate([geometry[...].astype(F32)] * 2, axis=0)
    padded_geometry = jnp.where(iota((8, width), 0) < 4, padded_geometry, 0.0)
    edge_term[...] = tn(small[...].astype(BF16), padded_geometry.astype(BF16))
    for load in loads:
        load.wait()
    back_out = nt(cotangent[...], update_outer[...])

    wait_all(0, rows_of(partial), enc_land)
    enc_sum = jnp.sum(enc_land[...].astype(F32), axis=0)
    enc_sum = nn(enc_sum.astype(BF16), encoder_outer[...])
    hidden = nn(enc_sum.astype(BF16), node_first[...]) + position_term
    hidden = (hidden * sigmoid(hidden)).astype(BF16)
    latent = layer_norm(nn(hidden, node_second[...])).astype(BF16)
    coarse_own[...] = latent[0:COARSE, :]
    latents[me] = latent

    def far_copy(place, land):
        return pltpu.make_async_remote_copy(
            src_ref=coarse_own,
            dst_ref=coarse_land.at[land],
            send_sem=far_send.at[place],
            recv_sem=far_recv.at[land],
            device_id={"mesh": (band + step_of(place) + n_mesh) & (n_mesh - 1)},
            device_id_type=MESH,
        )

    def far_start(k, carry):
        place = n_mesh - k
        far_copy(place, place_of(-step_of(place), n_mesh)).start()
        return carry

    lax.fori_loop(1, n_mesh, far_start, 0)
    latent_rows = lambda peer: latents.at[me]
    start_all(1, latent_rows, latents)
    coarse_land[0] = coarse_own[...]

    def relay(group, owner, peer):
        return pltpu.make_async_remote_copy(
            src_ref=coarse.at[me, group],
            dst_ref=coarse.at[owner, group],
            send_sem=relay_send.at[group, peer],
            recv_sem=relay_recv.at[group, owner],
            device_id={"edge": peer},
            device_id_type=MESH,
        )

    for group in range(groups):
        for k in range(per_group):
            place = group * per_group + k
            if place > 0:
                far_copy(place, place).wait_recv()
        rows = [coarse_land[group * per_group + k].astype(F32) for k in range(per_group)]
        coarse[me, group] = jnp.concatenate(rows, axis=0).astype(BF16)
        each_peer("edge", n_edge, lambda own, peer: relay(group, own, peer).start())

    wait_all(1, latent_rows, latents)
    band_latent = latents[...].reshape(shard, width)
    recv_rows = nn(recv_pick[...], band_latent).astype(BF16)
    send_rows = nn(send_pick[:, 0:shard], band_latent)
    edge_term[...] += nn(recv_rows, edge_receiver[...])

    def far_finish(k, carry):
        far_copy(k, k).wait_send()
        return carry

    lax.fori_loop(1, n_mesh, far_finish, 0)
    for group in range(groups):

        def relay_finish(own, peer):
            relay(group, own, peer).wait_send()
            relay(group, peer, peer).wait_recv()

        each_peer("edge", n_edge, relay_finish)

    far_latent = coarse[...].reshape(n_edge * far_rows, width)
    send_rows = (send_rows + nn(send_pick[:, shard:], far_latent)).astype(BF16)
    pre = edge_term[...] + nn(send_rows, edge_sender[...])
    sigma = sigmoid(pre)
    act = (pre * sigma).astype(BF16)
    slope[...] = sigma * (1.0 + pre * (1.0 - sigma))
    proc_send[...] = nn(recv_drop[...], act).astype(BF16)
    start_all(2, rows_of(proc_send), proc_land)
    proc_land[me] = proc_send[own_slice, :]
    state_term = nn(latents[me], update_state[...])
    wait_all(2, rows_of(proc_send), proc_land)
    proc_sum = jnp.sum(proc_land[...].astype(F32), axis=0)
    proc_sum = nn(proc_sum.astype(BF16), edge_outer[...]).astype(BF16)
    update_pre = nn(proc_sum, update_message[...]) + state_term
    sigma = sigmoid(update_pre)
    grad_pre = (back_out * (sigma * (1.0 + update_pre * (1.0 - sigma)))).astype(BF16)
    grad_sum = nt(grad_pre, update_message[...]).astype(BF16)
    grads[me] = nt(grad_sum, edge_outer[...]).astype(BF16)
    grad_rows = lambda peer: grads.at[me]
    start_all(3, grad_rows, grads)
    update_act = (update_pre * sigma).astype(BF16)
    mixed = latents[me].astype(F32) + nn(update_act, update_outer[...])
    output[...] = mixed.astype(BF16)
    grad_node = cotangent[...].astype(F32) + nt(grad_pre, update_state[...])
    wait_all(3, grad_rows, grads)
    band_grads = grads[...].reshape(shard, width)
    grad_edge = (nn(recv_pick[...], band_grads) * slope[...]).astype(BF16)
    far_sum = nn(send_drop[shard:, :], grad_edge).astype(BF16)
    back_coarse[...] = far_sum.reshape(n_edge, far_rows, width)
    coarse_rows = lambda peer: back_coarse.at[peer]
    start_all(4, coarse_rows, back_coarse_land)
    back_coarse_land[me] = back_coarse[me]
    to_sender = nn(send_drop[0:shard, :], grad_edge).astype(BF16)
    to_receiver = nn(recv_drop[...], grad_edge).astype(BF16)
    back = nt(to_sender, edge_sender[...]) + nt(to_receiver, edge_receiver[...])
    back_band[...] = back.astype(BF16)
    start_all(5, rows_of(back_band), back_band_land)
    back_band_land[me] = back_band[own_slice, :]
    wait_all(4, coarse_rows, back_coarse_land)
    far_total = jnp.sum(back_coarse_land[...].astype(F32), axis=0)

    def final_copy(place, land):
        return pltpu.make_async_remote_copy(
            src_ref=back_far.at[place],
            dst_ref=back_far_land.at[land],
            send_sem=final_send.at[place],
            recv_sem=final_recv.at[land],
            device_id={"mesh": (band + step_of(place) + n_mesh) & (n_mesh - 1)},
            device_id_type=MESH,
        )

    for place in range(1, n_mesh):
        back_far[place] = far_total[place * COARSE : (place + 1) * COARSE, :].astype(BF16)

    def final_start(k, carry):
        place = n_mesh - k
        final_copy(place, place_of(-step_of(place), n_mesh)).start()
        return carry

    lax.fori_loop(1, n_mesh, final_start, 0)
    wait_all(5, rows_of(back_band), back_band_land)
    result = grad_node + jnp.sum(back_band_land[...].astype(F32), axis=0)

    def final_finish(k, carry):
        final_copy(k, k).wait_send()
        final_copy(k, k).wait_recv()
        return carry

    lax.fori_loop(1, n_mesh, final_finish, 0)
    arrived = back_far_land[1].astype(F32)
    for place in range(2, n_mesh):
        arrived = arrived + back_far_land[place].astype(F32)
    tail[...] = jnp.zeros_like(tail)
    tail[0:COARSE, :] = arrived
    gradient[...] = result + nt(tail[...].astype(BF16), edge_sender[...])


def vmem():
    return pl.BlockSpec(memory_space=pltpu.VMEM)


def anywhere():
    return pl.BlockSpec(memory_space=pl.ANY)


def shards(
    n_mesh,
    n_edge,
    grid_input,
    mesh_position,
    encoder_senders,
    encoder_receivers,
    encoder_features,
    encoder_counts,
    mesh_senders,
    mesh_receivers,
    mesh_features,
    cotangent,
    grid_first,
    grid_second,
    encoder_inner,
    encoder_geometry,
    encoder_outer,
    node_first,
    node_position,
    node_second,
    edge_sender,
    edge_receiver,
    edge_geometry,
    edge_outer,
    update_message,
    update_state,
    update_outer,
):
    grid_rows, channels = grid_input.shape
    width = grid_second.shape[1]
    slots = encoder_senders.shape[0]
    blocks = slots // BLOCK
    own_rows = mesh_position.shape[1]
    shard = own_rows * n_edge
    edges = mesh_senders.shape[0]
    dma = pltpu.SemaphoreType.DMA
    packed, features, projected = pl.pallas_call(
        functools.partial(embed_kernel, n_edge),
        out_shape=(
            jax.ShapeDtypeStruct((n_edge, blocks, BLOCK), I32),
            jax.ShapeDtypeStruct((n_edge, 4, slots), BF16),
            jax.ShapeDtypeStruct((width, grid_rows), BF16),
        ),
        in_specs=[pl.BlockSpec(memory_space=pltpu.SMEM)] + [vmem()] * 3 + [anywhere()] * 4,
        out_specs=(vmem(), vmem(), vmem()),
        scratch_shapes=[
            pltpu.VMEM((grid_rows, channels), BF16),
            pltpu.VMEM((channels, width), BF16),
            pltpu.VMEM((width, width), BF16),
            pltpu.VMEM((width, width), BF16),
            dma((4,)),
            dma((n_edge,)),
            dma((n_edge,)),
            dma((n_edge,)),
            dma((n_edge,)),
        ],
        compiler_params=pltpu.CompilerParams(collective_id=0, has_side_effects=True),
    )(
        encoder_counts,
        encoder_senders.reshape(blocks, BLOCK),
        encoder_receivers.reshape(blocks, BLOCK),
        encoder_features,
        grid_input,
        grid_first,
        grid_second,
        encoder_inner,
    )
    all_blocks = n_edge * blocks
    partial = pl.pallas_call(
        functools.partial(encode_kernel, n_edge, shard),
        out_shape=jax.ShapeDtypeStruct((shard, width), BF16),
        in_specs=[vmem()] * 4,
        out_specs=vmem(),
        scratch_shapes=[
            pltpu.VMEM((all_blocks, BLOCK), I32),
            pltpu.VMEM((8, all_blocks), I32),
            pltpu.SMEM((8, all_blocks), I32),
            pltpu.VMEM((8, n_edge * slots + 2 * WINDOW), F32),
            pltpu.VMEM((8, width), F32),
            pltpu.VMEM((shard, width), F32),
            dma(()),
        ],
    )(packed.reshape(all_blocks, BLOCK), features, projected, encoder_geometry)
    far_rows = n_mesh * COARSE
    groups = far_rows // own_rows
    table_rows = shard + n_edge * far_rows
    weights = [
        encoder_outer,
        node_first,
        node_second,
        edge_sender,
        edge_receiver,
        edge_outer,
        update_message,
        update_state,
        update_outer,
    ]
    return pl.pallas_call(
        functools.partial(process_kernel, n_mesh, n_edge),
        out_shape=(
            jax.ShapeDtypeStruct((own_rows, width), BF16),
            jax.ShapeDtypeStruct((own_rows, width), F32),
        ),
        in_specs=[vmem()] * 8 + [anywhere()] * 9,
        out_specs=(vmem(), vmem()),
        scratch_shapes=[pltpu.VMEM((width, width), BF16) for _ in weights]
        + [
            pltpu.VMEM((128, 128), F32),
            pltpu.VMEM((8, edges), F32),
            pltpu.VMEM((n_edge, own_rows, width), BF16),
            pltpu.VMEM((n_edge, own_rows, width), BF16),
            pltpu.VMEM((COARSE, width), BF16),
            pltpu.VMEM((n_mesh, COARSE, width), BF16),
            pltpu.VMEM((n_edge, groups, own_rows, width), BF16),
            pltpu.VMEM((edges, table_rows), BF16),
            pltpu.VMEM((edges, shard), BF16),
            pltpu.VMEM((table_rows, edges), BF16),
            pltpu.VMEM((shard, edges), BF16),
            pltpu.VMEM((edges, width), F32),
            pltpu.VMEM((edges, width), F32),
            pltpu.VMEM((shard, width), BF16),
            pltpu.VMEM((n_edge, own_rows, width), BF16),
            pltpu.VMEM((n_edge, own_rows, width), BF16),
            pltpu.VMEM((shard, width), BF16),
            pltpu.VMEM((n_edge, own_rows, width), BF16),
            pltpu.VMEM((n_edge, far_rows, width), BF16),
            pltpu.VMEM((n_edge, far_rows, width), BF16),
            pltpu.VMEM((n_mesh, COARSE, width), BF16),
            pltpu.VMEM((n_mesh, COARSE, width), BF16),
            pltpu.VMEM((own_rows, width), F32),
            dma((9,)),
            dma((6, n_edge)),
            dma((6, n_edge)),
            dma((n_mesh,)),
            dma((n_mesh,)),
            dma((groups, n_edge)),
            dma((groups, n_edge)),
            dma((n_mesh,)),
            dma((n_mesh,)),
        ],
        compiler_params=pltpu.CompilerParams(collective_id=1, has_side_effects=True),
    )(
        partial,
        mesh_position,
        mesh_senders.reshape(1, edges),
        mesh_receivers.reshape(1, edges),
        mesh_features,
        cotangent,
        node_position,
        edge_geometry,
        *weights,
    )


def solution(mesh):
    banded = ("mesh", "edge")
    every = ("groups", "mesh", "edge")
    in_specs = (
        P(every, None),
        P(None, banded),
        P(banded),
        P(banded),
        P(None, banded),
        P(banded),
        P(banded),
        P(banded),
        P(None, banded),
        P(every, None),
    ) + (P(),) * 15
    return jax.shard_map(
        functools.partial(shards, mesh.shape["mesh"], mesh.shape["edge"]),
        mesh=mesh,
        in_specs=in_specs,
        out_specs=(P(every, None), P(every, None)),
        check_vma=False,
    )
```

```python
import functools

import jax
import jax.numpy as jnp
from jax import lax
from jax.experimental import pallas as pl
from jax.experimental.pallas import tpu as pltpu
from jax.sharding import PartitionSpec as P

BLOCK = 128
CHUNK_ROWS = 8
WINDOW = 256
STEP = 512
COARSE = 4
MESH = pl.DeviceIdType.MESH
F32 = jnp.float32
BF16 = jnp.bfloat16
I32 = jnp.int32


def bits(size):
    return size.bit_length() - 1


def nn(left, right):
    return jnp.dot(left, right, preferred_element_type=F32)


def nt(left, right):
    return lax.dot_general(left, right, (((1,), (1,)), ((), ())), preferred_element_type=F32)


def tn(left, right):
    return lax.dot_general(left, right, (((0,), (0,)), ((), ())), preferred_element_type=F32)


def tt(left, right):
    return lax.dot_general(left, right, (((0,), (1,)), ((), ())), preferred_element_type=F32)


def sigmoid(values):
    return 0.5 + 0.5 * jnp.tanh(0.5 * values)


def layer_norm(values):
    centred = values - jnp.mean(values, axis=-1, keepdims=True)
    variance = jnp.mean(centred * centred, axis=-1, keepdims=True)
    return centred * lax.rsqrt(variance + 1e-05)


def iota(shape, dim):
    return lax.broadcasted_iota(I32, shape, dim)


def one_hot(hits):
    return jnp.where(hits, 1.0, 0.0).astype(BF16)


def greet(axis, count):
    me = lax.axis_index(axis)
    barrier = pltpu.get_barrier_semaphore()

    def signal(k, carry):
        pl.semaphore_signal(
            barrier, inc=1, device_id={axis: lax.rem(me + k, count)}, device_id_type=MESH
        )
        return carry

    lax.fori_loop(1, count, signal, 0)


def each_peer(axis, count, action):
    me = lax.axis_index(axis)

    def step(k, carry):
        action(me, lax.rem(me + k, count))
        return carry

    lax.fori_loop(1, count, step, 0)


def embed_kernel(
    n_edge,
    count,
    senders,
    receivers,
    features,
    mesh_senders,
    mesh_receivers,
    mesh_features,
    grid_input,
    first,
    second,
    inner,
    packed_all,
    features_all,
    projected,
    pair_senders,
    pair_receivers,
    pair_features,
    senders_v,
    receivers_v,
    rows_v,
    first_v,
    second_v,
    inner_v,
    load_sem,
    send_a,
    send_b,
    recv_a,
    recv_b,
    pair_send,
    pair_recv,
):
    me = lax.axis_index("edge")
    band = lax.axis_index("mesh")
    core = me & 1
    loads = [
        pltpu.make_async_copy(src, dst, load_sem.at[k])
        for k, (src, dst) in enumerate(
            [
                (senders, senders_v),
                (receivers, receivers_v),
                (features, features_all.at[me]),
                (mesh_senders, pair_senders.at[core]),
                (mesh_receivers, pair_receivers.at[core]),
                (mesh_features, pair_features.at[core]),
                (grid_input, rows_v),
                (first, first_v),
                (second, second_v),
                (inner, inner_v),
            ]
        )
    ]
    for load in loads:
        load.start()
    greet("edge", n_edge)
    blocks = senders.shape[0]
    rows = grid_input.shape[1]
    shard = packed_shard(n_edge)
    loads[0].wait()
    loads[1].wait()
    low = senders_v[...] - band * (rows * n_edge)
    near = receivers_v[...] - band * shard
    live = iota((blocks, BLOCK), 0) < count[0]
    packed_all[me] = jnp.where(live, low * shard + near, -1)
    for load in loads[2:6]:
        load.wait()
    pl.semaphore_wait(pltpu.get_barrier_semaphore(), n_edge - 1)

    def copy_packed(owner, peer, sem):
        return pltpu.make_async_remote_copy(
            src_ref=packed_all.at[owner],
            dst_ref=packed_all.at[owner],
            send_sem=send_a.at[sem],
            recv_sem=recv_a.at[owner],
            device_id={"edge": peer},
            device_id_type=MESH,
        )

    def copy_features(owner, peer, sem):
        return pltpu.make_async_remote_copy(
            src_ref=features_all.at[owner],
            dst_ref=features_all.at[owner],
            send_sem=send_b.at[sem],
            recv_sem=recv_b.at[owner],
            device_id={"edge": peer},
            device_id_type=MESH,
        )

    def send(own, peer):
        copy_packed(own, peer, peer).start()
        copy_features(own, peer, peer).start()

    each_peer("edge", n_edge, send)

    def copy_pair(ref, slot, k):
        return pltpu.make_async_remote_copy(
            src_ref=ref.at[slot],
            dst_ref=ref.at[slot],
            send_sem=pair_send.at[k],
            recv_sem=pair_recv.at[k],
            device_id={"edge": me ^ 1},
            device_id_type=MESH,
        )

    pairs = (pair_senders, pair_receivers, pair_features)
    for k, ref in enumerate(pairs):
        copy_pair(ref, core, k).start()
    loads[6].wait()
    loads[7].wait()
    hidden = tn(rows_v[...], first_v[...])
    hidden = (hidden * sigmoid(hidden)).astype(BF16)
    loads[8].wait()
    latent = layer_norm(nn(hidden, second_v[...])).astype(BF16)
    loads[9].wait()
    projected[...] = tt(inner_v[...], latent).astype(BF16)

    def arrive(own, peer):
        copy_packed(own, peer, peer).wait_send()
        copy_features(own, peer, peer).wait_send()
        copy_packed(peer, peer, peer).wait_recv()
        copy_features(peer, peer, peer).wait_recv()

    each_peer("edge", n_edge, arrive)
    for k, ref in enumerate(pairs):
        copy_pair(ref, core, k).wait_send()
        copy_pair(ref, core ^ 1, k).wait_recv()


def packed_shard(n_edge):
    return 16 * n_edge


def encode_kernel(
    n_edge,
    shard,
    packed,
    features,
    projected,
    geometry,
    partial,
    position,
    bounds_v,
    bounds,
    queue,
    geometry_v,
    geometry_w,
    total,
    sem,
    geometry_sem,
):
    me = lax.axis_index("edge")
    load = pltpu.make_async_copy(geometry, geometry_w, geometry_sem)
    load.start()
    blocks = packed.shape[0]
    per_device = blocks // n_edge
    grid_rows = projected.shape[1]
    width = projected.shape[0]
    shift = bits(shard)
    row_bits = bits(grid_rows)
    index = packed[...]
    own = (index >> (shift + row_bits)) == me
    own_b = one_hot(own)
    upper = one_hot(iota((BLOCK, BLOCK), 0) < iota((BLOCK, BLOCK), 1))
    before = one_hot(iota((blocks, blocks), 0) < iota((blocks, blocks), 1))
    lower = one_hot(iota((blocks, blocks), 0) > iota((blocks, blocks), 1))
    ones = jnp.ones((BLOCK, BLOCK), BF16)
    rank = nn(own_b, upper)
    per_block = nn(own_b, ones)
    base = nn(lower, per_block.astype(BF16))
    position[...] = jnp.where(own, (rank + base).astype(I32), -1)
    totals = nt(jnp.ones((8, BLOCK), BF16), own_b)
    starts = nn(totals.astype(BF16), before)
    stops = starts + totals
    bounds_v[...] = jnp.where(iota((8, blocks), 0) == 0, starts, stops).astype(I32)
    copy = pltpu.make_async_copy(bounds_v, bounds, sem)
    copy.start()
    queue[...] = jnp.zeros_like(queue)
    total[...] = jnp.zeros_like(total)
    geometry_v[...] = jnp.zeros_like(geometry_v)
    copy.wait()
    chunk = CHUNK_ROWS * BLOCK
    per_chunk = per_device // CHUNK_ROWS

    def chunk_of(c, device, lane, row):
        code = packed[pl.ds(row, CHUNK_ROWS), :]
        where = position[pl.ds(row, CHUNK_ROWS), :]
        code_row = jnp.concatenate([code[k : k + 1, :] for k in range(CHUNK_ROWS)], axis=1)
        where_row = jnp.concatenate([where[k : k + 1, :] for k in range(CHUNK_ROWS)], axis=1)
        sender = (code_row >> shift) & (grid_rows - 1)
        parts = features[device, :, pl.ds(lane, chunk)].astype(F32)
        parts = jnp.concatenate([parts, jnp.zeros_like(parts)], axis=0)
        place = iota((8, chunk), 0)
        parts = jnp.where(place == 4, (sender >> 7).astype(F32), parts)
        parts = jnp.where(place == 5, (sender & 127).astype(F32), parts)
        parts = jnp.where(place == 6, ((code_row & (shard - 1)) + 1).astype(F32), parts)
        return parts.astype(BF16), where_row

    def fill(parts, where_row, offset):
        offset = pl.multiple_of(offset, BLOCK)
        hits = one_hot(iota((WINDOW, chunk), 0) == where_row - offset)
        queue[:, pl.ds(offset, WINDOW)] += nt(parts, hits)

    for device in range(n_edge):
        c = device * per_chunk
        parts, where_row = chunk_of(c, device, 0, c * CHUNK_ROWS)
        fill(parts, where_row, bounds[0, c * CHUNK_ROWS] & -BLOCK)

    def sort_chunk(c, carry):
        first = bounds[0, c * CHUNK_ROWS]
        last = bounds[1, c * CHUNK_ROWS + CHUNK_ROWS - 1]
        part = c & (per_chunk - 1)
        skip = jnp.where(part == 0, WINDOW, 0)
        start = (first & -BLOCK) + skip

        @pl.when((last > first) & (last > start))
        def _():
            lane = pl.multiple_of(part * chunk, chunk)
            row = pl.multiple_of(c * CHUNK_ROWS, CHUNK_ROWS)
            parts, where_row = chunk_of(c, c >> bits(per_chunk), lane, row)

            def more(w, inner_carry):
                fill(parts, where_row, start + w * WINDOW)
                return inner_carry

            lax.fori_loop(0, (last - start + WINDOW - 1) >> bits(WINDOW), more, 0)

        return carry

    lax.fori_loop(0, n_edge * per_chunk, sort_chunk, 0)
    load.wait()
    geometry_v[0:4, :] = geometry_w[...].astype(F32)
    found = bounds[1, blocks - 1]

    def encode(j, carry):
        offset = pl.multiple_of(j * STEP, STEP)
        parts = queue[:, pl.ds(offset, STEP)]
        sender = (parts[4:5, :] * 128.0 + parts[5:6, :]).astype(I32)
        target = parts[6:7, :].astype(I32)
        picks = one_hot(iota((grid_rows, STEP), 0) == sender)
        goes = one_hot(iota((shard, STEP), 0) + 1 == target)
        pre = nn(projected[...], picks)
        pre = pre + tn(geometry_v[...].astype(BF16), parts.astype(BF16))
        act = (pre * sigmoid(pre)).astype(BF16)
        total[...] += nt(goes, act)
        return carry

    lax.fori_loop(0, lax.div(found + STEP - 1, STEP), encode, 0)
    partial[...] = total[...].astype(BF16)


def step_of(place):
    return jnp.where((place & 1) == 1, (place + 1) >> 1, -(place >> 1))


def place_of(step, n_mesh):
    step = step & (n_mesh - 1)
    return jnp.where(
        step == 0, 0, jnp.where(step <= n_mesh // 2, 2 * step - 1, 2 * (n_mesh - step))
    )


def process_kernel(
    n_mesh,
    n_edge,
    partial,
    mesh_position,
    pair_senders,
    pair_receivers,
    pair_features,
    cotangent,
    node_position,
    geometry,
    w_encoder_outer,
    w_node_first,
    w_node_second,
    w_edge_sender,
    w_edge_receiver,
    w_edge_outer,
    w_update_message,
    w_update_state,
    w_update_outer,
    output,
    gradient,
    encoder_outer,
    node_first,
    node_second,
    edge_sender,
    edge_receiver,
    edge_outer,
    update_message,
    update_state,
    update_outer,
    padded,
    small,
    enc_land,
    latents,
    coarse_own,
    coarse_land,
    coarse,
    send_pick,
    recv_pick,
    send_drop,
    recv_drop,
    edge_term,
    slope,
    proc_send,
    proc_land,
    grads,
    back_band,
    back_band_land,
    back_coarse,
    back_coarse_land,
    back_far,
    back_far_land,
    tail,
    enc_node,
    edge_update,
    load_sem,
    send_sem,
    recv_sem,
    far_send,
    far_recv,
    relay_send,
    relay_recv,
    forward_send,
    final_send,
    final_recv,
):
    me = lax.axis_index("edge")
    band = lax.axis_index("mesh")
    own_rows = cotangent.shape[0]
    shard = own_rows * n_edge
    groups = n_mesh * COARSE // own_rows
    per_group = own_rows // COARSE
    edges = 2 * pair_senders.shape[2]
    far_rows = n_mesh * COARSE
    loads = [
        pltpu.make_async_copy(src, dst, load_sem.at[k])
        for k, (src, dst) in enumerate(
            [
                (w_encoder_outer, encoder_outer),
                (w_node_first, node_first),
                (w_node_second, node_second),
                (w_edge_sender, edge_sender),
                (w_edge_receiver, edge_receiver),
                (w_edge_outer, edge_outer),
                (w_update_message, update_message),
                (w_update_state, update_state),
                (w_update_outer, update_outer),
            ]
        )
    ]
    for load in loads:
        load.start()
    greet("edge", n_edge)
    greet("mesh", n_mesh)

    padded[...] = jnp.zeros_like(padded)
    padded[0:3, 0:own_rows] = mesh_position[...].astype(F32)
    place_columns = padded[...].T
    position_term = jnp.zeros((own_rows, node_position.shape[1]), F32)
    for k in range(3):
        position_term += (
            place_columns[0:own_rows, k : k + 1] * node_position[k : k + 1, :].astype(F32)
        )

    pl.semaphore_wait(pltpu.get_barrier_semaphore(), n_edge - 1 + n_mesh - 1)

    core = me & 1
    chip = me >> 1
    chips = n_edge // 2
    chip_rows = chips * own_rows

    def each_chip(action):
        def step(k, carry):
            action(((chip + k) & (chips - 1)) * 2 + core)
            return carry

        lax.fori_loop(1, chips, step, 0)

    def to_peer(phase, src, dst, sem, land):
        def copy(peer):
            return pltpu.make_async_remote_copy(
                src_ref=src(peer),
                dst_ref=dst,
                send_sem=send_sem.at[phase, sem(peer)],
                recv_sem=recv_sem.at[phase, land],
                device_id={"edge": peer},
                device_id_type=MESH,
            )

        return copy

    def start_all(phase, src, dst):
        each_peer(
            "edge",
            n_edge,
            lambda own, peer: to_peer(phase, src, dst.at[own], lambda p: p, own)(peer).start(),
        )

    def wait_all(phase, src, dst):
        def finish(own, peer):
            to_peer(phase, src, dst.at[own], lambda p: p, own)(peer).wait_send()
            to_peer(phase, src, dst.at[peer], lambda p: p, peer)(peer).wait_recv()

        each_peer("edge", n_edge, finish)

    def chip_all(phase, ref, land, rows):
        def copy(peer, slot):
            start = pl.multiple_of((peer >> 1) * rows, rows)
            return pltpu.make_async_remote_copy(
                src_ref=ref.at[pl.ds(start, rows), :],
                dst_ref=land.at[slot],
                send_sem=send_sem.at[phase, peer],
                recv_sem=recv_sem.at[phase, slot],
                device_id={"edge": peer},
                device_id_type=MESH,
            )

        def start():
            each_chip(lambda peer: copy(peer, chip).start())
            land[chip] = ref[pl.ds(pl.multiple_of(chip * rows, rows), rows), :]

        def finish():
            each_chip(lambda peer: copy(peer, chip).wait_send())
            each_chip(lambda peer: copy(peer, peer >> 1).wait_recv())

        return start, finish

    def rows_of(ref):
        return lambda peer: ref.at[pl.ds(pl.multiple_of(peer * own_rows, own_rows), own_rows), :]

    own_slice = pl.ds(pl.multiple_of(me * own_rows, own_rows), own_rows)
    start_all(0, rows_of(partial), enc_land)
    enc_land[me] = partial[own_slice, :]

    sender = jnp.concatenate([pair_senders[0], pair_senders[1]], axis=1)
    receiver = jnp.concatenate([pair_receivers[0], pair_receivers[1]], axis=1)
    owner_band = sender >> bits(shard)
    near = owner_band == band
    owner_edge = (sender >> bits(own_rows)) & (n_edge - 1)
    far_place = place_of(owner_band - band, n_mesh)
    far_row = far_place * COARSE + (sender & (COARSE - 1))
    local = sender - band * shard
    pick = jnp.where(near, local, shard + owner_edge * far_rows + far_row)
    receiver = receiver - band * shard
    table_rows = shard + n_edge * far_rows

    def chip_row(row, owner):
        own_core = (owner & 1) == core
        return jnp.where(own_core, (owner >> 1) * own_rows + (row & (own_rows - 1)), -1)

    drop_near = jnp.where(near, chip_row(local, owner_edge), -1)
    drop_far = jnp.where((owner_edge & 1) == core, (owner_edge >> 1) * far_rows + far_row, -1)
    drop_far = jnp.where(near, -1, drop_far)
    drop_recv = chip_row(receiver, receiver >> bits(own_rows))
    send_drop[0:chip_rows, :] = one_hot(iota((chip_rows, edges), 0) == drop_near)
    send_drop[chip_rows:, :] = one_hot(iota((chips * far_rows, edges), 0) == drop_far)
    recv_drop[...] = one_hot(iota((chip_rows, edges), 0) == drop_recv)
    pick_columns = jnp.broadcast_to(pick.astype(F32), (128, edges)).T.astype(I32)
    recv_columns = jnp.broadcast_to(receiver.astype(F32), (128, edges)).T.astype(I32)
    lanes = iota((edges, 128), 1)
    for k in range(table_rows // 128):
        send_pick[:, k * 128 : (k + 1) * 128] = one_hot(lanes + k * 128 == pick_columns)
    for k in range(shard // 128):
        recv_pick[:, k * 128 : (k + 1) * 128] = one_hot(lanes + k * 128 == recv_columns)
    small[...] = jnp.zeros_like(small)
    half = edges // 2
    small[0:4, 0:half] = pair_features[0].astype(F32)
    small[0:4, half:edges] = pair_features[1].astype(F32)
    width = geometry.shape[1]
    padded_geometry = jnp.concatenate([geometry[...].astype(F32)] * 2, axis=0)
    padded_geometry = jnp.where(iota((8, width), 0) < 4, padded_geometry, 0.0)
    edge_term[...] = tn(small[...].astype(BF16), padded_geometry.astype(BF16))
    for load in loads:
        load.wait()
    back_out = nt(cotangent[...], update_outer[...])
    enc_node[...] = nn(encoder_outer[...], node_first[...]).astype(BF16)

    wait_all(0, rows_of(partial), enc_land)
    enc_sum = jnp.sum(enc_land[...].astype(F32), axis=0)
    hidden = nn(enc_sum.astype(BF16), enc_node[...]) + position_term
    hidden = (hidden * sigmoid(hidden)).astype(BF16)
    latent = layer_norm(nn(hidden, node_second[...])).astype(BF16)
    coarse_own[...] = latent[0:COARSE, :]
    latents[me] = latent

    def far_copy(place, land):
        return pltpu.make_async_remote_copy(
            src_ref=coarse_own,
            dst_ref=coarse_land.at[land],
            send_sem=far_send.at[place],
            recv_sem=far_recv.at[land],
            device_id={"mesh": (band + step_of(place) + n_mesh) & (n_mesh - 1)},
            device_id_type=MESH,
        )

    def far_start(k, carry):
        place = n_mesh - k
        far_copy(place, place_of(-step_of(place), n_mesh)).start()
        return carry

    lax.fori_loop(1, n_mesh, far_start, 0)
    latent_rows = lambda peer: latents.at[me]
    start_all(1, latent_rows, latents)
    coarse_land[0] = coarse_own[...]

    def relay(group, owner, peer):
        return pltpu.make_async_remote_copy(
            src_ref=coarse.at[owner, group],
            dst_ref=coarse.at[owner, group],
            send_sem=relay_send.at[group, peer],
            recv_sem=relay_recv.at[group, owner],
            device_id={"edge": peer},
            device_id_type=MESH,
        )

    def forward(group, owner):
        return pltpu.make_async_remote_copy(
            src_ref=coarse.at[owner, group],
            dst_ref=coarse.at[owner, group],
            send_sem=forward_send.at[group, owner],
            recv_sem=relay_recv.at[group, owner],
            device_id={"edge": me ^ 1},
            device_id_type=MESH,
        )

    def pass_on(group):
        def step(owner):
            relay(group, owner, owner).wait_recv()
            forward(group, owner).start()

        each_chip(step)

    for group in range(groups):
        for k in range(per_group):
            place = group * per_group + k
            if place > 0:
                far_copy(place, place).wait_recv()
        rows = [coarse_land[group * per_group + k].astype(F32) for k in range(per_group)]
        coarse[me, group] = jnp.concatenate(rows, axis=0).astype(BF16)
        each_chip(lambda peer: relay(group, me, peer).start())
        relay(group, me, me ^ 1).start()
        if group > 0:
            pass_on(group - 1)
    pass_on(groups - 1)

    edge_update[...] = nn(edge_outer[...], update_message[...]).astype(BF16)
    wait_all(1, latent_rows, latents)
    band_latent = latents[...].reshape(shard, width)
    recv_rows = nn(recv_pick[...], band_latent).astype(BF16)
    send_rows = nn(send_pick[:, 0:shard], band_latent)
    edge_term[...] += nn(recv_rows, edge_receiver[...])

    def far_finish(k, carry):
        far_copy(k, k).wait_send()
        return carry

    lax.fori_loop(1, n_mesh, far_finish, 0)
    for group in range(groups):

        def relay_finish(peer):
            relay(group, me, peer).wait_send()
            forward(group, peer).wait_send()
            forward(group, peer ^ 1).wait_recv()

        each_chip(relay_finish)
        relay(group, me, me ^ 1).wait_send()
        relay(group, me ^ 1, me).wait_recv()

    far_latent = coarse[...].reshape(n_edge * far_rows, width)
    send_rows = (send_rows + nn(send_pick[:, shard:], far_latent)).astype(BF16)
    pre = edge_term[...] + nn(send_rows, edge_sender[...])
    sigma = sigmoid(pre)
    act = (pre * sigma).astype(BF16)
    slope[...] = sigma * (1.0 + pre * (1.0 - sigma))
    proc_send[...] = nn(recv_drop[...], act).astype(BF16)
    proc_start, proc_finish = chip_all(2, proc_send, proc_land, own_rows)
    proc_start()
    state_term = nn(latents[me], update_state[...])
    proc_finish()
    proc_sum = jnp.sum(proc_land[...].astype(F32), axis=0)
    update_pre = nn(proc_sum.astype(BF16), edge_update[...]) + state_term
    sigma = sigmoid(update_pre)
    grad_pre = (back_out * (sigma * (1.0 + update_pre * (1.0 - sigma)))).astype(BF16)
    grads[me] = nt(grad_pre, edge_update[...]).astype(BF16)
    grad_rows = lambda peer: grads.at[me]
    start_all(3, grad_rows, grads)
    update_act = (update_pre * sigma).astype(BF16)
    mixed = latents[me].astype(F32) + nn(update_act, update_outer[...])
    output[...] = mixed.astype(BF16)
    grad_node = cotangent[...].astype(F32) + nt(grad_pre, update_state[...])
    wait_all(3, grad_rows, grads)
    band_grads = grads[...].reshape(shard, width)
    grad_edge = (nn(recv_pick[...], band_grads) * slope[...]).astype(BF16)
    back_coarse[...] = nn(send_drop[chip_rows:, :], grad_edge).astype(BF16)
    coarse_start, coarse_finish = chip_all(4, back_coarse, back_coarse_land, far_rows)
    coarse_start()
    to_sender = nn(send_drop[0:chip_rows, :], grad_edge).astype(BF16)
    to_receiver = nn(recv_drop[...], grad_edge).astype(BF16)
    back = nt(to_sender, edge_sender[...]) + nt(to_receiver, edge_receiver[...])
    back_band[...] = back.astype(BF16)
    band_start, band_finish = chip_all(5, back_band, back_band_land, own_rows)
    band_start()
    coarse_finish()
    far_total = jnp.sum(back_coarse_land[...].astype(F32), axis=0)

    def final_copy(place, land):
        return pltpu.make_async_remote_copy(
            src_ref=back_far.at[place],
            dst_ref=back_far_land.at[land],
            send_sem=final_send.at[place],
            recv_sem=final_recv.at[land],
            device_id={"mesh": (band + step_of(place) + n_mesh) & (n_mesh - 1)},
            device_id_type=MESH,
        )

    for place in range(1, n_mesh):
        back_far[place] = far_total[place * COARSE : (place + 1) * COARSE, :].astype(BF16)

    def final_start(k, carry):
        place = n_mesh - k
        final_copy(place, place_of(-step_of(place), n_mesh)).start()
        return carry

    lax.fori_loop(1, n_mesh, final_start, 0)
    band_finish()
    result = grad_node + jnp.sum(back_band_land[...].astype(F32), axis=0)

    def final_finish(k, carry):
        final_copy(k, k).wait_send()
        final_copy(k, k).wait_recv()
        return carry

    lax.fori_loop(1, n_mesh, final_finish, 0)
    arrived = back_far_land[1].astype(F32)
    for place in range(2, n_mesh):
        arrived = arrived + back_far_land[place].astype(F32)
    tail[...] = jnp.zeros_like(tail)
    tail[0:COARSE, :] = arrived
    gradient[...] = result + nt(tail[...].astype(BF16), edge_sender[...])


def finish_kernel(output, gradient, output_copy, gradient_copy):
    output_copy[...] = output[...]
    gradient_copy[...] = gradient[...]


def vmem():
    return pl.BlockSpec(memory_space=pltpu.VMEM)


def anywhere():
    return pl.BlockSpec(memory_space=pltpu.HBM)


def hbm(value):
    return pltpu.with_memory_space_constraint(value, pltpu.HBM)


def shards(
    n_mesh,
    n_edge,
    grid_input,
    mesh_position,
    encoder_senders,
    encoder_receivers,
    encoder_features,
    encoder_counts,
    mesh_senders,
    mesh_receivers,
    mesh_features,
    cotangent,
    grid_first,
    grid_second,
    encoder_inner,
    encoder_geometry,
    encoder_outer,
    node_first,
    node_position,
    node_second,
    edge_sender,
    edge_receiver,
    edge_geometry,
    edge_outer,
    update_message,
    update_state,
    update_outer,
):
    grid_rows, channels = grid_input.shape
    width = grid_second.shape[1]
    slots = encoder_senders.shape[0]
    blocks = slots // BLOCK
    own_rows = mesh_position.shape[1]
    shard = own_rows * n_edge
    edges = mesh_senders.shape[0]
    dma = pltpu.SemaphoreType.DMA
    packed, features, projected, pair_senders, pair_receivers, pair_features = pl.pallas_call(
        functools.partial(embed_kernel, n_edge),
        out_shape=(
            jax.ShapeDtypeStruct((n_edge, blocks, BLOCK), I32),
            jax.ShapeDtypeStruct((n_edge, 4, slots), BF16),
            jax.ShapeDtypeStruct((width, grid_rows), BF16),
            jax.ShapeDtypeStruct((2, 1, edges), I32),
            jax.ShapeDtypeStruct((2, 1, edges), I32),
            jax.ShapeDtypeStruct((2, 4, edges), BF16),
        ),
        in_specs=[pl.BlockSpec(memory_space=pltpu.SMEM)] + [anywhere()] * 10,
        out_specs=(vmem(),) * 6,
        scratch_shapes=[
            pltpu.VMEM((blocks, BLOCK), I32),
            pltpu.VMEM((blocks, BLOCK), I32),
            pltpu.VMEM((channels, grid_rows), BF16),
            pltpu.VMEM((channels, width), BF16),
            pltpu.VMEM((width, width), BF16),
            pltpu.VMEM((width, width), BF16),
            dma((10,)),
            dma((n_edge,)),
            dma((n_edge,)),
            dma((n_edge,)),
            dma((n_edge,)),
            dma((3,)),
            dma((3,)),
        ],
        compiler_params=pltpu.CompilerParams(
            collective_id=0, has_side_effects=True, vmem_limit_bytes=12 << 20
        ),
    )(
        encoder_counts,
        hbm(encoder_senders.reshape(blocks, BLOCK)),
        hbm(encoder_receivers.reshape(blocks, BLOCK)),
        hbm(encoder_features),
        hbm(mesh_senders.reshape(1, edges)),
        hbm(mesh_receivers.reshape(1, edges)),
        hbm(mesh_features),
        hbm(grid_input.T),
        hbm(grid_first),
        hbm(grid_second),
        hbm(encoder_inner),
    )
    all_blocks = n_edge * blocks
    partial = pl.pallas_call(
        functools.partial(encode_kernel, n_edge, shard),
        out_shape=jax.ShapeDtypeStruct((shard, width), BF16),
        in_specs=[vmem()] * 3 + [anywhere()],
        out_specs=vmem(),
        scratch_shapes=[
            pltpu.VMEM((all_blocks, BLOCK), I32),
            pltpu.VMEM((8, all_blocks), I32),
            pltpu.SMEM((8, all_blocks), I32),
            pltpu.VMEM((8, n_edge * slots + STEP), F32),
            pltpu.VMEM((8, width), F32),
            pltpu.VMEM((4, width), BF16),
            pltpu.VMEM((shard, width), F32),
            dma(()),
            dma(()),
        ],
        compiler_params=pltpu.CompilerParams(vmem_limit_bytes=16 << 20),
    )(packed.reshape(all_blocks, BLOCK), features, projected, hbm(encoder_geometry))
    far_rows = n_mesh * COARSE
    groups = far_rows // own_rows
    table_rows = shard + n_edge * far_rows
    chips = n_edge // 2
    chip_rows = chips * own_rows
    weights = [
        encoder_outer,
        node_first,
        node_second,
        edge_sender,
        edge_receiver,
        edge_outer,
        update_message,
        update_state,
        update_outer,
    ]
    output, gradient = pl.pallas_call(
        functools.partial(process_kernel, n_mesh, n_edge),
        out_shape=(
            jax.ShapeDtypeStruct((own_rows, width), BF16),
            jax.ShapeDtypeStruct((own_rows, width), F32),
        ),
        in_specs=[vmem()] * 8 + [anywhere()] * 9,
        out_specs=(vmem(), vmem()),
        scratch_shapes=[pltpu.VMEM((width, width), BF16) for _ in weights]
        + [
            pltpu.VMEM((128, 128), F32),
            pltpu.VMEM((8, 2 * edges), F32),
            pltpu.VMEM((n_edge, own_rows, width), BF16),
            pltpu.VMEM((n_edge, own_rows, width), BF16),
            pltpu.VMEM((COARSE, width), BF16),
            pltpu.VMEM((n_mesh, COARSE, width), BF16),
            pltpu.VMEM((n_edge, groups, own_rows, width), BF16),
            pltpu.VMEM((2 * edges, table_rows), BF16),
            pltpu.VMEM((2 * edges, shard), BF16),
            pltpu.VMEM((chip_rows + chips * far_rows, 2 * edges), BF16),
            pltpu.VMEM((chip_rows, 2 * edges), BF16),
            pltpu.VMEM((2 * edges, width), F32),
            pltpu.VMEM((2 * edges, width), F32),
            pltpu.VMEM((chip_rows, width), BF16),
            pltpu.VMEM((chips, own_rows, width), BF16),
            pltpu.VMEM((n_edge, own_rows, width), BF16),
            pltpu.VMEM((chip_rows, width), BF16),
            pltpu.VMEM((chips, own_rows, width), BF16),
            pltpu.VMEM((chips * far_rows, width), BF16),
            pltpu.VMEM((chips, far_rows, width), BF16),
            pltpu.VMEM((n_mesh, COARSE, width), BF16),
            pltpu.VMEM((n_mesh, COARSE, width), BF16),
            pltpu.VMEM((own_rows, width), F32),
            pltpu.VMEM((width, width), BF16),
            pltpu.VMEM((width, width), BF16),
            dma((9,)),
            dma((6, n_edge)),
            dma((6, n_edge)),
            dma((n_mesh,)),
            dma((n_mesh,)),
            dma((groups, n_edge)),
            dma((groups, n_edge)),
            dma((groups, n_edge)),
            dma((n_mesh,)),
            dma((n_mesh,)),
        ],
        compiler_params=pltpu.CompilerParams(
            collective_id=1, has_side_effects=True, vmem_limit_bytes=28 << 20
        ),
    )(
        partial,
        mesh_position,
        pair_senders,
        pair_receivers,
        pair_features,
        cotangent,
        node_position,
        edge_geometry,
        *[hbm(weight) for weight in weights],
    )
    return pl.pallas_call(
        finish_kernel,
        out_shape=(
            jax.ShapeDtypeStruct((own_rows, width), BF16),
            jax.ShapeDtypeStruct((own_rows, width), F32),
        ),
        in_specs=[vmem()] * 2,
        out_specs=(vmem(), vmem()),
        compiler_params=pltpu.CompilerParams(vmem_limit_bytes=1 << 20),
    )(output, gradient)


def solution(mesh):
    banded = ("mesh", "edge")
    every = ("groups", "mesh", "edge")
    in_specs = (
        P(every, None),
        P(None, banded),
        P(banded),
        P(banded),
        P(None, banded),
        P(banded),
        P(banded),
        P(banded),
        P(None, banded),
        P(every, None),
    ) + (P(),) * 15
    return jax.shard_map(
        functools.partial(shards, mesh.shape["mesh"], mesh.shape["edge"]),
        mesh=mesh,
        in_specs=in_specs,
        out_specs=(P(every, None), P(every, None)),
        check_vma=False,
    )
```

```python
import functools

import jax
import jax.numpy as jnp
from jax import lax
from jax.experimental import pallas as pl
from jax.experimental.pallas import tpu as pltpu
from jax.sharding import PartitionSpec as P

BLOCK = 128
CHUNK_ROWS = 8
WINDOW = 256
STEP = 512
COARSE = 4
MESH = pl.DeviceIdType.MESH
F32 = jnp.float32
BF16 = jnp.bfloat16
I32 = jnp.int32


def bits(size):
    return size.bit_length() - 1


def nn(left, right):
    return jnp.dot(left, right, preferred_element_type=F32)


def nt(left, right):
    return lax.dot_general(left, right, (((1,), (1,)), ((), ())), preferred_element_type=F32)


def tn(left, right):
    return lax.dot_general(left, right, (((0,), (0,)), ((), ())), preferred_element_type=F32)


def tt(left, right):
    return lax.dot_general(left, right, (((0,), (1,)), ((), ())), preferred_element_type=F32)


def sigmoid(values):
    return 0.5 + 0.5 * jnp.tanh(0.5 * values)


def layer_norm(values):
    centred = values - jnp.mean(values, axis=-1, keepdims=True)
    variance = jnp.mean(centred * centred, axis=-1, keepdims=True)
    return centred * lax.rsqrt(variance + 1e-05)


def iota(shape, dim):
    return lax.broadcasted_iota(I32, shape, dim)


def one_hot(hits):
    return jnp.where(hits, 1.0, 0.0).astype(BF16)


def greet(axis, count):
    me = lax.axis_index(axis)
    barrier = pltpu.get_barrier_semaphore()

    def signal(k, carry):
        pl.semaphore_signal(
            barrier, inc=1, device_id={axis: lax.rem(me + k, count)}, device_id_type=MESH
        )
        return carry

    lax.fori_loop(1, count, signal, 0)


def each_peer(axis, count, action):
    me = lax.axis_index(axis)

    def step(k, carry):
        action(me, lax.rem(me + k, count))
        return carry

    lax.fori_loop(1, count, step, 0)


def embed_kernel(
    n_edge,
    count,
    senders,
    receivers,
    features,
    mesh_senders,
    mesh_receivers,
    mesh_features,
    grid_input,
    first,
    second,
    inner,
    packed_all,
    features_all,
    projected,
    pair_senders,
    pair_receivers,
    pair_features,
    senders_v,
    receivers_v,
    rows_v,
    first_v,
    second_v,
    inner_v,
    load_sem,
    send_a,
    send_b,
    recv_a,
    recv_b,
    pair_send,
    pair_recv,
):
    me = lax.axis_index("edge")
    band = lax.axis_index("mesh")
    core = me & 1
    loads = [
        pltpu.make_async_copy(src, dst, load_sem.at[k])
        for k, (src, dst) in enumerate(
            [
                (senders, senders_v),
                (receivers, receivers_v),
                (features, features_all.at[me]),
                (mesh_senders, pair_senders.at[core]),
                (mesh_receivers, pair_receivers.at[core]),
                (mesh_features, pair_features.at[core]),
                (grid_input, rows_v),
                (first, first_v),
                (second, second_v),
                (inner, inner_v),
            ]
        )
    ]
    for load in loads:
        load.start()
    greet("edge", n_edge)
    blocks = senders.shape[0]
    rows = grid_input.shape[1]
    shard = packed_shard(n_edge)
    loads[0].wait()
    loads[1].wait()
    low = senders_v[...] - band * (rows * n_edge)
    near = receivers_v[...] - band * shard
    live = iota((blocks, BLOCK), 0) < count[0]
    packed_all[me] = jnp.where(live, low * shard + near, -1)
    for load in loads[2:6]:
        load.wait()
    pl.semaphore_wait(pltpu.get_barrier_semaphore(), n_edge - 1)

    def copy_packed(owner, peer, sem):
        return pltpu.make_async_remote_copy(
            src_ref=packed_all.at[owner],
            dst_ref=packed_all.at[owner],
            send_sem=send_a.at[sem],
            recv_sem=recv_a.at[owner],
            device_id={"edge": peer},
            device_id_type=MESH,
        )

    def copy_features(owner, peer, sem):
        return pltpu.make_async_remote_copy(
            src_ref=features_all.at[owner],
            dst_ref=features_all.at[owner],
            send_sem=send_b.at[sem],
            recv_sem=recv_b.at[owner],
            device_id={"edge": peer},
            device_id_type=MESH,
        )

    def send(own, peer):
        copy_packed(own, peer, peer).start()
        copy_features(own, peer, peer).start()

    each_peer("edge", n_edge, send)

    def copy_pair(ref, slot, k):
        return pltpu.make_async_remote_copy(
            src_ref=ref.at[slot],
            dst_ref=ref.at[slot],
            send_sem=pair_send.at[k],
            recv_sem=pair_recv.at[k],
            device_id={"edge": me ^ 1},
            device_id_type=MESH,
        )

    pairs = (pair_senders, pair_receivers, pair_features)
    for k, ref in enumerate(pairs):
        copy_pair(ref, core, k).start()
    loads[6].wait()
    loads[7].wait()
    hidden = tn(rows_v[...], first_v[...])
    hidden = (hidden * sigmoid(hidden)).astype(BF16)
    loads[8].wait()
    latent = layer_norm(nn(hidden, second_v[...])).astype(BF16)
    loads[9].wait()
    projected[...] = tt(inner_v[...], latent).astype(BF16)

    def arrive(own, peer):
        copy_packed(own, peer, peer).wait_send()
        copy_features(own, peer, peer).wait_send()
        copy_packed(peer, peer, peer).wait_recv()
        copy_features(peer, peer, peer).wait_recv()

    each_peer("edge", n_edge, arrive)
    for k, ref in enumerate(pairs):
        copy_pair(ref, core, k).wait_send()
        copy_pair(ref, core ^ 1, k).wait_recv()


def packed_shard(n_edge):
    return 16 * n_edge


def encode_kernel(
    n_edge,
    shard,
    packed,
    features,
    projected,
    geometry,
    partial,
    position,
    bounds_v,
    bounds,
    queue,
    geometry_v,
    geometry_w,
    total,
    sem,
    geometry_sem,
):
    me = lax.axis_index("edge")
    load = pltpu.make_async_copy(geometry, geometry_w, geometry_sem)
    load.start()
    blocks = packed.shape[0]
    per_device = blocks // n_edge
    grid_rows = projected.shape[1]
    width = projected.shape[0]
    shift = bits(shard)
    row_bits = bits(grid_rows)
    index = packed[...]
    own = (index >> (shift + row_bits)) == me
    own_b = one_hot(own)
    upper = one_hot(iota((BLOCK, BLOCK), 0) < iota((BLOCK, BLOCK), 1))
    before = one_hot(iota((blocks, blocks), 0) < iota((blocks, blocks), 1))
    lower = one_hot(iota((blocks, blocks), 0) > iota((blocks, blocks), 1))
    ones = jnp.ones((BLOCK, BLOCK), BF16)
    rank = nn(own_b, upper)
    per_block = nn(own_b, ones)
    base = nn(lower, per_block.astype(BF16))
    aligned = base.astype(I32) & -BLOCK
    position[...] = jnp.where(own, (rank + base).astype(I32), -1)
    totals = nt(jnp.ones((8, BLOCK), BF16), own_b)
    starts = nn(totals.astype(BF16), before)
    stops = starts + totals
    bounds_v[...] = jnp.where(iota((8, blocks), 0) == 0, starts, stops).astype(I32)
    copy = pltpu.make_async_copy(bounds_v, bounds, sem)
    copy.start()
    queue[...] = jnp.zeros_like(queue)
    total[...] = jnp.zeros_like(total)
    geometry_v[...] = jnp.zeros_like(geometry_v)
    chunk = CHUNK_ROWS * BLOCK
    per_chunk = per_device // CHUNK_ROWS

    def chunk_of(c, device, lane, row):
        code = packed[pl.ds(row, CHUNK_ROWS), :]
        where = position[pl.ds(row, CHUNK_ROWS), :]
        code_row = jnp.concatenate([code[k : k + 1, :] for k in range(CHUNK_ROWS)], axis=1)
        where_row = jnp.concatenate([where[k : k + 1, :] for k in range(CHUNK_ROWS)], axis=1)
        sender = (code_row >> shift) & (grid_rows - 1)
        parts = features[device, :, pl.ds(lane, chunk)].astype(F32)
        parts = jnp.concatenate([parts, jnp.zeros_like(parts)], axis=0)
        place = iota((8, chunk), 0)
        parts = jnp.where(place == 4, (sender >> 7).astype(F32), parts)
        parts = jnp.where(place == 5, (sender & 127).astype(F32), parts)
        parts = jnp.where(place == 6, ((code_row & (shard - 1)) + 1).astype(F32), parts)
        return parts.astype(BF16), where_row

    def sorted_window(parts, where_row):
        return nt(parts, one_hot(iota((WINDOW, chunk), 0) == where_row))

    def add(offset, window):
        queue[:, pl.ds(pl.multiple_of(offset, BLOCK), WINDOW)] += window

    windows = []
    for device in range(n_edge):
        c = device * per_chunk
        parts, where_row = chunk_of(c, device, 0, c * CHUNK_ROWS)
        from_row = aligned[c * CHUNK_ROWS : c * CHUNK_ROWS + 1, :]
        from_row = jnp.concatenate([from_row] * CHUNK_ROWS, axis=1)
        windows.append(sorted_window(parts, where_row - from_row))
    copy.wait()
    for device, window in enumerate(windows):
        add(bounds[0, device * per_chunk * CHUNK_ROWS] & -BLOCK, window)

    def sort_chunk(c, carry):
        first = bounds[0, c * CHUNK_ROWS]
        last = bounds[1, c * CHUNK_ROWS + CHUNK_ROWS - 1]
        part = c & (per_chunk - 1)
        skip = jnp.where(part == 0, WINDOW, 0)
        start = (first & -BLOCK) + skip

        @pl.when((last > first) & (last > start))
        def _():
            lane = pl.multiple_of(part * chunk, chunk)
            row = pl.multiple_of(c * CHUNK_ROWS, CHUNK_ROWS)
            parts, where_row = chunk_of(c, c >> bits(per_chunk), lane, row)

            def more(w, inner_carry):
                offset = start + w * WINDOW
                add(offset, sorted_window(parts, where_row - offset))
                return inner_carry

            lax.fori_loop(0, (last - start + WINDOW - 1) >> bits(WINDOW), more, 0)

        return carry

    lax.fori_loop(0, n_edge * per_chunk, sort_chunk, 0)
    load.wait()
    geometry_v[0:4, :] = geometry_w[...].astype(F32)
    found = bounds[1, blocks - 1]

    def encode(j, carry):
        offset = pl.multiple_of(j * STEP, STEP)
        parts = queue[:, pl.ds(offset, STEP)]
        sender = (parts[4:5, :] * 128.0 + parts[5:6, :]).astype(I32)
        target = parts[6:7, :].astype(I32)
        picks = one_hot(iota((grid_rows, STEP), 0) == sender)
        goes = one_hot(iota((shard, STEP), 0) + 1 == target)
        pre = nn(projected[...], picks)
        pre = pre + tn(geometry_v[...].astype(BF16), parts.astype(BF16))
        act = (pre * sigmoid(pre)).astype(BF16)
        total[...] += nt(goes, act)
        return carry

    lax.fori_loop(0, lax.div(found + STEP - 1, STEP), encode, 0)
    partial[...] = total[...].astype(BF16)


def step_of(place):
    return jnp.where((place & 1) == 1, (place + 1) >> 1, -(place >> 1))


def place_of(step, n_mesh):
    step = step & (n_mesh - 1)
    return jnp.where(
        step == 0, 0, jnp.where(step <= n_mesh // 2, 2 * step - 1, 2 * (n_mesh - step))
    )


def process_kernel(
    n_mesh,
    n_edge,
    partial,
    mesh_position,
    pair_senders,
    pair_receivers,
    pair_features,
    cotangent,
    node_position,
    geometry,
    w_encoder_outer,
    w_node_first,
    w_node_second,
    w_edge_sender,
    w_edge_receiver,
    w_edge_outer,
    w_update_message,
    w_update_state,
    w_update_outer,
    output,
    gradient,
    encoder_outer,
    node_first,
    node_second,
    edge_sender,
    edge_receiver,
    edge_outer,
    update_message,
    update_state,
    update_outer,
    padded,
    small,
    enc_land,
    latents,
    coarse_own,
    coarse_land,
    coarse,
    send_pick,
    recv_pick,
    send_drop,
    recv_drop,
    edge_term,
    slope,
    proc_send,
    proc_land,
    grads,
    back_band,
    back_band_land,
    back_coarse,
    back_coarse_land,
    back_far,
    back_far_land,
    tail,
    enc_node,
    edge_update,
    load_sem,
    send_sem,
    recv_sem,
    far_send,
    far_recv,
    relay_send,
    relay_recv,
    forward_send,
    final_send,
    final_recv,
    band_ready,
    far_ready,
):
    me = lax.axis_index("edge")
    band = lax.axis_index("mesh")
    own_rows = cotangent.shape[0]
    shard = own_rows * n_edge
    groups = n_mesh * COARSE // own_rows
    per_group = own_rows // COARSE
    edges = 2 * pair_senders.shape[2]
    far_rows = n_mesh * COARSE
    loads = [
        pltpu.make_async_copy(src, dst, load_sem.at[k])
        for k, (src, dst) in enumerate(
            [
                (w_encoder_outer, encoder_outer),
                (w_node_first, node_first),
                (w_node_second, node_second),
                (w_edge_sender, edge_sender),
                (w_edge_receiver, edge_receiver),
                (w_edge_outer, edge_outer),
                (w_update_message, update_message),
                (w_update_state, update_state),
                (w_update_outer, update_outer),
            ]
        )
    ]
    for load in loads:
        load.start()
    core = me & 1
    chip = me >> 1
    chips = n_edge // 2
    chip_rows = chips * own_rows
    barrier = pltpu.get_barrier_semaphore()

    def signal_band(k, carry):
        @pl.when((k > 0) | (core == 1))
        def _():
            pl.semaphore_signal(
                barrier,
                inc=1,
                device_id={"edge": 2 * ((chip + k) & (chips - 1))},
                device_id_type=MESH,
            )

        return carry

    def signal_far(k, carry):
        pl.semaphore_signal(
            barrier,
            inc=1,
            device_id={"mesh": (band + k) & (n_mesh - 1), "edge": me | 1},
            device_id_type=MESH,
        )
        return carry

    lax.fori_loop(0, chips, signal_band, 0)
    lax.fori_loop(1, n_mesh, signal_far, 0)

    @pl.when(core == 0)
    def _():
        pl.semaphore_wait(barrier, n_edge - 1)
        pl.semaphore_signal(band_ready, inc=1, device_id={"edge": me ^ 1}, device_id_type=MESH)

    @pl.when(core == 1)
    def _():
        pl.semaphore_wait(band_ready, 1)

    def each_chip(action):
        def step(k, carry):
            action(((chip + k) & (chips - 1)) * 2 + core)
            return carry

        lax.fori_loop(1, chips, step, 0)

    def to_peer(phase, src, dst, sem, land):
        def copy(peer):
            return pltpu.make_async_remote_copy(
                src_ref=src(peer),
                dst_ref=dst,
                send_sem=send_sem.at[phase, sem(peer)],
                recv_sem=recv_sem.at[phase, land],
                device_id={"edge": peer},
                device_id_type=MESH,
            )

        return copy

    def start_all(phase, src, dst):
        each_peer(
            "edge",
            n_edge,
            lambda own, peer: to_peer(phase, src, dst.at[own], lambda p: p, own)(peer).start(),
        )

    def wait_all(phase, src, dst):
        def finish(own, peer):
            to_peer(phase, src, dst.at[own], lambda p: p, own)(peer).wait_send()
            to_peer(phase, src, dst.at[peer], lambda p: p, peer)(peer).wait_recv()

        each_peer("edge", n_edge, finish)

    def chip_all(phase, ref, land, rows):
        def copy(peer, slot):
            start = pl.multiple_of((peer >> 1) * rows, rows)
            return pltpu.make_async_remote_copy(
                src_ref=ref.at[pl.ds(start, rows), :],
                dst_ref=land.at[slot],
                send_sem=send_sem.at[phase, peer],
                recv_sem=recv_sem.at[phase, slot],
                device_id={"edge": peer},
                device_id_type=MESH,
            )

        def start():
            each_chip(lambda peer: copy(peer, chip).start())
            land[chip] = ref[pl.ds(pl.multiple_of(chip * rows, rows), rows), :]

        def finish():
            each_chip(lambda peer: copy(peer, chip).wait_send())
            each_chip(lambda peer: copy(peer, peer >> 1).wait_recv())

        return start, finish

    def rows_of(ref):
        return lambda peer: ref.at[pl.ds(pl.multiple_of(peer * own_rows, own_rows), own_rows), :]

    own_slice = pl.ds(pl.multiple_of(me * own_rows, own_rows), own_rows)
    start_all(0, rows_of(partial), enc_land)
    enc_land[me] = partial[own_slice, :]

    padded[...] = jnp.zeros_like(padded)
    padded[0:3, 0:own_rows] = mesh_position[...].astype(F32)
    place_columns = padded[...].T
    position_term = jnp.zeros((own_rows, node_position.shape[1]), F32)
    for k in range(3):
        position_term += (
            place_columns[0:own_rows, k : k + 1] * node_position[k : k + 1, :].astype(F32)
        )

    sender = jnp.concatenate([pair_senders[0], pair_senders[1]], axis=1)
    receiver = jnp.concatenate([pair_receivers[0], pair_receivers[1]], axis=1)
    owner_band = sender >> bits(shard)
    near = owner_band == band
    owner_edge = (sender >> bits(own_rows)) & (n_edge - 1)
    far_place = place_of(owner_band - band, n_mesh)
    far_row = far_place * COARSE + (sender & (COARSE - 1))
    local = sender - band * shard
    pick = jnp.where(near, local, shard + owner_edge * far_rows + far_row)
    receiver = receiver - band * shard
    table_rows = shard + n_edge * far_rows

    def chip_row(row, owner):
        own_core = (owner & 1) == core
        return jnp.where(own_core, (owner >> 1) * own_rows + (row & (own_rows - 1)), -1)

    drop_near = jnp.where(near, chip_row(local, owner_edge), -1)
    drop_far = jnp.where((owner_edge & 1) == core, (owner_edge >> 1) * far_rows + far_row, -1)
    drop_far = jnp.where(near, -1, drop_far)
    drop_recv = chip_row(receiver, receiver >> bits(own_rows))
    send_drop[0:chip_rows, :] = one_hot(iota((chip_rows, edges), 0) == drop_near)
    send_drop[chip_rows:, :] = one_hot(iota((chips * far_rows, edges), 0) == drop_far)
    recv_drop[...] = one_hot(iota((chip_rows, edges), 0) == drop_recv)
    pick_columns = jnp.broadcast_to(pick.astype(F32), (128, edges)).T.astype(I32)
    recv_columns = jnp.broadcast_to(receiver.astype(F32), (128, edges)).T.astype(I32)
    lanes = iota((edges, 128), 1)
    for k in range(table_rows // 128):
        send_pick[:, k * 128 : (k + 1) * 128] = one_hot(lanes + k * 128 == pick_columns)
    for k in range(shard // 128):
        recv_pick[:, k * 128 : (k + 1) * 128] = one_hot(lanes + k * 128 == recv_columns)
    small[...] = jnp.zeros_like(small)
    half = edges // 2
    small[0:4, 0:half] = pair_features[0].astype(F32)
    small[0:4, half:edges] = pair_features[1].astype(F32)
    width = geometry.shape[1]
    padded_geometry = jnp.concatenate([geometry[...].astype(F32)] * 2, axis=0)
    padded_geometry = jnp.where(iota((8, width), 0) < 4, padded_geometry, 0.0)
    edge_term[...] = tn(small[...].astype(BF16), padded_geometry.astype(BF16))
    for load in loads:
        load.wait()
    back_out = nt(cotangent[...], update_outer[...])
    enc_node[...] = nn(encoder_outer[...], node_first[...]).astype(BF16)

    wait_all(0, rows_of(partial), enc_land)
    enc_sum = jnp.sum(enc_land[...].astype(F32), axis=0)
    hidden = nn(enc_sum.astype(BF16), enc_node[...]) + position_term
    hidden = (hidden * sigmoid(hidden)).astype(BF16)
    latent = layer_norm(nn(hidden, node_second[...])).astype(BF16)
    coarse_own[...] = latent[0:COARSE, :]
    latents[me] = latent

    latent_rows = lambda peer: latents.at[me]
    start_all(1, latent_rows, latents)

    def far_copy(place, land):
        return pltpu.make_async_remote_copy(
            src_ref=coarse_own,
            dst_ref=coarse_land.at[land],
            send_sem=far_send.at[place],
            recv_sem=far_recv.at[land],
            device_id={"mesh": (band + step_of(place) + n_mesh) & (n_mesh - 1)},
            device_id_type=MESH,
        )

    def far_start(k, carry):
        place = n_mesh - k
        far_copy(place, place_of(-step_of(place), n_mesh)).start()
        return carry

    @pl.when(core == 1)
    def _():
        pl.semaphore_wait(barrier, 2 * (n_mesh - 1))
        pl.semaphore_signal(far_ready, inc=1, device_id={"edge": me ^ 1}, device_id_type=MESH)

    @pl.when(core == 0)
    def _():
        pl.semaphore_wait(far_ready, 1)

    lax.fori_loop(1, n_mesh, far_start, 0)
    coarse_land[0] = coarse_own[...]

    def relay(group, owner, peer):
        return pltpu.make_async_remote_copy(
            src_ref=coarse.at[owner, group],
            dst_ref=coarse.at[owner, group],
            send_sem=relay_send.at[group, peer],
            recv_sem=relay_recv.at[group, owner],
            device_id={"edge": peer},
            device_id_type=MESH,
        )

    def forward(group, owner):
        return pltpu.make_async_remote_copy(
            src_ref=coarse.at[owner, group],
            dst_ref=coarse.at[owner, group],
            send_sem=forward_send.at[group, owner],
            recv_sem=relay_recv.at[group, owner],
            device_id={"edge": me ^ 1},
            device_id_type=MESH,
        )

    def pass_on(group):
        def step(owner):
            relay(group, owner, owner).wait_recv()
            forward(group, owner).start()

        each_chip(step)

    for group in range(groups):
        for k in range(per_group):
            place = group * per_group + k
            if place > 0:
                far_copy(place, place).wait_recv()
        rows = [coarse_land[group * per_group + k].astype(F32) for k in range(per_group)]
        coarse[me, group] = jnp.concatenate(rows, axis=0).astype(BF16)
        each_chip(lambda peer: relay(group, me, peer).start())
        relay(group, me, me ^ 1).start()
        if group > 0:
            pass_on(group - 1)
    pass_on(groups - 1)

    edge_update[...] = nn(edge_outer[...], update_message[...]).astype(BF16)
    wait_all(1, latent_rows, latents)
    band_latent = latents[...].reshape(shard, width)
    recv_rows = nn(recv_pick[...], band_latent).astype(BF16)
    send_rows = nn(send_pick[:, 0:shard], band_latent)
    edge_term[...] += nn(recv_rows, edge_receiver[...])

    def far_finish(k, carry):
        far_copy(k, k).wait_send()
        return carry

    lax.fori_loop(1, n_mesh, far_finish, 0)
    for group in range(groups):

        def relay_finish(peer):
            relay(group, me, peer).wait_send()
            forward(group, peer).wait_send()
            forward(group, peer ^ 1).wait_recv()

        each_chip(relay_finish)
        relay(group, me, me ^ 1).wait_send()
        relay(group, me ^ 1, me).wait_recv()

    far_latent = coarse[...].reshape(n_edge * far_rows, width)
    send_rows = (send_rows + nn(send_pick[:, shard:], far_latent)).astype(BF16)
    pre = edge_term[...] + nn(send_rows, edge_sender[...])
    sigma = sigmoid(pre)
    act = (pre * sigma).astype(BF16)
    slope[...] = sigma * (1.0 + pre * (1.0 - sigma))
    proc_send[...] = nn(recv_drop[...], act).astype(BF16)
    proc_start, proc_finish = chip_all(2, proc_send, proc_land, own_rows)
    proc_start()
    state_term = nn(latents[me], update_state[...])
    proc_finish()
    proc_sum = jnp.sum(proc_land[...].astype(F32), axis=0)
    update_pre = nn(proc_sum.astype(BF16), edge_update[...]) + state_term
    sigma = sigmoid(update_pre)
    grad_pre = (back_out * (sigma * (1.0 + update_pre * (1.0 - sigma)))).astype(BF16)
    grads[me] = nt(grad_pre, edge_update[...]).astype(BF16)
    grad_rows = lambda peer: grads.at[me]
    start_all(3, grad_rows, grads)
    update_act = (update_pre * sigma).astype(BF16)
    mixed = latents[me].astype(F32) + nn(update_act, update_outer[...])
    output[...] = mixed.astype(BF16)
    grad_node = cotangent[...].astype(F32) + nt(grad_pre, update_state[...])
    wait_all(3, grad_rows, grads)
    band_grads = grads[...].reshape(shard, width)
    grad_edge = (nn(recv_pick[...], band_grads) * slope[...]).astype(BF16)
    back_coarse[...] = nn(send_drop[chip_rows:, :], grad_edge).astype(BF16)
    coarse_start, coarse_finish = chip_all(4, back_coarse, back_coarse_land, far_rows)
    coarse_start()
    to_sender = nn(send_drop[0:chip_rows, :], grad_edge).astype(BF16)
    to_receiver = nn(recv_drop[...], grad_edge).astype(BF16)
    back = nt(to_sender, edge_sender[...]) + nt(to_receiver, edge_receiver[...])
    back_band[...] = back.astype(BF16)
    band_start, band_finish = chip_all(5, back_band, back_band_land, own_rows)
    band_start()
    coarse_finish()
    far_total = jnp.sum(back_coarse_land[...].astype(F32), axis=0)

    def final_copy(place, land):
        return pltpu.make_async_remote_copy(
            src_ref=back_far.at[place],
            dst_ref=back_far_land.at[land],
            send_sem=final_send.at[place],
            recv_sem=final_recv.at[land],
            device_id={"mesh": (band + step_of(place) + n_mesh) & (n_mesh - 1)},
            device_id_type=MESH,
        )

    for place in range(1, n_mesh):
        back_far[place] = far_total[place * COARSE : (place + 1) * COARSE, :].astype(BF16)

    def final_start(k, carry):
        place = n_mesh - k
        final_copy(place, place_of(-step_of(place), n_mesh)).start()
        return carry

    lax.fori_loop(1, n_mesh, final_start, 0)
    band_finish()
    result = grad_node + jnp.sum(back_band_land[...].astype(F32), axis=0)

    def final_finish(k, carry):
        final_copy(k, k).wait_send()
        final_copy(k, k).wait_recv()
        return carry

    lax.fori_loop(1, n_mesh, final_finish, 0)
    arrived = back_far_land[1].astype(F32)
    for place in range(2, n_mesh):
        arrived = arrived + back_far_land[place].astype(F32)
    tail[...] = jnp.zeros_like(tail)
    tail[0:COARSE, :] = arrived
    gradient[...] = result + nt(tail[...].astype(BF16), edge_sender[...])


def finish_kernel(output, gradient, output_copy, gradient_copy):
    output_copy[...] = output[...]
    gradient_copy[...] = gradient[...]


def vmem():
    return pl.BlockSpec(memory_space=pltpu.VMEM)


def anywhere():
    return pl.BlockSpec(memory_space=pltpu.HBM)


def hbm(value):
    return pltpu.with_memory_space_constraint(value, pltpu.HBM)


def shards(
    n_mesh,
    n_edge,
    grid_input,
    mesh_position,
    encoder_senders,
    encoder_receivers,
    encoder_features,
    encoder_counts,
    mesh_senders,
    mesh_receivers,
    mesh_features,
    cotangent,
    grid_first,
    grid_second,
    encoder_inner,
    encoder_geometry,
    encoder_outer,
    node_first,
    node_position,
    node_second,
    edge_sender,
    edge_receiver,
    edge_geometry,
    edge_outer,
    update_message,
    update_state,
    update_outer,
):
    grid_rows, channels = grid_input.shape
    width = grid_second.shape[1]
    slots = encoder_senders.shape[0]
    blocks = slots // BLOCK
    own_rows = mesh_position.shape[1]
    shard = own_rows * n_edge
    edges = mesh_senders.shape[0]
    dma = pltpu.SemaphoreType.DMA
    packed, features, projected, pair_senders, pair_receivers, pair_features = pl.pallas_call(
        functools.partial(embed_kernel, n_edge),
        out_shape=(
            jax.ShapeDtypeStruct((n_edge, blocks, BLOCK), I32),
            jax.ShapeDtypeStruct((n_edge, 4, slots), BF16),
            jax.ShapeDtypeStruct((width, grid_rows), BF16),
            jax.ShapeDtypeStruct((2, 1, edges), I32),
            jax.ShapeDtypeStruct((2, 1, edges), I32),
            jax.ShapeDtypeStruct((2, 4, edges), BF16),
        ),
        in_specs=[pl.BlockSpec(memory_space=pltpu.SMEM)] + [anywhere()] * 10,
        out_specs=(vmem(),) * 6,
        scratch_shapes=[
            pltpu.VMEM((blocks, BLOCK), I32),
            pltpu.VMEM((blocks, BLOCK), I32),
            pltpu.VMEM((channels, grid_rows), BF16),
            pltpu.VMEM((channels, width), BF16),
            pltpu.VMEM((width, width), BF16),
            pltpu.VMEM((width, width), BF16),
            dma((10,)),
            dma((n_edge,)),
            dma((n_edge,)),
            dma((n_edge,)),
            dma((n_edge,)),
            dma((3,)),
            dma((3,)),
        ],
        compiler_params=pltpu.CompilerParams(
            collective_id=0, has_side_effects=True, vmem_limit_bytes=12 << 20
        ),
    )(
        encoder_counts,
        hbm(encoder_senders.reshape(blocks, BLOCK)),
        hbm(encoder_receivers.reshape(blocks, BLOCK)),
        hbm(encoder_features),
        hbm(mesh_senders.reshape(1, edges)),
        hbm(mesh_receivers.reshape(1, edges)),
        hbm(mesh_features),
        hbm(grid_input.T),
        hbm(grid_first),
        hbm(grid_second),
        hbm(encoder_inner),
    )
    all_blocks = n_edge * blocks
    partial = pl.pallas_call(
        functools.partial(encode_kernel, n_edge, shard),
        out_shape=jax.ShapeDtypeStruct((shard, width), BF16),
        in_specs=[vmem()] * 3 + [anywhere()],
        out_specs=vmem(),
        scratch_shapes=[
            pltpu.VMEM((all_blocks, BLOCK), I32),
            pltpu.VMEM((8, all_blocks), I32),
            pltpu.SMEM((8, all_blocks), I32),
            pltpu.VMEM((8, n_edge * slots + STEP), F32),
            pltpu.VMEM((8, width), F32),
            pltpu.VMEM((4, width), BF16),
            pltpu.VMEM((shard, width), F32),
            dma(()),
            dma(()),
        ],
        compiler_params=pltpu.CompilerParams(vmem_limit_bytes=16 << 20),
    )(packed.reshape(all_blocks, BLOCK), features, projected, hbm(encoder_geometry))
    far_rows = n_mesh * COARSE
    groups = far_rows // own_rows
    table_rows = shard + n_edge * far_rows
    chips = n_edge // 2
    chip_rows = chips * own_rows
    weights = [
        encoder_outer,
        node_first,
        node_second,
        edge_sender,
        edge_receiver,
        edge_outer,
        update_message,
        update_state,
        update_outer,
    ]
    output, gradient = pl.pallas_call(
        functools.partial(process_kernel, n_mesh, n_edge),
        out_shape=(
            jax.ShapeDtypeStruct((own_rows, width), BF16),
            jax.ShapeDtypeStruct((own_rows, width), F32),
        ),
        in_specs=[vmem()] * 8 + [anywhere()] * 9,
        out_specs=(vmem(), vmem()),
        scratch_shapes=[pltpu.VMEM((width, width), BF16) for _ in weights]
        + [
            pltpu.VMEM((128, 128), F32),
            pltpu.VMEM((8, 2 * edges), F32),
            pltpu.VMEM((n_edge, own_rows, width), BF16),
            pltpu.VMEM((n_edge, own_rows, width), BF16),
            pltpu.VMEM((COARSE, width), BF16),
            pltpu.VMEM((n_mesh, COARSE, width), BF16),
            pltpu.VMEM((n_edge, groups, own_rows, width), BF16),
            pltpu.VMEM((2 * edges, table_rows), BF16),
            pltpu.VMEM((2 * edges, shard), BF16),
            pltpu.VMEM((chip_rows + chips * far_rows, 2 * edges), BF16),
            pltpu.VMEM((chip_rows, 2 * edges), BF16),
            pltpu.VMEM((2 * edges, width), F32),
            pltpu.VMEM((2 * edges, width), F32),
            pltpu.VMEM((chip_rows, width), BF16),
            pltpu.VMEM((chips, own_rows, width), BF16),
            pltpu.VMEM((n_edge, own_rows, width), BF16),
            pltpu.VMEM((chip_rows, width), BF16),
            pltpu.VMEM((chips, own_rows, width), BF16),
            pltpu.VMEM((chips * far_rows, width), BF16),
            pltpu.VMEM((chips, far_rows, width), BF16),
            pltpu.VMEM((n_mesh, COARSE, width), BF16),
            pltpu.VMEM((n_mesh, COARSE, width), BF16),
            pltpu.VMEM((own_rows, width), F32),
            pltpu.VMEM((width, width), BF16),
            pltpu.VMEM((width, width), BF16),
            dma((9,)),
            dma((6, n_edge)),
            dma((6, n_edge)),
            dma((n_mesh,)),
            dma((n_mesh,)),
            dma((groups, n_edge)),
            dma((groups, n_edge)),
            dma((groups, n_edge)),
            dma((n_mesh,)),
            dma((n_mesh,)),
            pltpu.SemaphoreType.REGULAR,
            pltpu.SemaphoreType.REGULAR,
        ],
        compiler_params=pltpu.CompilerParams(
            collective_id=1, has_side_effects=True, vmem_limit_bytes=28 << 20
        ),
    )(
        partial,
        mesh_position,
        pair_senders,
        pair_receivers,
        pair_features,
        cotangent,
        node_position,
        edge_geometry,
        *[hbm(weight) for weight in weights],
    )
    return pl.pallas_call(
        finish_kernel,
        out_shape=(
            jax.ShapeDtypeStruct((own_rows, width), BF16),
            jax.ShapeDtypeStruct((own_rows, width), F32),
        ),
        in_specs=[vmem()] * 2,
        out_specs=(vmem(), vmem()),
        compiler_params=pltpu.CompilerParams(vmem_limit_bytes=1 << 20),
    )(output, gradient)


def solution(mesh):
    banded = ("mesh", "edge")
    every = ("groups", "mesh", "edge")
    in_specs = (
        P(every, None),
        P(None, banded),
        P(banded),
        P(banded),
        P(None, banded),
        P(banded),
        P(banded),
        P(banded),
        P(None, banded),
        P(every, None),
    ) + (P(),) * 15
    return jax.shard_map(
        functools.partial(shards, mesh.shape["mesh"], mesh.shape["edge"]),
        mesh=mesh,
        in_specs=in_specs,
        out_specs=(P(every, None), P(every, None)),
        check_vma=False,
    )
```

```python
import functools

import jax
import jax.numpy as jnp
from jax import lax
from jax.experimental import pallas as pl
from jax.experimental.pallas import tpu as pltpu
from jax.sharding import PartitionSpec as P

BLOCK = 128
CHUNK_ROWS = 8
WINDOW = 256
STEP = 512
COARSE = 4
MESH = pl.DeviceIdType.MESH
F32 = jnp.float32
BF16 = jnp.bfloat16
I32 = jnp.int32


def bits(size):
    return size.bit_length() - 1


def nn(left, right):
    return jnp.dot(left, right, preferred_element_type=F32)


def nt(left, right):
    return lax.dot_general(left, right, (((1,), (1,)), ((), ())), preferred_element_type=F32)


def tn(left, right):
    return lax.dot_general(left, right, (((0,), (0,)), ((), ())), preferred_element_type=F32)


def tt(left, right):
    return lax.dot_general(left, right, (((0,), (1,)), ((), ())), preferred_element_type=F32)


def sigmoid(values):
    return 0.5 + 0.5 * jnp.tanh(0.5 * values)


def layer_norm(values):
    centred = values - jnp.mean(values, axis=-1, keepdims=True)
    variance = jnp.mean(centred * centred, axis=-1, keepdims=True)
    return centred * lax.rsqrt(variance + 1e-05)


def iota(shape, dim):
    return lax.broadcasted_iota(I32, shape, dim)


def one_hot(hits):
    return jnp.where(hits, 1.0, 0.0).astype(BF16)


def greet(axis, count):
    me = lax.axis_index(axis)
    barrier = pltpu.get_barrier_semaphore()

    def signal(k, carry):
        pl.semaphore_signal(
            barrier, inc=1, device_id={axis: lax.rem(me + k, count)}, device_id_type=MESH
        )
        return carry

    lax.fori_loop(1, count, signal, 0)


def chip_steps(chips):
    return sorted(range(1, chips), key=lambda step: -min(step, chips - step))


def each_chip(n_edge, action):
    me = lax.axis_index("edge")
    chips = n_edge // 2
    for step in chip_steps(chips):
        action((me + 2 * step) & (n_edge - 1))


def each_peer(n_edge, action):
    me = lax.axis_index("edge")
    chips = n_edge // 2
    for step in chip_steps(chips):
        peer = (me + 2 * step) & (n_edge - 1)
        action(me, peer)
        action(me, peer ^ 1)
    action(me, me ^ 1)


def embed_kernel(
    n_edge,
    count,
    senders,
    receivers,
    features,
    mesh_senders,
    mesh_receivers,
    mesh_features,
    grid_input,
    first,
    second,
    inner,
    packed_all,
    features_all,
    projected,
    pair_senders,
    pair_receivers,
    pair_features,
    senders_v,
    receivers_v,
    rows_v,
    first_v,
    second_v,
    inner_v,
    load_sem,
    send_a,
    send_b,
    recv_a,
    recv_b,
    pair_send,
    pair_recv,
):
    me = lax.axis_index("edge")
    band = lax.axis_index("mesh")
    core = me & 1
    loads = [
        pltpu.make_async_copy(src, dst, load_sem.at[k])
        for k, (src, dst) in enumerate(
            [
                (senders, senders_v),
                (receivers, receivers_v),
                (features, features_all.at[me]),
                (mesh_senders, pair_senders.at[core]),
                (mesh_receivers, pair_receivers.at[core]),
                (mesh_features, pair_features.at[core]),
                (grid_input, rows_v),
                (first, first_v),
                (second, second_v),
                (inner, inner_v),
            ]
        )
    ]
    for load in loads:
        load.start()
    greet("edge", n_edge)
    blocks = senders.shape[0]
    rows = grid_input.shape[1]
    shard = packed_shard(n_edge)
    loads[0].wait()
    loads[1].wait()
    low = senders_v[...] - band * (rows * n_edge)
    near = receivers_v[...] - band * shard
    live = iota((blocks, BLOCK), 0) < count[0]
    packed_all[me] = jnp.where(live, low * shard + near, -1)
    for load in loads[2:6]:
        load.wait()
    pl.semaphore_wait(pltpu.get_barrier_semaphore(), n_edge - 1)

    def copy_packed(owner, peer, sem):
        return pltpu.make_async_remote_copy(
            src_ref=packed_all.at[owner],
            dst_ref=packed_all.at[owner],
            send_sem=send_a.at[sem],
            recv_sem=recv_a.at[owner],
            device_id={"edge": peer},
            device_id_type=MESH,
        )

    def copy_features(owner, peer, sem):
        return pltpu.make_async_remote_copy(
            src_ref=features_all.at[owner],
            dst_ref=features_all.at[owner],
            send_sem=send_b.at[sem],
            recv_sem=recv_b.at[owner],
            device_id={"edge": peer},
            device_id_type=MESH,
        )

    def send(own, peer):
        copy_packed(own, peer, peer).start()
        copy_features(own, peer, peer).start()

    each_peer(n_edge, send)

    def copy_pair(ref, slot, k):
        return pltpu.make_async_remote_copy(
            src_ref=ref.at[slot],
            dst_ref=ref.at[slot],
            send_sem=pair_send.at[k],
            recv_sem=pair_recv.at[k],
            device_id={"edge": me ^ 1},
            device_id_type=MESH,
        )

    pairs = (pair_senders, pair_receivers, pair_features)
    for k, ref in enumerate(pairs):
        copy_pair(ref, core, k).start()
    loads[6].wait()
    loads[7].wait()
    hidden = tn(rows_v[...], first_v[...])
    hidden = (hidden * sigmoid(hidden)).astype(BF16)
    loads[8].wait()
    latent = layer_norm(nn(hidden, second_v[...])).astype(BF16)
    loads[9].wait()
    projected[...] = tt(inner_v[...], latent).astype(BF16)

    def arrive(own, peer):
        copy_packed(peer, peer, peer).wait_recv()
        copy_features(peer, peer, peer).wait_recv()

    def sent(own, peer):
        copy_packed(own, peer, peer).wait_send()
        copy_features(own, peer, peer).wait_send()

    each_peer(n_edge, arrive)
    each_peer(n_edge, sent)
    for k, ref in enumerate(pairs):
        copy_pair(ref, core, k).wait_send()
        copy_pair(ref, core ^ 1, k).wait_recv()


def packed_shard(n_edge):
    return 16 * n_edge


def encode_kernel(
    n_edge,
    shard,
    packed,
    features,
    projected,
    geometry,
    partial,
    position,
    bounds_v,
    bounds,
    queue,
    geometry_v,
    geometry_w,
    total,
    sem,
    geometry_sem,
):
    me = lax.axis_index("edge")
    load = pltpu.make_async_copy(geometry, geometry_w, geometry_sem)
    load.start()
    blocks = packed.shape[0]
    per_device = blocks // n_edge
    grid_rows = projected.shape[1]
    width = projected.shape[0]
    shift = bits(shard)
    row_bits = bits(grid_rows)
    index = packed[...]
    own = (index >> (shift + row_bits)) == me
    own_b = one_hot(own)
    upper = one_hot(iota((BLOCK, BLOCK), 0) < iota((BLOCK, BLOCK), 1))
    before = one_hot(iota((blocks, blocks), 0) < iota((blocks, blocks), 1))
    lower = one_hot(iota((blocks, blocks), 0) > iota((blocks, blocks), 1))
    ones = jnp.ones((BLOCK, BLOCK), BF16)
    rank = nn(own_b, upper)
    per_block = nn(own_b, ones)
    base = nn(lower, per_block.astype(BF16))
    aligned = base.astype(I32) & -BLOCK
    position[...] = jnp.where(own, (rank + base).astype(I32), -1)
    totals = nt(jnp.ones((8, BLOCK), BF16), own_b)
    starts = nn(totals.astype(BF16), before)
    stops = starts + totals
    bounds_v[...] = jnp.where(iota((8, blocks), 0) == 0, starts, stops).astype(I32)
    copy = pltpu.make_async_copy(bounds_v, bounds, sem)
    copy.start()
    queue[...] = jnp.zeros_like(queue)
    total[...] = jnp.zeros_like(total)
    geometry_v[...] = jnp.zeros_like(geometry_v)
    chunk = CHUNK_ROWS * BLOCK
    per_chunk = per_device // CHUNK_ROWS

    def chunk_of(c, device, lane, row):
        code = packed[pl.ds(row, CHUNK_ROWS), :]
        where = position[pl.ds(row, CHUNK_ROWS), :]
        code_row = jnp.concatenate([code[k : k + 1, :] for k in range(CHUNK_ROWS)], axis=1)
        where_row = jnp.concatenate([where[k : k + 1, :] for k in range(CHUNK_ROWS)], axis=1)
        sender = (code_row >> shift) & (grid_rows - 1)
        parts = features[device, :, pl.ds(lane, chunk)].astype(F32)
        parts = jnp.concatenate([parts, jnp.zeros_like(parts)], axis=0)
        place = iota((8, chunk), 0)
        parts = jnp.where(place == 4, (sender >> 7).astype(F32), parts)
        parts = jnp.where(place == 5, (sender & 127).astype(F32), parts)
        parts = jnp.where(place == 6, ((code_row & (shard - 1)) + 1).astype(F32), parts)
        return parts.astype(BF16), where_row

    def sorted_window(parts, where_row):
        return nt(parts, one_hot(iota((WINDOW, chunk), 0) == where_row))

    def add(offset, window):
        queue[:, pl.ds(pl.multiple_of(offset, BLOCK), WINDOW)] += window

    windows = []
    for device in range(n_edge):
        c = device * per_chunk
        parts, where_row = chunk_of(c, device, 0, c * CHUNK_ROWS)
        from_row = aligned[c * CHUNK_ROWS : c * CHUNK_ROWS + 1, :]
        from_row = jnp.concatenate([from_row] * CHUNK_ROWS, axis=1)
        windows.append(sorted_window(parts, where_row - from_row))
    copy.wait()
    for device, window in enumerate(windows):
        add(bounds[0, device * per_chunk * CHUNK_ROWS] & -BLOCK, window)

    def sort_chunk(c, carry):
        first = bounds[0, c * CHUNK_ROWS]
        last = bounds[1, c * CHUNK_ROWS + CHUNK_ROWS - 1]
        part = c & (per_chunk - 1)
        skip = jnp.where(part == 0, WINDOW, 0)
        start = (first & -BLOCK) + skip

        @pl.when((last > first) & (last > start))
        def _():
            lane = pl.multiple_of(part * chunk, chunk)
            row = pl.multiple_of(c * CHUNK_ROWS, CHUNK_ROWS)
            parts, where_row = chunk_of(c, c >> bits(per_chunk), lane, row)

            def more(w, inner_carry):
                offset = start + w * WINDOW
                add(offset, sorted_window(parts, where_row - offset))
                return inner_carry

            lax.fori_loop(0, (last - start + WINDOW - 1) >> bits(WINDOW), more, 0)

        return carry

    lax.fori_loop(0, n_edge * per_chunk, sort_chunk, 0)
    load.wait()
    geometry_v[0:4, :] = geometry_w[...].astype(F32)
    found = bounds[1, blocks - 1]

    def encode(j, carry):
        offset = pl.multiple_of(j * STEP, STEP)
        parts = queue[:, pl.ds(offset, STEP)]
        sender = (parts[4:5, :] * 128.0 + parts[5:6, :]).astype(I32)
        target = parts[6:7, :].astype(I32)
        picks = one_hot(iota((grid_rows, STEP), 0) == sender)
        goes = one_hot(iota((shard, STEP), 0) + 1 == target)
        pre = nn(projected[...], picks)
        pre = pre + tn(geometry_v[...].astype(BF16), parts.astype(BF16))
        act = (pre * sigmoid(pre)).astype(BF16)
        total[...] += nt(goes, act)
        return carry

    lax.fori_loop(0, lax.div(found + STEP - 1, STEP), encode, 0)
    partial[...] = total[...].astype(BF16)


def step_of(place):
    return jnp.where((place & 1) == 1, (place + 1) >> 1, -(place >> 1))


def place_of(step, n_mesh):
    step = step & (n_mesh - 1)
    return jnp.where(
        step == 0, 0, jnp.where(step <= n_mesh // 2, 2 * step - 1, 2 * (n_mesh - step))
    )


def process_kernel(
    n_mesh,
    n_edge,
    partial,
    mesh_position,
    pair_senders,
    pair_receivers,
    pair_features,
    cotangent,
    node_position,
    geometry,
    w_encoder_outer,
    w_node_first,
    w_node_second,
    w_edge_sender,
    w_edge_receiver,
    w_edge_outer,
    w_update_message,
    w_update_state,
    w_update_outer,
    output,
    gradient,
    encoder_outer,
    node_first,
    node_second,
    edge_sender,
    edge_receiver,
    edge_outer,
    update_message,
    update_state,
    update_outer,
    padded,
    small,
    enc_land,
    latents,
    coarse_own,
    coarse_land,
    coarse,
    send_pick,
    recv_pick,
    send_drop,
    recv_drop,
    edge_term,
    slope,
    proc_send,
    proc_land,
    grads,
    back_band,
    back_band_land,
    back_coarse,
    back_coarse_land,
    back_far,
    back_far_land,
    tail,
    enc_node,
    edge_update,
    load_sem,
    send_sem,
    recv_sem,
    far_send,
    far_recv,
    relay_send,
    relay_recv,
    forward_send,
    final_send,
    final_recv,
    band_ready,
    far_ready,
):
    me = lax.axis_index("edge")
    band = lax.axis_index("mesh")
    own_rows = cotangent.shape[0]
    shard = own_rows * n_edge
    groups = n_mesh * COARSE // own_rows
    per_group = own_rows // COARSE
    edges = 2 * pair_senders.shape[2]
    far_rows = n_mesh * COARSE
    loads = [
        pltpu.make_async_copy(src, dst, load_sem.at[k])
        for k, (src, dst) in enumerate(
            [
                (w_encoder_outer, encoder_outer),
                (w_node_first, node_first),
                (w_node_second, node_second),
                (w_edge_sender, edge_sender),
                (w_edge_receiver, edge_receiver),
                (w_edge_outer, edge_outer),
                (w_update_message, update_message),
                (w_update_state, update_state),
                (w_update_outer, update_outer),
            ]
        )
    ]
    for load in loads:
        load.start()
    core = me & 1
    chip = me >> 1
    chips = n_edge // 2
    chip_rows = chips * own_rows
    barrier = pltpu.get_barrier_semaphore()

    def signal_band(k, carry):
        @pl.when((k > 0) | (core == 1))
        def _():
            pl.semaphore_signal(
                barrier,
                inc=1,
                device_id={"edge": 2 * ((chip + k) & (chips - 1))},
                device_id_type=MESH,
            )

        return carry

    def signal_far(k, carry):
        pl.semaphore_signal(
            barrier,
            inc=1,
            device_id={"mesh": (band + k) & (n_mesh - 1), "edge": me | 1},
            device_id_type=MESH,
        )
        return carry

    lax.fori_loop(0, chips, signal_band, 0)
    lax.fori_loop(1, n_mesh, signal_far, 0)

    @pl.when(core == 0)
    def _():
        pl.semaphore_wait(barrier, n_edge - 1)
        pl.semaphore_signal(band_ready, inc=1, device_id={"edge": me ^ 1}, device_id_type=MESH)

    @pl.when(core == 1)
    def _():
        pl.semaphore_wait(band_ready, 1)

    unsent = []

    def to_peer(phase, src, dst, sem, land):
        def copy(peer):
            return pltpu.make_async_remote_copy(
                src_ref=src(peer),
                dst_ref=dst,
                send_sem=send_sem.at[phase, sem(peer)],
                recv_sem=recv_sem.at[phase, land],
                device_id={"edge": peer},
                device_id_type=MESH,
            )

        return copy

    def start_all(phase, src, dst):
        def start(own, peer):
            copy = to_peer(phase, src, dst.at[own], lambda p: p, own)(peer)
            copy.start()
            unsent.append(copy)

        each_peer(n_edge, start)

    def wait_all(phase, src, dst):
        each_peer(
            n_edge,
            lambda own, peer: to_peer(phase, src, dst.at[peer], lambda p: p, peer)(peer).wait_recv(),
        )

    def chip_all(phase, ref, land, rows):
        def copy(peer, slot):
            start = pl.multiple_of((peer >> 1) * rows, rows)
            return pltpu.make_async_remote_copy(
                src_ref=ref.at[pl.ds(start, rows), :],
                dst_ref=land.at[slot],
                send_sem=send_sem.at[phase, peer],
                recv_sem=recv_sem.at[phase, slot],
                device_id={"edge": peer},
                device_id_type=MESH,
            )

        def begin(peer):
            sent = copy(peer, chip)
            sent.start()
            unsent.append(sent)

        def start():
            each_chip(n_edge, begin)
            land[chip] = ref[pl.ds(pl.multiple_of(chip * rows, rows), rows), :]

        def finish():
            each_chip(n_edge, lambda peer: copy(peer, peer >> 1).wait_recv())

        return start, finish

    def rows_of(ref):
        return lambda peer: ref.at[pl.ds(pl.multiple_of(peer * own_rows, own_rows), own_rows), :]

    own_slice = pl.ds(pl.multiple_of(me * own_rows, own_rows), own_rows)
    start_all(0, rows_of(partial), enc_land)
    enc_land[me] = partial[own_slice, :]

    padded[...] = jnp.zeros_like(padded)
    padded[0:3, 0:own_rows] = mesh_position[...].astype(F32)
    place_columns = padded[...].T
    position_term = jnp.zeros((own_rows, node_position.shape[1]), F32)
    for k in range(3):
        position_term += (
            place_columns[0:own_rows, k : k + 1] * node_position[k : k + 1, :].astype(F32)
        )

    sender = jnp.concatenate([pair_senders[0], pair_senders[1]], axis=1)
    receiver = jnp.concatenate([pair_receivers[0], pair_receivers[1]], axis=1)
    owner_band = sender >> bits(shard)
    near = owner_band == band
    owner_edge = (sender >> bits(own_rows)) & (n_edge - 1)
    far_place = place_of(owner_band - band, n_mesh)
    far_row = far_place * COARSE + (sender & (COARSE - 1))
    local = sender - band * shard
    place_low = far_place & (per_group - 1)
    far_slot = ((far_place >> bits(per_group)) * n_edge + owner_edge) * own_rows
    far_slot = far_slot + place_low * COARSE + (sender & (COARSE - 1))
    pick = jnp.where(near, local, shard + far_slot)
    receiver = receiver - band * shard
    table_rows = shard + n_edge * far_rows

    def chip_row(row, owner):
        own_core = (owner & 1) == core
        return jnp.where(own_core, (owner >> 1) * own_rows + (row & (own_rows - 1)), -1)

    drop_near = jnp.where(near, chip_row(local, owner_edge), -1)
    drop_far = jnp.where((owner_edge & 1) == core, (owner_edge >> 1) * far_rows + far_row, -1)
    drop_far = jnp.where(near, -1, drop_far)
    drop_recv = chip_row(receiver, receiver >> bits(own_rows))
    send_drop[0:chip_rows, :] = one_hot(iota((chip_rows, edges), 0) == drop_near)
    send_drop[chip_rows:, :] = one_hot(iota((chips * far_rows, edges), 0) == drop_far)
    recv_drop[...] = one_hot(iota((chip_rows, edges), 0) == drop_recv)
    pick_columns = jnp.broadcast_to(pick.astype(F32), (128, edges)).T.astype(I32)
    recv_columns = jnp.broadcast_to(receiver.astype(F32), (128, edges)).T.astype(I32)
    lanes = iota((edges, 128), 1)
    for k in range(table_rows // 128):
        send_pick[:, k * 128 : (k + 1) * 128] = one_hot(lanes + k * 128 == pick_columns)
    for k in range(shard // 128):
        recv_pick[:, k * 128 : (k + 1) * 128] = one_hot(lanes + k * 128 == recv_columns)
    small[...] = jnp.zeros_like(small)
    half = edges // 2
    small[0:4, 0:half] = pair_features[0].astype(F32)
    small[0:4, half:edges] = pair_features[1].astype(F32)
    width = geometry.shape[1]
    padded_geometry = jnp.concatenate([geometry[...].astype(F32)] * 2, axis=0)
    padded_geometry = jnp.where(iota((8, width), 0) < 4, padded_geometry, 0.0)
    edge_term[...] = tn(small[...].astype(BF16), padded_geometry.astype(BF16))
    for load in loads:
        load.wait()
    back_out = nt(cotangent[...], update_outer[...])
    enc_node[...] = nn(encoder_outer[...], node_first[...]).astype(BF16)

    wait_all(0, rows_of(partial), enc_land)
    enc_sum = jnp.sum(enc_land[...].astype(F32), axis=0)
    hidden = nn(enc_sum.astype(BF16), enc_node[...]) + position_term
    hidden = (hidden * sigmoid(hidden)).astype(BF16)
    latent = layer_norm(nn(hidden, node_second[...])).astype(BF16)
    coarse_own[...] = latent[0:COARSE, :]
    latents[me] = latent

    latent_rows = lambda peer: latents.at[me]
    start_all(1, latent_rows, latents)

    def far_copy(place, land):
        return pltpu.make_async_remote_copy(
            src_ref=coarse_own,
            dst_ref=coarse_land.at[land],
            send_sem=far_send.at[place],
            recv_sem=far_recv.at[land],
            device_id={"mesh": (band + step_of(place) + n_mesh) & (n_mesh - 1)},
            device_id_type=MESH,
        )

    def far_start(k, carry):
        place = n_mesh - k
        far_copy(place, place_of(-step_of(place), n_mesh)).start()
        return carry

    @pl.when(core == 1)
    def _():
        pl.semaphore_wait(barrier, 2 * (n_mesh - 1))
        pl.semaphore_signal(far_ready, inc=1, device_id={"edge": me ^ 1}, device_id_type=MESH)

    @pl.when(core == 0)
    def _():
        pl.semaphore_wait(far_ready, 1)

    lax.fori_loop(1, n_mesh, far_start, 0)
    coarse_land[0] = coarse_own[...]

    def relay(group, owner, peer):
        return pltpu.make_async_remote_copy(
            src_ref=coarse.at[owner, group],
            dst_ref=coarse.at[owner, group],
            send_sem=relay_send.at[group, peer],
            recv_sem=relay_recv.at[group, owner],
            device_id={"edge": peer},
            device_id_type=MESH,
        )

    def forward(group, owner):
        return pltpu.make_async_remote_copy(
            src_ref=coarse.at[owner, group],
            dst_ref=coarse.at[owner, group],
            send_sem=forward_send.at[group, owner],
            recv_sem=relay_recv.at[group, owner],
            device_id={"edge": me ^ 1},
            device_id_type=MESH,
        )

    def pass_on(group):
        def step(owner):
            relay(group, owner, owner).wait_recv()
            copy = forward(group, owner)
            copy.start()
            unsent.append(copy)

        each_chip(n_edge, step)

    def relay_start(group, peer):
        copy = relay(group, me, peer)
        copy.start()
        unsent.append(copy)

    def take_in(group):
        each_chip(n_edge, lambda peer: forward(group, peer ^ 1).wait_recv())
        relay(group, me ^ 1, me).wait_recv()
        table = coarse[:, group].reshape(n_edge * own_rows, width)
        table = nn(table, edge_sender[...]).astype(BF16)
        first = shard + group * n_edge * own_rows
        edge_term[...] += nn(send_pick[:, first : first + n_edge * own_rows], table)

    edge_update[...] = nn(edge_outer[...], update_message[...]).astype(BF16)
    wait_all(1, latent_rows, latents)
    band_latent = latents[...].reshape(shard, width)
    near_table = nn(band_latent, edge_sender[...]).astype(BF16)
    recv_table = nn(band_latent, edge_receiver[...]).astype(BF16)
    edge_term[...] += nn(send_pick[:, 0:shard], near_table) + nn(recv_pick[...], recv_table)

    for group in range(groups):
        for k in range(per_group):
            place = group * per_group + k
            if place > 0:
                far_copy(place, place).wait_recv()
        rows = [coarse_land[group * per_group + k].astype(F32) for k in range(per_group)]
        coarse[me, group] = jnp.concatenate(rows, axis=0).astype(BF16)
        each_chip(n_edge, lambda peer: relay_start(group, peer))
        relay_start(group, me ^ 1)
        if group > 0:
            pass_on(group - 1)
        if group > 1:
            take_in(group - 2)
    if groups > 1:
        take_in(groups - 2)
    pass_on(groups - 1)
    take_in(groups - 1)
    pre = edge_term[...]
    sigma = sigmoid(pre)
    act = (pre * sigma).astype(BF16)
    slope[...] = sigma * (1.0 + pre * (1.0 - sigma))
    proc_send[...] = nn(recv_drop[...], act).astype(BF16)
    proc_start, proc_finish = chip_all(2, proc_send, proc_land, own_rows)
    proc_start()
    state_term = nn(latents[me], update_state[...])
    proc_finish()
    proc_sum = jnp.sum(proc_land[...].astype(F32), axis=0)
    update_pre = nn(proc_sum.astype(BF16), edge_update[...]) + state_term
    sigma = sigmoid(update_pre)
    grad_pre = (back_out * (sigma * (1.0 + update_pre * (1.0 - sigma)))).astype(BF16)
    grads[me] = nt(grad_pre, edge_update[...]).astype(BF16)
    grad_rows = lambda peer: grads.at[me]
    start_all(3, grad_rows, grads)
    update_act = (update_pre * sigma).astype(BF16)
    mixed = latents[me].astype(F32) + nn(update_act, update_outer[...])
    output[...] = mixed.astype(BF16)
    grad_node = cotangent[...].astype(F32) + nt(grad_pre, update_state[...])
    wait_all(3, grad_rows, grads)
    band_grads = grads[...].reshape(shard, width)
    grad_edge = (nn(recv_pick[...], band_grads) * slope[...]).astype(BF16)
    back_coarse[...] = nn(send_drop[chip_rows:, :], grad_edge).astype(BF16)
    coarse_start, coarse_finish = chip_all(4, back_coarse, back_coarse_land, far_rows)
    coarse_start()
    to_sender = nn(send_drop[0:chip_rows, :], grad_edge).astype(BF16)
    to_receiver = nn(recv_drop[...], grad_edge).astype(BF16)
    back = nt(to_sender, edge_sender[...]) + nt(to_receiver, edge_receiver[...])
    back_band[...] = back.astype(BF16)
    band_start, band_finish = chip_all(5, back_band, back_band_land, own_rows)
    band_start()
    coarse_finish()
    far_total = jnp.sum(back_coarse_land[...].astype(F32), axis=0)

    def final_copy(place, land):
        return pltpu.make_async_remote_copy(
            src_ref=back_far.at[place],
            dst_ref=back_far_land.at[land],
            send_sem=final_send.at[place],
            recv_sem=final_recv.at[land],
            device_id={"mesh": (band + step_of(place) + n_mesh) & (n_mesh - 1)},
            device_id_type=MESH,
        )

    for place in range(1, n_mesh):
        back_far[place] = far_total[place * COARSE : (place + 1) * COARSE, :].astype(BF16)

    def final_start(k, carry):
        place = n_mesh - k
        final_copy(place, place_of(-step_of(place), n_mesh)).start()
        return carry

    lax.fori_loop(1, n_mesh, final_start, 0)
    band_finish()
    result = grad_node + jnp.sum(back_band_land[...].astype(F32), axis=0)

    def final_finish(k, carry):
        final_copy(k, k).wait_recv()
        return carry

    lax.fori_loop(1, n_mesh, final_finish, 0)
    arrived = back_far_land[1].astype(F32)
    for place in range(2, n_mesh):
        arrived = arrived + back_far_land[place].astype(F32)
    tail[...] = jnp.zeros_like(tail)
    tail[0:COARSE, :] = arrived
    gradient[...] = result + nt(tail[...].astype(BF16), edge_sender[...])

    def far_sent(k, carry):
        far_copy(k, k).wait_send()
        final_copy(k, k).wait_send()
        return carry

    lax.fori_loop(1, n_mesh, far_sent, 0)
    for copy in unsent:
        copy.wait_send()


def finish_kernel(output, gradient, output_copy, gradient_copy):
    output_copy[...] = output[...]
    gradient_copy[...] = gradient[...]


def vmem():
    return pl.BlockSpec(memory_space=pltpu.VMEM)


def anywhere():
    return pl.BlockSpec(memory_space=pltpu.HBM)


def hbm(value):
    return pltpu.with_memory_space_constraint(value, pltpu.HBM)


def shards(
    n_mesh,
    n_edge,
    grid_input,
    mesh_position,
    encoder_senders,
    encoder_receivers,
    encoder_features,
    encoder_counts,
    mesh_senders,
    mesh_receivers,
    mesh_features,
    cotangent,
    grid_first,
    grid_second,
    encoder_inner,
    encoder_geometry,
    encoder_outer,
    node_first,
    node_position,
    node_second,
    edge_sender,
    edge_receiver,
    edge_geometry,
    edge_outer,
    update_message,
    update_state,
    update_outer,
):
    grid_rows, channels = grid_input.shape
    width = grid_second.shape[1]
    slots = encoder_senders.shape[0]
    blocks = slots // BLOCK
    own_rows = mesh_position.shape[1]
    shard = own_rows * n_edge
    edges = mesh_senders.shape[0]
    dma = pltpu.SemaphoreType.DMA
    packed, features, projected, pair_senders, pair_receivers, pair_features = pl.pallas_call(
        functools.partial(embed_kernel, n_edge),
        out_shape=(
            jax.ShapeDtypeStruct((n_edge, blocks, BLOCK), I32),
            jax.ShapeDtypeStruct((n_edge, 4, slots), BF16),
            jax.ShapeDtypeStruct((width, grid_rows), BF16),
            jax.ShapeDtypeStruct((2, 1, edges), I32),
            jax.ShapeDtypeStruct((2, 1, edges), I32),
            jax.ShapeDtypeStruct((2, 4, edges), BF16),
        ),
        in_specs=[pl.BlockSpec(memory_space=pltpu.SMEM)] + [anywhere()] * 10,
        out_specs=(vmem(),) * 6,
        scratch_shapes=[
            pltpu.VMEM((blocks, BLOCK), I32),
            pltpu.VMEM((blocks, BLOCK), I32),
            pltpu.VMEM((channels, grid_rows), BF16),
            pltpu.VMEM((channels, width), BF16),
            pltpu.VMEM((width, width), BF16),
            pltpu.VMEM((width, width), BF16),
            dma((10,)),
            dma((n_edge,)),
            dma((n_edge,)),
            dma((n_edge,)),
            dma((n_edge,)),
            dma((3,)),
            dma((3,)),
        ],
        compiler_params=pltpu.CompilerParams(
            collective_id=0, has_side_effects=True, vmem_limit_bytes=12 << 20
        ),
    )(
        encoder_counts,
        hbm(encoder_senders.reshape(blocks, BLOCK)),
        hbm(encoder_receivers.reshape(blocks, BLOCK)),
        hbm(encoder_features),
        hbm(mesh_senders.reshape(1, edges)),
        hbm(mesh_receivers.reshape(1, edges)),
        hbm(mesh_features),
        hbm(grid_input.T),
        hbm(grid_first),
        hbm(grid_second),
        hbm(encoder_inner),
    )
    all_blocks = n_edge * blocks
    partial = pl.pallas_call(
        functools.partial(encode_kernel, n_edge, shard),
        out_shape=jax.ShapeDtypeStruct((shard, width), BF16),
        in_specs=[vmem()] * 3 + [anywhere()],
        out_specs=vmem(),
        scratch_shapes=[
            pltpu.VMEM((all_blocks, BLOCK), I32),
            pltpu.VMEM((8, all_blocks), I32),
            pltpu.SMEM((8, all_blocks), I32),
            pltpu.VMEM((8, n_edge * slots + STEP), F32),
            pltpu.VMEM((8, width), F32),
            pltpu.VMEM((4, width), BF16),
            pltpu.VMEM((shard, width), F32),
            dma(()),
            dma(()),
        ],
        compiler_params=pltpu.CompilerParams(vmem_limit_bytes=16 << 20),
    )(packed.reshape(all_blocks, BLOCK), features, projected, hbm(encoder_geometry))
    far_rows = n_mesh * COARSE
    groups = far_rows // own_rows
    table_rows = shard + n_edge * far_rows
    chips = n_edge // 2
    chip_rows = chips * own_rows
    weights = [
        encoder_outer,
        node_first,
        node_second,
        edge_sender,
        edge_receiver,
        edge_outer,
        update_message,
        update_state,
        update_outer,
    ]
    output, gradient = pl.pallas_call(
        functools.partial(process_kernel, n_mesh, n_edge),
        out_shape=(
            jax.ShapeDtypeStruct((own_rows, width), BF16),
            jax.ShapeDtypeStruct((own_rows, width), F32),
        ),
        in_specs=[vmem()] * 8 + [anywhere()] * 9,
        out_specs=(vmem(), vmem()),
        scratch_shapes=[pltpu.VMEM((width, width), BF16) for _ in weights]
        + [
            pltpu.VMEM((128, 128), F32),
            pltpu.VMEM((8, 2 * edges), F32),
            pltpu.VMEM((n_edge, own_rows, width), BF16),
            pltpu.VMEM((n_edge, own_rows, width), BF16),
            pltpu.VMEM((COARSE, width), BF16),
            pltpu.VMEM((n_mesh, COARSE, width), BF16),
            pltpu.VMEM((n_edge, groups, own_rows, width), BF16),
            pltpu.VMEM((2 * edges, table_rows), BF16),
            pltpu.VMEM((2 * edges, shard), BF16),
            pltpu.VMEM((chip_rows + chips * far_rows, 2 * edges), BF16),
            pltpu.VMEM((chip_rows, 2 * edges), BF16),
            pltpu.VMEM((2 * edges, width), F32),
            pltpu.VMEM((2 * edges, width), F32),
            pltpu.VMEM((chip_rows, width), BF16),
            pltpu.VMEM((chips, own_rows, width), BF16),
            pltpu.VMEM((n_edge, own_rows, width), BF16),
            pltpu.VMEM((chip_rows, width), BF16),
            pltpu.VMEM((chips, own_rows, width), BF16),
            pltpu.VMEM((chips * far_rows, width), BF16),
            pltpu.VMEM((chips, far_rows, width), BF16),
            pltpu.VMEM((n_mesh, COARSE, width), BF16),
            pltpu.VMEM((n_mesh, COARSE, width), BF16),
            pltpu.VMEM((own_rows, width), F32),
            pltpu.VMEM((width, width), BF16),
            pltpu.VMEM((width, width), BF16),
            dma((9,)),
            dma((6, n_edge)),
            dma((6, n_edge)),
            dma((n_mesh,)),
            dma((n_mesh,)),
            dma((groups, n_edge)),
            dma((groups, n_edge)),
            dma((groups, n_edge)),
            dma((n_mesh,)),
            dma((n_mesh,)),
            pltpu.SemaphoreType.REGULAR,
            pltpu.SemaphoreType.REGULAR,
        ],
        compiler_params=pltpu.CompilerParams(
            collective_id=1, has_side_effects=True, vmem_limit_bytes=28 << 20
        ),
    )(
        partial,
        mesh_position,
        pair_senders,
        pair_receivers,
        pair_features,
        cotangent,
        node_position,
        edge_geometry,
        *[hbm(weight) for weight in weights],
    )
    return pl.pallas_call(
        finish_kernel,
        out_shape=(
            jax.ShapeDtypeStruct((own_rows, width), BF16),
            jax.ShapeDtypeStruct((own_rows, width), F32),
        ),
        in_specs=[vmem()] * 2,
        out_specs=(vmem(), vmem()),
        compiler_params=pltpu.CompilerParams(vmem_limit_bytes=1 << 20),
    )(output, gradient)


def solution(mesh):
    banded = ("mesh", "edge")
    every = ("groups", "mesh", "edge")
    in_specs = (
        P(every, None),
        P(None, banded),
        P(banded),
        P(banded),
        P(None, banded),
        P(banded),
        P(banded),
        P(banded),
        P(None, banded),
        P(every, None),
    ) + (P(),) * 15
    return jax.shard_map(
        functools.partial(shards, mesh.shape["mesh"], mesh.shape["edge"]),
        mesh=mesh,
        in_specs=in_specs,
        out_specs=(P(every, None), P(every, None)),
        check_vma=False,
    )
```

```python
import functools

import jax
import jax.numpy as jnp
from jax import lax
from jax.experimental import pallas as pl
from jax.experimental.pallas import tpu as pltpu
from jax.sharding import PartitionSpec as P

BLOCK = 128
CHUNK_ROWS = 8
WINDOW = 256
STEP = 512
COARSE = 4
MESH = pl.DeviceIdType.MESH
F32 = jnp.float32
BF16 = jnp.bfloat16
I32 = jnp.int32


def bits(size):
    return size.bit_length() - 1


def nn(left, right):
    return jnp.dot(left, right, preferred_element_type=F32)


def nt(left, right):
    return lax.dot_general(left, right, (((1,), (1,)), ((), ())), preferred_element_type=F32)


def tn(left, right):
    return lax.dot_general(left, right, (((0,), (0,)), ((), ())), preferred_element_type=F32)


def tt(left, right):
    return lax.dot_general(left, right, (((0,), (1,)), ((), ())), preferred_element_type=F32)


def sigmoid(values):
    return 0.5 + 0.5 * jnp.tanh(0.5 * values)


def layer_norm(values):
    centred = values - jnp.mean(values, axis=-1, keepdims=True)
    variance = jnp.mean(centred * centred, axis=-1, keepdims=True)
    return centred * lax.rsqrt(variance + 1e-05)


def iota(shape, dim):
    return lax.broadcasted_iota(I32, shape, dim)


def one_hot(hits):
    return jnp.where(hits, 1.0, 0.0).astype(BF16)


def greet(axis, count):
    me = lax.axis_index(axis)
    barrier = pltpu.get_barrier_semaphore()

    def signal(k, carry):
        pl.semaphore_signal(
            barrier, inc=1, device_id={axis: lax.rem(me + k, count)}, device_id_type=MESH
        )
        return carry

    lax.fori_loop(1, count, signal, 0)


def chip_steps(chips):
    return sorted(range(1, chips), key=lambda step: -min(step, chips - step))


def each_chip(n_edge, action):
    me = lax.axis_index("edge")
    chips = n_edge // 2
    for step in chip_steps(chips):
        action((me + 2 * step) & (n_edge - 1))


def each_peer(n_edge, action):
    me = lax.axis_index("edge")
    chips = n_edge // 2
    for step in chip_steps(chips):
        peer = (me + 2 * step) & (n_edge - 1)
        action(me, peer)
        action(me, peer ^ 1)
    action(me, me ^ 1)


def embed_kernel(
    n_edge,
    count,
    senders,
    receivers,
    features,
    mesh_senders,
    mesh_receivers,
    mesh_features,
    grid_input,
    first,
    second,
    inner,
    packed_all,
    features_all,
    projected,
    band_senders,
    band_receivers,
    band_features,
    senders_v,
    receivers_v,
    rows_v,
    first_v,
    second_v,
    inner_v,
    load_sem,
    send_sem,
    recv_sem,
):
    me = lax.axis_index("edge")
    band = lax.axis_index("mesh")
    loads = [
        pltpu.make_async_copy(src, dst, load_sem.at[k])
        for k, (src, dst) in enumerate(
            [
                (senders, senders_v),
                (receivers, receivers_v),
                (features, features_all.at[me]),
                (mesh_senders, band_senders.at[me]),
                (mesh_receivers, band_receivers.at[me]),
                (mesh_features, band_features.at[me]),
                (grid_input, rows_v),
                (first, first_v),
                (second, second_v),
                (inner, inner_v),
            ]
        )
    ]
    for load in loads:
        load.start()
    greet("edge", n_edge)
    blocks = senders.shape[0]
    rows = grid_input.shape[1]
    shard = packed_shard(n_edge)
    loads[0].wait()
    loads[1].wait()
    low = senders_v[...] - band * (rows * n_edge)
    near = receivers_v[...] - band * shard
    live = iota((blocks, BLOCK), 0) < count[0]
    packed_all[me] = jnp.where(live, low * shard + near, -1)
    for load in loads[2:6]:
        load.wait()
    pl.semaphore_wait(pltpu.get_barrier_semaphore(), n_edge - 1)

    tables = (packed_all, features_all, band_senders, band_receivers, band_features)

    def copy(k, owner, peer):
        return pltpu.make_async_remote_copy(
            src_ref=tables[k].at[owner],
            dst_ref=tables[k].at[owner],
            send_sem=send_sem.at[k, peer],
            recv_sem=recv_sem.at[k, owner],
            device_id={"edge": peer},
            device_id_type=MESH,
        )

    for group in ((0, 1), (2, 3, 4)):
        each_peer(n_edge, lambda own, peer: [copy(k, own, peer).start() for k in group])
    loads[6].wait()
    loads[7].wait()
    hidden = tn(rows_v[...], first_v[...])
    hidden = (hidden * sigmoid(hidden)).astype(BF16)
    loads[8].wait()
    latent = layer_norm(nn(hidden, second_v[...])).astype(BF16)
    loads[9].wait()
    projected[...] = tt(inner_v[...], latent).astype(BF16)

    def arrive(own, peer):
        for k in range(len(tables)):
            copy(k, peer, peer).wait_recv()

    def sent(own, peer):
        for k in range(len(tables)):
            copy(k, own, peer).wait_send()

    each_peer(n_edge, arrive)
    each_peer(n_edge, sent)


def packed_shard(n_edge):
    return 16 * n_edge


def encode_kernel(
    n_edge,
    shard,
    packed,
    features,
    projected,
    geometry,
    partial,
    position,
    bounds_v,
    bounds,
    queue,
    geometry_v,
    geometry_w,
    total,
    sem,
    geometry_sem,
):
    me = lax.axis_index("edge")
    load = pltpu.make_async_copy(geometry, geometry_w, geometry_sem)
    load.start()
    blocks = packed.shape[0]
    per_device = blocks // n_edge
    grid_rows = projected.shape[1]
    width = projected.shape[0]
    shift = bits(shard)
    row_bits = bits(grid_rows)
    index = packed[...]
    own = (index >> (shift + row_bits)) == me
    own_b = one_hot(own)
    upper = one_hot(iota((BLOCK, BLOCK), 0) < iota((BLOCK, BLOCK), 1))
    before = one_hot(iota((blocks, blocks), 0) < iota((blocks, blocks), 1))
    lower = one_hot(iota((blocks, blocks), 0) > iota((blocks, blocks), 1))
    ones = jnp.ones((BLOCK, BLOCK), BF16)
    rank = nn(own_b, upper)
    per_block = nn(own_b, ones)
    base = nn(lower, per_block.astype(BF16))
    aligned = base.astype(I32) & -BLOCK
    position[...] = jnp.where(own, (rank + base).astype(I32), -1)
    totals = nt(jnp.ones((8, BLOCK), BF16), own_b)
    starts = nn(totals.astype(BF16), before)
    stops = starts + totals
    bounds_v[...] = jnp.where(iota((8, blocks), 0) == 0, starts, stops).astype(I32)
    copy = pltpu.make_async_copy(bounds_v, bounds, sem)
    copy.start()
    queue[...] = jnp.zeros_like(queue)
    total[...] = jnp.zeros_like(total)
    geometry_v[...] = jnp.zeros_like(geometry_v)
    chunk = CHUNK_ROWS * BLOCK
    per_chunk = per_device // CHUNK_ROWS

    def chunk_of(c, device, lane, row):
        code = packed[pl.ds(row, CHUNK_ROWS), :]
        where = position[pl.ds(row, CHUNK_ROWS), :]
        code_row = jnp.concatenate([code[k : k + 1, :] for k in range(CHUNK_ROWS)], axis=1)
        where_row = jnp.concatenate([where[k : k + 1, :] for k in range(CHUNK_ROWS)], axis=1)
        sender = (code_row >> shift) & (grid_rows - 1)
        parts = features[device, :, pl.ds(lane, chunk)].astype(F32)
        parts = jnp.concatenate([parts, jnp.zeros_like(parts)], axis=0)
        place = iota((8, chunk), 0)
        parts = jnp.where(place == 4, (sender >> 7).astype(F32), parts)
        parts = jnp.where(place == 5, (sender & 127).astype(F32), parts)
        parts = jnp.where(place == 6, ((code_row & (shard - 1)) + 1).astype(F32), parts)
        return parts.astype(BF16), where_row

    def sorted_window(parts, where_row):
        return nt(parts, one_hot(iota((WINDOW, chunk), 0) == where_row))

    def add(offset, window):
        queue[:, pl.ds(pl.multiple_of(offset, BLOCK), WINDOW)] += window

    windows = []
    for device in range(n_edge):
        c = device * per_chunk
        parts, where_row = chunk_of(c, device, 0, c * CHUNK_ROWS)
        from_row = aligned[c * CHUNK_ROWS : c * CHUNK_ROWS + 1, :]
        from_row = jnp.concatenate([from_row] * CHUNK_ROWS, axis=1)
        windows.append(sorted_window(parts, where_row - from_row))
    copy.wait()
    for device, window in enumerate(windows):
        add(bounds[0, device * per_chunk * CHUNK_ROWS] & -BLOCK, window)

    def sort_chunk(c, carry):
        first = bounds[0, c * CHUNK_ROWS]
        last = bounds[1, c * CHUNK_ROWS + CHUNK_ROWS - 1]
        part = c & (per_chunk - 1)
        skip = jnp.where(part == 0, WINDOW, 0)
        start = (first & -BLOCK) + skip

        @pl.when((last > first) & (last > start))
        def _():
            lane = pl.multiple_of(part * chunk, chunk)
            row = pl.multiple_of(c * CHUNK_ROWS, CHUNK_ROWS)
            parts, where_row = chunk_of(c, c >> bits(per_chunk), lane, row)

            def more(w, inner_carry):
                offset = start + w * WINDOW
                add(offset, sorted_window(parts, where_row - offset))
                return inner_carry

            lax.fori_loop(0, (last - start + WINDOW - 1) >> bits(WINDOW), more, 0)

        return carry

    lax.fori_loop(0, n_edge * per_chunk, sort_chunk, 0)
    load.wait()
    geometry_v[0:4, :] = geometry_w[...].astype(F32)
    found = bounds[1, blocks - 1]

    def encode(j, carry):
        offset = pl.multiple_of(j * STEP, STEP)
        parts = queue[:, pl.ds(offset, STEP)]
        sender = (parts[4:5, :] * 128.0 + parts[5:6, :]).astype(I32)
        target = parts[6:7, :].astype(I32)
        picks = one_hot(iota((grid_rows, STEP), 0) == sender)
        goes = one_hot(iota((shard, STEP), 0) + 1 == target)
        pre = nn(projected[...], picks)
        pre = pre + tn(geometry_v[...].astype(BF16), parts.astype(BF16))
        act = (pre * sigmoid(pre)).astype(BF16)
        total[...] += nt(goes, act)
        return carry

    lax.fori_loop(0, lax.div(found + STEP - 1, STEP), encode, 0)
    partial[...] = total[...].astype(BF16)


def step_of(place):
    return jnp.where((place & 1) == 1, (place + 1) >> 1, -(place >> 1))


def place_of(step, n_mesh):
    step = step & (n_mesh - 1)
    return jnp.where(
        step == 0, 0, jnp.where(step <= n_mesh // 2, 2 * step - 1, 2 * (n_mesh - step))
    )


def process_kernel(
    n_mesh,
    n_edge,
    partial,
    mesh_position,
    band_senders,
    band_receivers,
    band_features,
    cotangent,
    node_position,
    geometry,
    w_encoder_outer,
    w_node_first,
    w_node_second,
    w_edge_sender,
    w_edge_receiver,
    w_edge_outer,
    w_update_message,
    w_update_state,
    w_update_outer,
    output,
    gradient,
    encoder_outer,
    node_first,
    node_second,
    edge_sender,
    edge_receiver,
    edge_outer,
    update_message,
    update_state,
    update_outer,
    padded,
    small,
    enc_land,
    latents,
    coarse_own,
    coarse_land,
    coarse,
    send_pick,
    recv_pick,
    recv_drop,
    back_drop,
    edge_term,
    slope,
    cotangents,
    state_term,
    back_out,
    update_act,
    grad_pre,
    back_far,
    back_far_land,
    tail,
    enc_node,
    edge_update,
    load_sem,
    send_sem,
    recv_sem,
    far_send,
    far_recv,
    relay_send,
    relay_recv,
    forward_send,
    final_send,
    final_recv,
    band_ready,
    far_ready,
):
    me = lax.axis_index("edge")
    band = lax.axis_index("mesh")
    own_rows = cotangent.shape[0]
    shard = own_rows * n_edge
    groups = n_mesh * COARSE // own_rows
    per_group = own_rows // COARSE
    half = band_senders.shape[2]
    edges = 2 * half
    far_rows = n_mesh * COARSE
    loads = [
        pltpu.make_async_copy(src, dst, load_sem.at[k])
        for k, (src, dst) in enumerate(
            [
                (w_encoder_outer, encoder_outer),
                (w_node_first, node_first),
                (w_node_second, node_second),
                (w_edge_sender, edge_sender),
                (w_edge_receiver, edge_receiver),
                (w_edge_outer, edge_outer),
                (w_update_message, update_message),
                (w_update_state, update_state),
                (w_update_outer, update_outer),
            ]
        )
    ]
    for load in loads:
        load.start()
    core = me & 1
    chip = me >> 1
    chips = n_edge // 2
    barrier = pltpu.get_barrier_semaphore()

    def signal_band(k, carry):
        @pl.when((k > 0) | (core == 1))
        def _():
            pl.semaphore_signal(
                barrier,
                inc=1,
                device_id={"edge": 2 * ((chip + k) & (chips - 1))},
                device_id_type=MESH,
            )

        return carry

    def signal_far(k, carry):
        pl.semaphore_signal(
            barrier,
            inc=1,
            device_id={"mesh": (band + k) & (n_mesh - 1), "edge": me | 1},
            device_id_type=MESH,
        )
        return carry

    lax.fori_loop(0, chips, signal_band, 0)
    lax.fori_loop(1, n_mesh, signal_far, 0)

    @pl.when(core == 0)
    def _():
        pl.semaphore_wait(barrier, n_edge - 1)
        pl.semaphore_signal(band_ready, inc=1, device_id={"edge": me ^ 1}, device_id_type=MESH)

    @pl.when(core == 1)
    def _():
        pl.semaphore_wait(band_ready, 1)

    unsent = []

    def to_peer(phase, src, dst, sem, land):
        def copy(peer):
            return pltpu.make_async_remote_copy(
                src_ref=src(peer),
                dst_ref=dst,
                send_sem=send_sem.at[phase, sem(peer)],
                recv_sem=recv_sem.at[phase, land],
                device_id={"edge": peer},
                device_id_type=MESH,
            )

        return copy

    def start_all(phase, src, dst):
        def start(own, peer):
            copy = to_peer(phase, src, dst.at[own], lambda p: p, own)(peer)
            copy.start()
            unsent.append(copy)

        each_peer(n_edge, start)

    def wait_all(phase, src, dst):
        each_peer(
            n_edge,
            lambda own, peer: to_peer(phase, src, dst.at[peer], lambda p: p, peer)(peer).wait_recv(),
        )

    def rows_of(ref):
        return lambda peer: ref.at[pl.ds(pl.multiple_of(peer * own_rows, own_rows), own_rows), :]

    own_slice = pl.ds(pl.multiple_of(me * own_rows, own_rows), own_rows)
    start_all(0, rows_of(partial), enc_land)
    enc_land[me] = partial[own_slice, :]

    padded[...] = jnp.zeros_like(padded)
    padded[0:3, 0:own_rows] = mesh_position[...].astype(F32)
    place_columns = padded[...].T
    position_term = jnp.zeros((own_rows, node_position.shape[1]), F32)
    for k in range(3):
        position_term += (
            place_columns[0:own_rows, k : k + 1] * node_position[k : k + 1, :].astype(F32)
        )

    width = geometry.shape[1]
    padded_geometry = jnp.concatenate([geometry[...].astype(F32)] * 2, axis=0)
    padded_geometry = jnp.where(iota((8, width), 0) < 4, padded_geometry, 0.0).astype(BF16)
    small[...] = jnp.zeros_like(small)
    blocks = n_edge // 2
    table_rows = shard + n_edge * far_rows

    def block_rows(block):
        return pl.ds(pl.multiple_of(block * edges, edges), edges)

    def prepare(block, carry):
        span = block_rows(block)
        first, second = 2 * block, 2 * block + 1
        sender = jnp.concatenate([band_senders[first], band_senders[second]], axis=1)
        receiver = jnp.concatenate([band_receivers[first], band_receivers[second]], axis=1)
        owner_band = sender >> bits(shard)
        near = owner_band == band
        owner_edge = (sender >> bits(own_rows)) & (n_edge - 1)
        far_place = place_of(owner_band - band, n_mesh)
        coarse_row = sender & (COARSE - 1)
        far_slot = ((far_place >> bits(per_group)) * n_edge + owner_edge) * own_rows
        far_slot = far_slot + (far_place & (per_group - 1)) * COARSE + coarse_row
        local = sender - band * shard
        receiver = receiver - band * shard
        pick = jnp.where(near, local, shard + far_slot)
        mine = owner_edge == me
        drop_far = jnp.where(mine & (owner_band != band), far_place * COARSE + coarse_row, -1)
        drop_near = jnp.where(mine & near, local & (own_rows - 1), -1)
        drop_recv = jnp.where(receiver >> bits(own_rows) == me, receiver & (own_rows - 1), -1)
        back_drop[0:far_rows, span] = one_hot(iota((far_rows, edges), 0) == drop_far)
        base = far_rows + own_rows
        back_drop[far_rows:base, span] = one_hot(iota((own_rows, edges), 0) == drop_near)
        back_drop[base:, span] = one_hot(iota((own_rows, edges), 0) == drop_recv)
        recv_drop[:, span] = one_hot(iota((shard, edges), 0) == receiver)
        pick_columns = jnp.broadcast_to(pick.astype(F32), (128, edges)).T.astype(I32)
        recv_columns = jnp.broadcast_to(receiver.astype(F32), (128, edges)).T.astype(I32)
        lanes = iota((edges, 128), 1)
        for k in range(table_rows // 128):
            send_pick[span, k * 128 : (k + 1) * 128] = one_hot(lanes + k * 128 == pick_columns)
        for k in range(shard // 128):
            recv_pick[span, k * 128 : (k + 1) * 128] = one_hot(lanes + k * 128 == recv_columns)
        small[0:4, 0:half] = band_features[first].astype(F32)
        small[0:4, half:edges] = band_features[second].astype(F32)
        edge_term[span, :] = tn(small[...].astype(BF16), padded_geometry)
        return carry

    lax.fori_loop(0, blocks, prepare, 0)
    for load in loads:
        load.wait()
    enc_node[...] = nn(encoder_outer[...], node_first[...]).astype(BF16)

    wait_all(0, rows_of(partial), enc_land)
    enc_sum = jnp.sum(enc_land[...].astype(F32), axis=0)
    hidden = nn(enc_sum.astype(BF16), enc_node[...]) + position_term
    hidden = (hidden * sigmoid(hidden)).astype(BF16)
    latent = layer_norm(nn(hidden, node_second[...])).astype(BF16)
    coarse_own[...] = latent[0:COARSE, :]
    latents[me] = latent

    latent_rows = lambda peer: latents.at[me]
    start_all(1, latent_rows, latents)
    start_all(2, lambda peer: cotangent, cotangents)
    cotangents[me] = cotangent[...]

    def far_copy(place, land):
        return pltpu.make_async_remote_copy(
            src_ref=coarse_own,
            dst_ref=coarse_land.at[land],
            send_sem=far_send.at[place],
            recv_sem=far_recv.at[land],
            device_id={"mesh": (band + step_of(place) + n_mesh) & (n_mesh - 1)},
            device_id_type=MESH,
        )

    def far_start(k, carry):
        place = n_mesh - k
        far_copy(place, place_of(-step_of(place), n_mesh)).start()
        return carry

    @pl.when(core == 1)
    def _():
        pl.semaphore_wait(barrier, 2 * (n_mesh - 1))
        pl.semaphore_signal(far_ready, inc=1, device_id={"edge": me ^ 1}, device_id_type=MESH)

    @pl.when(core == 0)
    def _():
        pl.semaphore_wait(far_ready, 1)

    lax.fori_loop(1, n_mesh, far_start, 0)
    coarse_land[0] = coarse_own[...]

    def relay(group, owner, peer):
        return pltpu.make_async_remote_copy(
            src_ref=coarse.at[owner, group],
            dst_ref=coarse.at[owner, group],
            send_sem=relay_send.at[group, peer],
            recv_sem=relay_recv.at[group, owner],
            device_id={"edge": peer},
            device_id_type=MESH,
        )

    def forward(group, owner):
        return pltpu.make_async_remote_copy(
            src_ref=coarse.at[owner, group],
            dst_ref=coarse.at[owner, group],
            send_sem=forward_send.at[group, owner],
            recv_sem=relay_recv.at[group, owner],
            device_id={"edge": me ^ 1},
            device_id_type=MESH,
        )

    def pass_on(group):
        def step(owner):
            relay(group, owner, owner).wait_recv()
            copy = forward(group, owner)
            copy.start()
            unsent.append(copy)

        each_chip(n_edge, step)

    def relay_start(group, peer):
        copy = relay(group, me, peer)
        copy.start()
        unsent.append(copy)

    def take_in(group):
        each_chip(n_edge, lambda peer: forward(group, peer ^ 1).wait_recv())
        relay(group, me ^ 1, me).wait_recv()
        table = coarse[:, group].reshape(n_edge * own_rows, width)
        table = nn(table, edge_sender[...]).astype(BF16)
        return pl.ds(shard + group * n_edge * own_rows, n_edge * own_rows), table

    def add_in(group):
        columns, table = take_in(group)

        def add(block, carry):
            span = block_rows(block)
            edge_term[span, :] += nn(send_pick[span, columns], table)
            return carry

        lax.fori_loop(0, blocks, add, 0)

    edge_update[...] = nn(edge_outer[...], update_message[...]).astype(BF16)
    wait_all(1, latent_rows, latents)
    band_latent = latents[...].reshape(shard, width)
    near_table = nn(band_latent, edge_sender[...]).astype(BF16)
    recv_table = nn(band_latent, edge_receiver[...]).astype(BF16)

    def add_near(block, carry):
        span = block_rows(block)
        edge_term[span, :] += nn(send_pick[span, 0:shard], near_table) + nn(
            recv_pick[span, :], recv_table
        )
        return carry

    lax.fori_loop(0, blocks, add_near, 0)
    state_term[...] = nn(band_latent, update_state[...])
    wait_all(2, lambda peer: cotangent, cotangents)
    back_out[...] = nt(cotangents[...].reshape(shard, width), update_outer[...])

    for group in range(groups):
        for k in range(per_group):
            place = group * per_group + k
            if place > 0:
                far_copy(place, place).wait_recv()
        rows = [coarse_land[group * per_group + k].astype(F32) for k in range(per_group)]
        coarse[me, group] = jnp.concatenate(rows, axis=0).astype(BF16)
        each_chip(n_edge, lambda peer: relay_start(group, peer))
        relay_start(group, me ^ 1)
        if group > 0:
            pass_on(group - 1)
        if group > 1:
            add_in(group - 2)
    if groups > 1:
        add_in(groups - 2)
    pass_on(groups - 1)
    columns, table = take_in(groups - 1)
    proc_sum = jnp.zeros((shard, width), F32)
    for block in range(blocks):
        span = pl.ds(block * edges, edges)
        pre = edge_term[span, :] + nn(send_pick[span, columns], table)
        sigma = sigmoid(pre)
        slope[span, :] = sigma * (1.0 + pre * (1.0 - sigma))
        proc_sum = proc_sum + nn(recv_drop[:, span], (pre * sigma).astype(BF16))
    update_pre = nn(proc_sum.astype(BF16), edge_update[...]) + state_term[...]
    sigma = sigmoid(update_pre)
    slopes = sigma * (1.0 + update_pre * (1.0 - sigma))
    grad_all = (back_out[...] * slopes).astype(BF16)
    grad_pre[...] = grad_all
    update_act[...] = (update_pre * sigma).astype(BF16)
    band_grads = nt(grad_all, edge_update[...]).astype(BF16)
    back = jnp.zeros((far_rows + 2 * own_rows, width), F32)
    for block in range(blocks):
        span = pl.ds(block * edges, edges)
        grad_edge = (nn(recv_pick[span, :], band_grads) * slope[span, :]).astype(BF16)
        back = back + nn(back_drop[:, span], grad_edge)
    far_total = back[0:far_rows, :]

    def final_copy(place, land):
        return pltpu.make_async_remote_copy(
            src_ref=back_far.at[place],
            dst_ref=back_far_land.at[land],
            send_sem=final_send.at[place],
            recv_sem=final_recv.at[land],
            device_id={"mesh": (band + step_of(place) + n_mesh) & (n_mesh - 1)},
            device_id_type=MESH,
        )

    for place in range(1, n_mesh):
        back_far[place] = far_total[place * COARSE : (place + 1) * COARSE, :].astype(BF16)

    def final_start(k, carry):
        place = n_mesh - k
        final_copy(place, place_of(-step_of(place), n_mesh)).start()
        return carry

    lax.fori_loop(1, n_mesh, final_start, 0)
    mixed = latents[me].astype(F32) + nn(update_act[own_slice, :], update_outer[...])
    output[...] = mixed.astype(BF16)
    grad_node = cotangent[...].astype(F32) + nt(grad_pre[own_slice, :], update_state[...])
    to_receiver = back[far_rows + own_rows :, :].astype(BF16)
    result = grad_node + nt(to_receiver, edge_receiver[...])
    tail[...] = back[far_rows : far_rows + own_rows, :]

    def final_finish(k, carry):
        final_copy(k, k).wait_recv()
        return carry

    lax.fori_loop(1, n_mesh, final_finish, 0)
    arrived = back_far_land[1].astype(F32)
    for place in range(2, n_mesh):
        arrived = arrived + back_far_land[place].astype(F32)
    tail[0:COARSE, :] += arrived
    gradient[...] = result + nt(tail[...].astype(BF16), edge_sender[...])

    def far_sent(k, carry):
        far_copy(k, k).wait_send()
        final_copy(k, k).wait_send()
        return carry

    lax.fori_loop(1, n_mesh, far_sent, 0)
    for copy in unsent:
        copy.wait_send()


def finish_kernel(output, gradient, output_copy, gradient_copy):
    output_copy[...] = output[...]
    gradient_copy[...] = gradient[...]


def vmem():
    return pl.BlockSpec(memory_space=pltpu.VMEM)


def anywhere():
    return pl.BlockSpec(memory_space=pltpu.HBM)


def hbm(value):
    return pltpu.with_memory_space_constraint(value, pltpu.HBM)


def shards(
    n_mesh,
    n_edge,
    grid_input,
    mesh_position,
    encoder_senders,
    encoder_receivers,
    encoder_features,
    encoder_counts,
    mesh_senders,
    mesh_receivers,
    mesh_features,
    cotangent,
    grid_first,
    grid_second,
    encoder_inner,
    encoder_geometry,
    encoder_outer,
    node_first,
    node_position,
    node_second,
    edge_sender,
    edge_receiver,
    edge_geometry,
    edge_outer,
    update_message,
    update_state,
    update_outer,
):
    grid_rows, channels = grid_input.shape
    width = grid_second.shape[1]
    slots = encoder_senders.shape[0]
    blocks = slots // BLOCK
    own_rows = mesh_position.shape[1]
    shard = own_rows * n_edge
    edges = mesh_senders.shape[0]
    dma = pltpu.SemaphoreType.DMA
    packed, features, projected, band_senders, band_receivers, band_features = pl.pallas_call(
        functools.partial(embed_kernel, n_edge),
        out_shape=(
            jax.ShapeDtypeStruct((n_edge, blocks, BLOCK), I32),
            jax.ShapeDtypeStruct((n_edge, 4, slots), BF16),
            jax.ShapeDtypeStruct((width, grid_rows), BF16),
            jax.ShapeDtypeStruct((n_edge, 1, edges), I32),
            jax.ShapeDtypeStruct((n_edge, 1, edges), I32),
            jax.ShapeDtypeStruct((n_edge, 4, edges), BF16),
        ),
        in_specs=[pl.BlockSpec(memory_space=pltpu.SMEM)] + [anywhere()] * 10,
        out_specs=(vmem(),) * 6,
        scratch_shapes=[
            pltpu.VMEM((blocks, BLOCK), I32),
            pltpu.VMEM((blocks, BLOCK), I32),
            pltpu.VMEM((channels, grid_rows), BF16),
            pltpu.VMEM((channels, width), BF16),
            pltpu.VMEM((width, width), BF16),
            pltpu.VMEM((width, width), BF16),
            dma((10,)),
            dma((5, n_edge)),
            dma((5, n_edge)),
        ],
        compiler_params=pltpu.CompilerParams(
            collective_id=0, has_side_effects=True, vmem_limit_bytes=12 << 20
        ),
    )(
        encoder_counts,
        hbm(encoder_senders.reshape(blocks, BLOCK)),
        hbm(encoder_receivers.reshape(blocks, BLOCK)),
        hbm(encoder_features),
        hbm(mesh_senders.reshape(1, edges)),
        hbm(mesh_receivers.reshape(1, edges)),
        hbm(mesh_features),
        hbm(grid_input.T),
        hbm(grid_first),
        hbm(grid_second),
        hbm(encoder_inner),
    )
    all_blocks = n_edge * blocks
    partial = pl.pallas_call(
        functools.partial(encode_kernel, n_edge, shard),
        out_shape=jax.ShapeDtypeStruct((shard, width), BF16),
        in_specs=[vmem()] * 3 + [anywhere()],
        out_specs=vmem(),
        scratch_shapes=[
            pltpu.VMEM((all_blocks, BLOCK), I32),
            pltpu.VMEM((8, all_blocks), I32),
            pltpu.SMEM((8, all_blocks), I32),
            pltpu.VMEM((8, n_edge * slots + STEP), F32),
            pltpu.VMEM((8, width), F32),
            pltpu.VMEM((4, width), BF16),
            pltpu.VMEM((shard, width), F32),
            dma(()),
            dma(()),
        ],
        compiler_params=pltpu.CompilerParams(vmem_limit_bytes=16 << 20),
    )(packed.reshape(all_blocks, BLOCK), features, projected, hbm(encoder_geometry))
    far_rows = n_mesh * COARSE
    groups = far_rows // own_rows
    table_rows = shard + n_edge * far_rows
    weights = [
        encoder_outer,
        node_first,
        node_second,
        edge_sender,
        edge_receiver,
        edge_outer,
        update_message,
        update_state,
        update_outer,
    ]
    output, gradient = pl.pallas_call(
        functools.partial(process_kernel, n_mesh, n_edge),
        out_shape=(
            jax.ShapeDtypeStruct((own_rows, width), BF16),
            jax.ShapeDtypeStruct((own_rows, width), F32),
        ),
        in_specs=[vmem()] * 8 + [anywhere()] * 9,
        out_specs=(vmem(), vmem()),
        scratch_shapes=[pltpu.VMEM((width, width), BF16) for _ in weights]
        + [
            pltpu.VMEM((128, 128), F32),
            pltpu.VMEM((8, 2 * edges), F32),
            pltpu.VMEM((n_edge, own_rows, width), BF16),
            pltpu.VMEM((n_edge, own_rows, width), BF16),
            pltpu.VMEM((COARSE, width), BF16),
            pltpu.VMEM((n_mesh, COARSE, width), BF16),
            pltpu.VMEM((n_edge, groups, own_rows, width), BF16),
            pltpu.VMEM((n_edge * edges, table_rows), BF16),
            pltpu.VMEM((n_edge * edges, shard), BF16),
            pltpu.VMEM((shard, n_edge * edges), BF16),
            pltpu.VMEM((far_rows + 2 * own_rows, n_edge * edges), BF16),
            pltpu.VMEM((n_edge * edges, width), F32),
            pltpu.VMEM((n_edge * edges, width), F32),
            pltpu.VMEM((n_edge, own_rows, width), BF16),
            pltpu.VMEM((shard, width), F32),
            pltpu.VMEM((shard, width), F32),
            pltpu.VMEM((shard, width), BF16),
            pltpu.VMEM((shard, width), BF16),
            pltpu.VMEM((n_mesh, COARSE, width), BF16),
            pltpu.VMEM((n_mesh, COARSE, width), BF16),
            pltpu.VMEM((own_rows, width), F32),
            pltpu.VMEM((width, width), BF16),
            pltpu.VMEM((width, width), BF16),
            dma((9,)),
            dma((3, n_edge)),
            dma((3, n_edge)),
            dma((n_mesh,)),
            dma((n_mesh,)),
            dma((groups, n_edge)),
            dma((groups, n_edge)),
            dma((groups, n_edge)),
            dma((n_mesh,)),
            dma((n_mesh,)),
            pltpu.SemaphoreType.REGULAR,
            pltpu.SemaphoreType.REGULAR,
        ],
        compiler_params=pltpu.CompilerParams(
            collective_id=1, has_side_effects=True, vmem_limit_bytes=36 << 20
        ),
    )(
        partial,
        mesh_position,
        band_senders,
        band_receivers,
        band_features,
        cotangent,
        node_position,
        edge_geometry,
        *[hbm(weight) for weight in weights],
    )
    return pl.pallas_call(
        finish_kernel,
        out_shape=(
            jax.ShapeDtypeStruct((own_rows, width), BF16),
            jax.ShapeDtypeStruct((own_rows, width), F32),
        ),
        in_specs=[vmem()] * 2,
        out_specs=(vmem(), vmem()),
        compiler_params=pltpu.CompilerParams(vmem_limit_bytes=1 << 20),
    )(output, gradient)


def solution(mesh):
    banded = ("mesh", "edge")
    every = ("groups", "mesh", "edge")
    in_specs = (
        P(every, None),
        P(None, banded),
        P(banded),
        P(banded),
        P(None, banded),
        P(banded),
        P(banded),
        P(banded),
        P(None, banded),
        P(every, None),
    ) + (P(),) * 15
    return jax.shard_map(
        functools.partial(shards, mesh.shape["mesh"], mesh.shape["edge"]),
        mesh=mesh,
        in_specs=in_specs,
        out_specs=(P(every, None), P(every, None)),
        check_vma=False,
    )
```

```python
import functools

import jax
import jax.numpy as jnp
from jax import lax
from jax.experimental import pallas as pl
from jax.experimental.pallas import tpu as pltpu
from jax.sharding import PartitionSpec as P

BLOCK = 128
CHUNK_ROWS = 8
WINDOW = 256
STEP = 512
COARSE = 4
MESH = pl.DeviceIdType.MESH
F32 = jnp.float32
BF16 = jnp.bfloat16
I32 = jnp.int32


def bits(size):
    return size.bit_length() - 1


def nn(left, right):
    return jnp.dot(left, right, preferred_element_type=F32)


def nt(left, right):
    return lax.dot_general(left, right, (((1,), (1,)), ((), ())), preferred_element_type=F32)


def tn(left, right):
    return lax.dot_general(left, right, (((0,), (0,)), ((), ())), preferred_element_type=F32)


def tt(left, right):
    return lax.dot_general(left, right, (((0,), (1,)), ((), ())), preferred_element_type=F32)


def sigmoid(values):
    return 0.5 + 0.5 * jnp.tanh(0.5 * values)


def layer_norm(values):
    centred = values - jnp.mean(values, axis=-1, keepdims=True)
    variance = jnp.mean(centred * centred, axis=-1, keepdims=True)
    return centred * lax.rsqrt(variance + 1e-05)


def iota(shape, dim):
    return lax.broadcasted_iota(I32, shape, dim)


def one_hot(hits):
    return jnp.where(hits, 1.0, 0.0).astype(BF16)


def greet(axis, count):
    me = lax.axis_index(axis)
    barrier = pltpu.get_barrier_semaphore()

    def signal(k, carry):
        pl.semaphore_signal(
            barrier, inc=1, device_id={axis: lax.rem(me + k, count)}, device_id_type=MESH
        )
        return carry

    lax.fori_loop(1, count, signal, 0)


def chip_steps(chips):
    return sorted(range(1, chips), key=lambda step: -min(step, chips - step))


def each_chip(n_edge, action):
    me = lax.axis_index("edge")
    chips = n_edge // 2
    for step in chip_steps(chips):
        action((me + 2 * step) & (n_edge - 1))


def each_peer(n_edge, action):
    me = lax.axis_index("edge")
    chips = n_edge // 2
    for step in chip_steps(chips):
        peer = (me + 2 * step) & (n_edge - 1)
        action(me, peer)
        action(me, peer ^ 1)
    action(me, me ^ 1)


def embed_kernel(
    n_edge,
    count,
    senders,
    receivers,
    features,
    grid_input,
    first,
    second,
    inner,
    packed_all,
    features_all,
    projected,
    senders_v,
    receivers_v,
    rows_v,
    first_v,
    second_v,
    inner_v,
    load_sem,
    send_sem,
    recv_sem,
):
    me = lax.axis_index("edge")
    band = lax.axis_index("mesh")
    loads = [
        pltpu.make_async_copy(src, dst, load_sem.at[k])
        for k, (src, dst) in enumerate(
            [
                (senders, senders_v),
                (receivers, receivers_v),
                (features, features_all.at[me]),
                (grid_input, rows_v),
                (first, first_v),
                (second, second_v),
                (inner, inner_v),
            ]
        )
    ]
    for load in loads:
        load.start()
    greet("edge", n_edge)
    blocks = senders.shape[0]
    rows = grid_input.shape[1]
    shard = packed_shard(n_edge)
    loads[0].wait()
    loads[1].wait()
    low = senders_v[...] - band * (rows * n_edge)
    near = receivers_v[...] - band * shard
    live = iota((blocks, BLOCK), 0) < count[0]
    packed_all[me] = jnp.where(live, low * shard + near, -1)
    loads[2].wait()
    pl.semaphore_wait(pltpu.get_barrier_semaphore(), n_edge - 1)

    tables = (packed_all, features_all)

    def copy(k, owner, peer):
        return pltpu.make_async_remote_copy(
            src_ref=tables[k].at[owner],
            dst_ref=tables[k].at[owner],
            send_sem=send_sem.at[k, peer],
            recv_sem=recv_sem.at[k, owner],
            device_id={"edge": peer},
            device_id_type=MESH,
        )

    each_peer(n_edge, lambda own, peer: [copy(k, own, peer).start() for k in range(len(tables))])
    loads[3].wait()
    loads[4].wait()
    hidden = tn(rows_v[...], first_v[...])
    hidden = (hidden * sigmoid(hidden)).astype(BF16)
    loads[5].wait()
    latent = layer_norm(nn(hidden, second_v[...])).astype(BF16)
    loads[6].wait()
    projected[...] = tt(inner_v[...], latent).astype(BF16)

    def arrive(own, peer):
        for k in range(len(tables)):
            copy(k, peer, peer).wait_recv()

    def sent(own, peer):
        for k in range(len(tables)):
            copy(k, own, peer).wait_send()

    each_peer(n_edge, arrive)
    each_peer(n_edge, sent)


def packed_shard(n_edge):
    return 16 * n_edge


def encode_kernel(
    n_edge,
    shard,
    packed,
    features,
    projected,
    geometry,
    partial,
    position,
    bounds_v,
    bounds,
    queue,
    geometry_v,
    geometry_w,
    total,
    sem,
    geometry_sem,
):
    me = lax.axis_index("edge")
    load = pltpu.make_async_copy(geometry, geometry_w, geometry_sem)
    load.start()
    blocks = packed.shape[0]
    per_device = blocks // n_edge
    grid_rows = projected.shape[1]
    width = projected.shape[0]
    shift = bits(shard)
    row_bits = bits(grid_rows)
    index = packed[...]
    own = (index >> (shift + row_bits)) == me
    own_b = one_hot(own)
    upper = one_hot(iota((BLOCK, BLOCK), 0) < iota((BLOCK, BLOCK), 1))
    before = one_hot(iota((blocks, blocks), 0) < iota((blocks, blocks), 1))
    lower = one_hot(iota((blocks, blocks), 0) > iota((blocks, blocks), 1))
    ones = jnp.ones((BLOCK, BLOCK), BF16)
    rank = nn(own_b, upper)
    per_block = nn(own_b, ones)
    base = nn(lower, per_block.astype(BF16))
    aligned = base.astype(I32) & -BLOCK
    position[...] = jnp.where(own, (rank + base).astype(I32), -1)
    totals = nt(jnp.ones((8, BLOCK), BF16), own_b)
    starts = nn(totals.astype(BF16), before)
    stops = starts + totals
    bounds_v[...] = jnp.where(iota((8, blocks), 0) == 0, starts, stops).astype(I32)
    copy = pltpu.make_async_copy(bounds_v, bounds, sem)
    copy.start()
    queue[...] = jnp.zeros_like(queue)
    total[...] = jnp.zeros_like(total)
    geometry_v[...] = jnp.zeros_like(geometry_v)
    chunk = CHUNK_ROWS * BLOCK
    per_chunk = per_device // CHUNK_ROWS

    def chunk_of(c, device, lane, row):
        code = packed[pl.ds(row, CHUNK_ROWS), :]
        where = position[pl.ds(row, CHUNK_ROWS), :]
        code_row = jnp.concatenate([code[k : k + 1, :] for k in range(CHUNK_ROWS)], axis=1)
        where_row = jnp.concatenate([where[k : k + 1, :] for k in range(CHUNK_ROWS)], axis=1)
        sender = (code_row >> shift) & (grid_rows - 1)
        parts = features[device, :, pl.ds(lane, chunk)].astype(F32)
        parts = jnp.concatenate([parts, jnp.zeros_like(parts)], axis=0)
        place = iota((8, chunk), 0)
        parts = jnp.where(place == 4, (sender >> 7).astype(F32), parts)
        parts = jnp.where(place == 5, (sender & 127).astype(F32), parts)
        parts = jnp.where(place == 6, ((code_row & (shard - 1)) + 1).astype(F32), parts)
        return parts.astype(BF16), where_row

    def sorted_window(parts, where_row):
        return nt(parts, one_hot(iota((WINDOW, chunk), 0) == where_row))

    def add(offset, window):
        queue[:, pl.ds(pl.multiple_of(offset, BLOCK), WINDOW)] += window

    windows = []
    for device in range(n_edge):
        c = device * per_chunk
        parts, where_row = chunk_of(c, device, 0, c * CHUNK_ROWS)
        from_row = aligned[c * CHUNK_ROWS : c * CHUNK_ROWS + 1, :]
        from_row = jnp.concatenate([from_row] * CHUNK_ROWS, axis=1)
        windows.append(sorted_window(parts, where_row - from_row))
    copy.wait()
    for device, window in enumerate(windows):
        add(bounds[0, device * per_chunk * CHUNK_ROWS] & -BLOCK, window)

    def sort_chunk(c, carry):
        first = bounds[0, c * CHUNK_ROWS]
        last = bounds[1, c * CHUNK_ROWS + CHUNK_ROWS - 1]
        part = c & (per_chunk - 1)
        skip = jnp.where(part == 0, WINDOW, 0)
        start = (first & -BLOCK) + skip

        @pl.when((last > first) & (last > start))
        def _():
            lane = pl.multiple_of(part * chunk, chunk)
            row = pl.multiple_of(c * CHUNK_ROWS, CHUNK_ROWS)
            parts, where_row = chunk_of(c, c >> bits(per_chunk), lane, row)

            def more(w, inner_carry):
                offset = start + w * WINDOW
                add(offset, sorted_window(parts, where_row - offset))
                return inner_carry

            lax.fori_loop(0, (last - start + WINDOW - 1) >> bits(WINDOW), more, 0)

        return carry

    lax.fori_loop(0, n_edge * per_chunk, sort_chunk, 0)
    load.wait()
    geometry_v[0:4, :] = geometry_w[...].astype(F32)
    found = bounds[1, blocks - 1]

    def encode(j, carry):
        offset = pl.multiple_of(j * STEP, STEP)
        parts = queue[:, pl.ds(offset, STEP)]
        sender = (parts[4:5, :] * 128.0 + parts[5:6, :]).astype(I32)
        target = parts[6:7, :].astype(I32)
        picks = one_hot(iota((grid_rows, STEP), 0) == sender)
        goes = one_hot(iota((shard, STEP), 0) + 1 == target)
        pre = nn(projected[...], picks)
        pre = pre + tn(geometry_v[...].astype(BF16), parts.astype(BF16))
        act = (pre * sigmoid(pre)).astype(BF16)
        total[...] += nt(goes, act)
        return carry

    lax.fori_loop(0, lax.div(found + STEP - 1, STEP), encode, 0)
    partial[...] = total[...].astype(BF16)


def step_of(place):
    return jnp.where((place & 1) == 1, (place + 1) >> 1, -(place >> 1))


def place_of(step, n_mesh):
    step = step & (n_mesh - 1)
    return jnp.where(
        step == 0, 0, jnp.where(step <= n_mesh // 2, 2 * step - 1, 2 * (n_mesh - step))
    )


def process_kernel(
    n_mesh,
    n_edge,
    partial,
    mesh_position,
    mesh_senders,
    mesh_receivers,
    mesh_features,
    cotangent,
    node_position,
    geometry,
    w_encoder_outer,
    w_node_first,
    w_node_second,
    w_edge_sender,
    w_edge_receiver,
    w_edge_outer,
    w_update_message,
    w_update_state,
    w_update_outer,
    output,
    gradient,
    encoder_outer,
    node_first,
    node_second,
    edge_sender,
    edge_receiver,
    edge_outer,
    update_message,
    update_state,
    update_outer,
    padded,
    small,
    enc_land,
    latents,
    coarse_own,
    coarse_land,
    coarse,
    band_senders,
    band_receivers,
    band_features,
    send_pick,
    recv_pick,
    recv_drop,
    back_drop,
    edge_term,
    slope,
    cotangents,
    state_term,
    back_out,
    update_act,
    grad_pre,
    back_far,
    back_far_land,
    tail,
    enc_node,
    edge_update,
    load_sem,
    send_sem,
    recv_sem,
    far_send,
    far_recv,
    relay_send,
    relay_recv,
    forward_send,
    final_send,
    final_recv,
    band_ready,
    far_ready,
):
    me = lax.axis_index("edge")
    band = lax.axis_index("mesh")
    own_rows = cotangent.shape[0]
    shard = own_rows * n_edge
    groups = n_mesh * COARSE // own_rows
    per_group = own_rows // COARSE
    half = mesh_senders.shape[1]
    edges = 2 * half
    far_rows = n_mesh * COARSE
    loads = [
        pltpu.make_async_copy(src, dst, load_sem.at[k])
        for k, (src, dst) in enumerate(
            [
                (w_encoder_outer, encoder_outer),
                (w_node_first, node_first),
                (w_node_second, node_second),
                (w_edge_sender, edge_sender),
                (w_edge_receiver, edge_receiver),
                (w_edge_outer, edge_outer),
                (w_update_message, update_message),
                (w_update_state, update_state),
                (w_update_outer, update_outer),
            ]
        )
    ]
    for load in loads:
        load.start()
    core = me & 1
    chip = me >> 1
    chips = n_edge // 2
    barrier = pltpu.get_barrier_semaphore()

    def signal_band(k, carry):
        @pl.when((k > 0) | (core == 1))
        def _():
            pl.semaphore_signal(
                barrier,
                inc=1,
                device_id={"edge": 2 * ((chip + k) & (chips - 1))},
                device_id_type=MESH,
            )

        return carry

    def signal_far(k, carry):
        pl.semaphore_signal(
            barrier,
            inc=1,
            device_id={"mesh": (band + k) & (n_mesh - 1), "edge": me | 1},
            device_id_type=MESH,
        )
        return carry

    lax.fori_loop(0, chips, signal_band, 0)
    lax.fori_loop(1, n_mesh, signal_far, 0)

    @pl.when(core == 0)
    def _():
        pl.semaphore_wait(barrier, n_edge - 1)
        pl.semaphore_signal(band_ready, inc=1, device_id={"edge": me ^ 1}, device_id_type=MESH)

    @pl.when(core == 1)
    def _():
        pl.semaphore_wait(band_ready, 1)

    unsent = []

    def to_peer(phase, src, dst, sem, land):
        def copy(peer):
            return pltpu.make_async_remote_copy(
                src_ref=src(peer),
                dst_ref=dst,
                send_sem=send_sem.at[phase, sem(peer)],
                recv_sem=recv_sem.at[phase, land],
                device_id={"edge": peer},
                device_id_type=MESH,
            )

        return copy

    def start_all(phase, src, dst):
        def start(own, peer):
            copy = to_peer(phase, src, dst.at[own], lambda p: p, own)(peer)
            copy.start()
            unsent.append(copy)

        each_peer(n_edge, start)

    def wait_all(phase, src, dst):
        each_peer(
            n_edge,
            lambda own, peer: to_peer(phase, src, dst.at[peer], lambda p: p, peer)(peer).wait_recv(),
        )

    def rows_of(ref):
        return lambda peer: ref.at[pl.ds(pl.multiple_of(peer * own_rows, own_rows), own_rows), :]

    own_slice = pl.ds(pl.multiple_of(me * own_rows, own_rows), own_rows)
    start_all(0, rows_of(partial), enc_land)
    enc_land[me] = partial[own_slice, :]
    tables = (
        (3, mesh_senders, band_senders),
        (4, mesh_receivers, band_receivers),
        (5, mesh_features, band_features),
    )
    for phase, src, dst in tables:
        start_all(phase, lambda peer: src, dst)
        dst[me] = src[...]

    padded[...] = jnp.zeros_like(padded)
    padded[0:3, 0:own_rows] = mesh_position[...].astype(F32)
    place_columns = padded[...].T
    position_term = jnp.zeros((own_rows, node_position.shape[1]), F32)
    for k in range(3):
        position_term += (
            place_columns[0:own_rows, k : k + 1] * node_position[k : k + 1, :].astype(F32)
        )

    width = geometry.shape[1]
    for load in loads:
        load.wait()
    enc_node[...] = nn(encoder_outer[...], node_first[...]).astype(BF16)

    wait_all(0, rows_of(partial), enc_land)

    @pl.when(core == 1)
    def _():
        pl.semaphore_wait(barrier, 2 * (n_mesh - 1))
        pl.semaphore_signal(far_ready, inc=1, device_id={"edge": me ^ 1}, device_id_type=MESH)

    enc_sum = jnp.sum(enc_land[...].astype(F32), axis=0)
    hidden = nn(enc_sum.astype(BF16), enc_node[...]) + position_term
    hidden = (hidden * sigmoid(hidden)).astype(BF16)
    latent = layer_norm(nn(hidden, node_second[...])).astype(BF16)
    coarse_own[...] = latent[0:COARSE, :]
    latents[me] = latent

    latent_rows = lambda peer: latents.at[me]

    def far_copy(place, land):
        return pltpu.make_async_remote_copy(
            src_ref=coarse_own,
            dst_ref=coarse_land.at[land],
            send_sem=far_send.at[place],
            recv_sem=far_recv.at[land],
            device_id={"mesh": (band + step_of(place) + n_mesh) & (n_mesh - 1)},
            device_id_type=MESH,
        )

    def far_start(k, carry):
        place = n_mesh - k
        far_copy(place, place_of(-step_of(place), n_mesh)).start()
        return carry

    @pl.when(core == 0)
    def _():
        pl.semaphore_wait(far_ready, 1)

    lax.fori_loop(1, n_mesh, far_start, 0)
    start_all(1, latent_rows, latents)
    start_all(2, lambda peer: cotangent, cotangents)
    cotangents[me] = cotangent[...]
    coarse_land[0] = coarse_own[...]
    for phase, src, dst in tables:
        wait_all(phase, lambda peer: src, dst)
    padded_geometry = jnp.concatenate([geometry[...].astype(F32)] * 2, axis=0)
    padded_geometry = jnp.where(iota((8, width), 0) < 4, padded_geometry, 0.0).astype(BF16)
    small[...] = jnp.zeros_like(small)
    blocks = n_edge // 2
    table_rows = shard + n_edge * far_rows

    def block_rows(block):
        return pl.ds(pl.multiple_of(block * edges, edges), edges)

    def prepare(block, carry):
        span = block_rows(block)
        first, second = 2 * block, 2 * block + 1
        sender = jnp.concatenate([band_senders[first], band_senders[second]], axis=1)
        receiver = jnp.concatenate([band_receivers[first], band_receivers[second]], axis=1)
        owner_band = sender >> bits(shard)
        near = owner_band == band
        owner_edge = (sender >> bits(own_rows)) & (n_edge - 1)
        far_place = place_of(owner_band - band, n_mesh)
        coarse_row = sender & (COARSE - 1)
        far_slot = ((far_place >> bits(per_group)) * n_edge + owner_edge) * own_rows
        far_slot = far_slot + (far_place & (per_group - 1)) * COARSE + coarse_row
        local = sender - band * shard
        receiver = receiver - band * shard
        pick = jnp.where(near, local, shard + far_slot)
        mine = owner_edge == me
        drop_far = jnp.where(mine & (owner_band != band), far_place * COARSE + coarse_row, -1)
        drop_near = jnp.where(mine & near, local & (own_rows - 1), -1)
        drop_recv = jnp.where(receiver >> bits(own_rows) == me, receiver & (own_rows - 1), -1)
        back_drop[0:far_rows, span] = one_hot(iota((far_rows, edges), 0) == drop_far)
        base = far_rows + own_rows
        back_drop[far_rows:base, span] = one_hot(iota((own_rows, edges), 0) == drop_near)
        back_drop[base:, span] = one_hot(iota((own_rows, edges), 0) == drop_recv)
        recv_drop[:, span] = one_hot(iota((shard, edges), 0) == receiver)
        pick_columns = jnp.broadcast_to(pick.astype(F32), (128, edges)).T.astype(I32)
        recv_columns = jnp.broadcast_to(receiver.astype(F32), (128, edges)).T.astype(I32)
        lanes = iota((edges, 128), 1)
        for k in range(table_rows // 128):
            send_pick[span, k * 128 : (k + 1) * 128] = one_hot(lanes + k * 128 == pick_columns)
        for k in range(shard // 128):
            recv_pick[span, k * 128 : (k + 1) * 128] = one_hot(lanes + k * 128 == recv_columns)
        small[0:4, 0:half] = band_features[first].astype(F32)
        small[0:4, half:edges] = band_features[second].astype(F32)
        edge_term[span, :] = tn(small[...].astype(BF16), padded_geometry)
        return carry

    lax.fori_loop(0, blocks, prepare, 0)

    def relay(group, owner, peer):
        return pltpu.make_async_remote_copy(
            src_ref=coarse.at[owner, group],
            dst_ref=coarse.at[owner, group],
            send_sem=relay_send.at[group, peer],
            recv_sem=relay_recv.at[group, owner],
            device_id={"edge": peer},
            device_id_type=MESH,
        )

    def forward(group, owner):
        return pltpu.make_async_remote_copy(
            src_ref=coarse.at[owner, group],
            dst_ref=coarse.at[owner, group],
            send_sem=forward_send.at[group, owner],
            recv_sem=relay_recv.at[group, owner],
            device_id={"edge": me ^ 1},
            device_id_type=MESH,
        )

    def pass_on(group):
        def step(owner):
            relay(group, owner, owner).wait_recv()
            copy = forward(group, owner)
            copy.start()
            unsent.append(copy)

        each_chip(n_edge, step)

    def relay_start(group, peer):
        copy = relay(group, me, peer)
        copy.start()
        unsent.append(copy)

    def take_in(group):
        if group == groups - 1:
            each_peer(n_edge, lambda own, peer: relay(group, peer, me).wait_recv())
        else:
            each_chip(n_edge, lambda peer: forward(group, peer ^ 1).wait_recv())
            relay(group, me ^ 1, me).wait_recv()
        table = coarse[:, group].reshape(n_edge * own_rows, width)
        table = nn(table, edge_sender[...]).astype(BF16)
        return pl.ds(shard + group * n_edge * own_rows, n_edge * own_rows), table

    def add_in(group):
        columns, table = take_in(group)

        def add(block, carry):
            span = block_rows(block)
            edge_term[span, :] += nn(send_pick[span, columns], table)
            return carry

        lax.fori_loop(0, blocks, add, 0)

    edge_update[...] = nn(edge_outer[...], update_message[...]).astype(BF16)
    wait_all(1, latent_rows, latents)
    band_latent = latents[...].reshape(shard, width)
    near_table = nn(band_latent, edge_sender[...]).astype(BF16)
    recv_table = nn(band_latent, edge_receiver[...]).astype(BF16)

    def add_near(block, carry):
        span = block_rows(block)
        edge_term[span, :] += nn(send_pick[span, 0:shard], near_table) + nn(
            recv_pick[span, :], recv_table
        )
        return carry

    lax.fori_loop(0, blocks, add_near, 0)
    state_term[...] = nn(band_latent, update_state[...])
    wait_all(2, lambda peer: cotangent, cotangents)
    back_out[...] = nt(cotangents[...].reshape(shard, width), update_outer[...])

    for group in range(groups):
        for k in range(per_group):
            place = group * per_group + k
            if place > 0:
                far_copy(place, place).wait_recv()
        rows = [coarse_land[group * per_group + k].astype(F32) for k in range(per_group)]
        coarse[me, group] = jnp.concatenate(rows, axis=0).astype(BF16)
        if group == groups - 1:
            each_peer(n_edge, lambda own, peer: relay_start(group, peer))
        else:
            each_chip(n_edge, lambda peer: relay_start(group, peer))
            relay_start(group, me ^ 1)
        if group > 0:
            pass_on(group - 1)
        if group > 1:
            add_in(group - 2)
    if groups > 1:
        add_in(groups - 2)
    columns, table = take_in(groups - 1)
    proc_sum = jnp.zeros((shard, width), F32)
    for block in range(blocks):
        span = pl.ds(block * edges, edges)
        pre = edge_term[span, :] + nn(send_pick[span, columns], table)
        sigma = sigmoid(pre)
        slope[span, :] = sigma * (1.0 + pre * (1.0 - sigma))
        proc_sum = proc_sum + nn(recv_drop[:, span], (pre * sigma).astype(BF16))
    update_pre = nn(proc_sum.astype(BF16), edge_update[...]) + state_term[...]
    sigma = sigmoid(update_pre)
    slopes = sigma * (1.0 + update_pre * (1.0 - sigma))
    grad_all = (back_out[...] * slopes).astype(BF16)
    grad_pre[...] = grad_all
    update_act[...] = (update_pre * sigma).astype(BF16)
    band_grads = nt(grad_all, edge_update[...]).astype(BF16)
    back = jnp.zeros((far_rows + 2 * own_rows, width), F32)
    for block in range(blocks):
        span = pl.ds(block * edges, edges)
        grad_edge = (nn(recv_pick[span, :], band_grads) * slope[span, :]).astype(BF16)
        back = back + nn(back_drop[:, span], grad_edge)
    far_total = back[0:far_rows, :]

    def final_copy(place, land):
        return pltpu.make_async_remote_copy(
            src_ref=back_far.at[place],
            dst_ref=back_far_land.at[land],
            send_sem=final_send.at[place],
            recv_sem=final_recv.at[land],
            device_id={"mesh": (band + step_of(place) + n_mesh) & (n_mesh - 1)},
            device_id_type=MESH,
        )

    for place in range(1, n_mesh):
        back_far[place] = far_total[place * COARSE : (place + 1) * COARSE, :].astype(BF16)

    def final_start(k, carry):
        place = n_mesh - k
        final_copy(place, place_of(-step_of(place), n_mesh)).start()
        return carry

    lax.fori_loop(1, n_mesh, final_start, 0)
    mixed = latents[me].astype(F32) + nn(update_act[own_slice, :], update_outer[...])
    output[...] = mixed.astype(BF16)
    grad_node = cotangent[...].astype(F32) + nt(grad_pre[own_slice, :], update_state[...])
    to_receiver = back[far_rows + own_rows :, :].astype(BF16)
    result = grad_node + nt(to_receiver, edge_receiver[...])
    tail[...] = back[far_rows : far_rows + own_rows, :]

    def final_finish(k, carry):
        final_copy(k, k).wait_recv()
        return carry

    lax.fori_loop(1, n_mesh, final_finish, 0)
    arrived = back_far_land[1].astype(F32)
    for place in range(2, n_mesh):
        arrived = arrived + back_far_land[place].astype(F32)
    tail[0:COARSE, :] += arrived
    gradient[...] = result + nt(tail[...].astype(BF16), edge_sender[...])

    def far_sent(k, carry):
        far_copy(k, k).wait_send()
        final_copy(k, k).wait_send()
        return carry

    lax.fori_loop(1, n_mesh, far_sent, 0)
    for copy in unsent:
        copy.wait_send()


def finish_kernel(output, gradient, output_copy, gradient_copy):
    output_copy[...] = output[...]
    gradient_copy[...] = gradient[...]


def vmem():
    return pl.BlockSpec(memory_space=pltpu.VMEM)


def anywhere():
    return pl.BlockSpec(memory_space=pltpu.HBM)


def hbm(value):
    return pltpu.with_memory_space_constraint(value, pltpu.HBM)


def shards(
    n_mesh,
    n_edge,
    grid_input,
    mesh_position,
    encoder_senders,
    encoder_receivers,
    encoder_features,
    encoder_counts,
    mesh_senders,
    mesh_receivers,
    mesh_features,
    cotangent,
    grid_first,
    grid_second,
    encoder_inner,
    encoder_geometry,
    encoder_outer,
    node_first,
    node_position,
    node_second,
    edge_sender,
    edge_receiver,
    edge_geometry,
    edge_outer,
    update_message,
    update_state,
    update_outer,
):
    grid_rows, channels = grid_input.shape
    width = grid_second.shape[1]
    slots = encoder_senders.shape[0]
    blocks = slots // BLOCK
    own_rows = mesh_position.shape[1]
    shard = own_rows * n_edge
    edges = mesh_senders.shape[0]
    dma = pltpu.SemaphoreType.DMA
    packed, features, projected = pl.pallas_call(
        functools.partial(embed_kernel, n_edge),
        out_shape=(
            jax.ShapeDtypeStruct((n_edge, blocks, BLOCK), I32),
            jax.ShapeDtypeStruct((n_edge, 4, slots), BF16),
            jax.ShapeDtypeStruct((width, grid_rows), BF16),
        ),
        in_specs=[pl.BlockSpec(memory_space=pltpu.SMEM)] + [anywhere()] * 7,
        out_specs=(vmem(),) * 3,
        scratch_shapes=[
            pltpu.VMEM((blocks, BLOCK), I32),
            pltpu.VMEM((blocks, BLOCK), I32),
            pltpu.VMEM((channels, grid_rows), BF16),
            pltpu.VMEM((channels, width), BF16),
            pltpu.VMEM((width, width), BF16),
            pltpu.VMEM((width, width), BF16),
            dma((7,)),
            dma((2, n_edge)),
            dma((2, n_edge)),
        ],
        compiler_params=pltpu.CompilerParams(
            collective_id=0, has_side_effects=True, vmem_limit_bytes=12 << 20
        ),
    )(
        encoder_counts,
        hbm(encoder_senders.reshape(blocks, BLOCK)),
        hbm(encoder_receivers.reshape(blocks, BLOCK)),
        hbm(encoder_features),
        hbm(grid_input.T),
        hbm(grid_first),
        hbm(grid_second),
        hbm(encoder_inner),
    )
    all_blocks = n_edge * blocks
    partial = pl.pallas_call(
        functools.partial(encode_kernel, n_edge, shard),
        out_shape=jax.ShapeDtypeStruct((shard, width), BF16),
        in_specs=[vmem()] * 3 + [anywhere()],
        out_specs=vmem(),
        scratch_shapes=[
            pltpu.VMEM((all_blocks, BLOCK), I32),
            pltpu.VMEM((8, all_blocks), I32),
            pltpu.SMEM((8, all_blocks), I32),
            pltpu.VMEM((8, n_edge * slots + STEP), F32),
            pltpu.VMEM((8, width), F32),
            pltpu.VMEM((4, width), BF16),
            pltpu.VMEM((shard, width), F32),
            dma(()),
            dma(()),
        ],
        compiler_params=pltpu.CompilerParams(vmem_limit_bytes=16 << 20),
    )(packed.reshape(all_blocks, BLOCK), features, projected, hbm(encoder_geometry))
    far_rows = n_mesh * COARSE
    groups = far_rows // own_rows
    table_rows = shard + n_edge * far_rows
    weights = [
        encoder_outer,
        node_first,
        node_second,
        edge_sender,
        edge_receiver,
        edge_outer,
        update_message,
        update_state,
        update_outer,
    ]
    output, gradient = pl.pallas_call(
        functools.partial(process_kernel, n_mesh, n_edge),
        out_shape=(
            jax.ShapeDtypeStruct((own_rows, width), BF16),
            jax.ShapeDtypeStruct((own_rows, width), F32),
        ),
        in_specs=[vmem()] * 8 + [anywhere()] * 9,
        out_specs=(vmem(), vmem()),
        scratch_shapes=[pltpu.VMEM((width, width), BF16) for _ in weights]
        + [
            pltpu.VMEM((128, 128), F32),
            pltpu.VMEM((8, 2 * edges), F32),
            pltpu.VMEM((n_edge, own_rows, width), BF16),
            pltpu.VMEM((n_edge, own_rows, width), BF16),
            pltpu.VMEM((COARSE, width), BF16),
            pltpu.VMEM((n_mesh, COARSE, width), BF16),
            pltpu.VMEM((n_edge, groups, own_rows, width), BF16),
            pltpu.VMEM((n_edge, 1, edges), I32),
            pltpu.VMEM((n_edge, 1, edges), I32),
            pltpu.VMEM((n_edge, 4, edges), BF16),
            pltpu.VMEM((n_edge * edges, table_rows), BF16),
            pltpu.VMEM((n_edge * edges, shard), BF16),
            pltpu.VMEM((shard, n_edge * edges), BF16),
            pltpu.VMEM((far_rows + 2 * own_rows, n_edge * edges), BF16),
            pltpu.VMEM((n_edge * edges, width), F32),
            pltpu.VMEM((n_edge * edges, width), F32),
            pltpu.VMEM((n_edge, own_rows, width), BF16),
            pltpu.VMEM((shard, width), F32),
            pltpu.VMEM((shard, width), F32),
            pltpu.VMEM((shard, width), BF16),
            pltpu.VMEM((shard, width), BF16),
            pltpu.VMEM((n_mesh, COARSE, width), BF16),
            pltpu.VMEM((n_mesh, COARSE, width), BF16),
            pltpu.VMEM((own_rows, width), F32),
            pltpu.VMEM((width, width), BF16),
            pltpu.VMEM((width, width), BF16),
            dma((9,)),
            dma((6, n_edge)),
            dma((6, n_edge)),
            dma((n_mesh,)),
            dma((n_mesh,)),
            dma((groups, n_edge)),
            dma((groups, n_edge)),
            dma((groups, n_edge)),
            dma((n_mesh,)),
            dma((n_mesh,)),
            pltpu.SemaphoreType.REGULAR,
            pltpu.SemaphoreType.REGULAR,
        ],
        compiler_params=pltpu.CompilerParams(
            collective_id=1, has_side_effects=True, vmem_limit_bytes=36 << 20
        ),
    )(
        partial,
        mesh_position,
        mesh_senders.reshape(1, edges),
        mesh_receivers.reshape(1, edges),
        mesh_features,
        cotangent,
        node_position,
        edge_geometry,
        *[hbm(weight) for weight in weights],
    )
    return pl.pallas_call(
        finish_kernel,
        out_shape=(
            jax.ShapeDtypeStruct((own_rows, width), BF16),
            jax.ShapeDtypeStruct((own_rows, width), F32),
        ),
        in_specs=[vmem()] * 2,
        out_specs=(vmem(), vmem()),
        compiler_params=pltpu.CompilerParams(vmem_limit_bytes=1 << 20),
    )(output, gradient)


def solution(mesh):
    banded = ("mesh", "edge")
    every = ("groups", "mesh", "edge")
    in_specs = (
        P(every, None),
        P(None, banded),
        P(banded),
        P(banded),
        P(None, banded),
        P(banded),
        P(banded),
        P(banded),
        P(None, banded),
        P(every, None),
    ) + (P(),) * 15
    return jax.shard_map(
        functools.partial(shards, mesh.shape["mesh"], mesh.shape["edge"]),
        mesh=mesh,
        in_specs=in_specs,
        out_specs=(P(every, None), P(every, None)),
        check_vma=False,
    )
```

```python
import functools

import jax
import jax.numpy as jnp
from jax import lax
from jax.experimental import pallas as pl
from jax.experimental.pallas import tpu as pltpu
from jax.sharding import PartitionSpec as P

BLOCK = 128
CHUNK_ROWS = 8
WINDOW = 256
STEP = 512
COARSE = 4
MESH = pl.DeviceIdType.MESH
F32 = jnp.float32
BF16 = jnp.bfloat16
I32 = jnp.int32


def bits(size):
    return size.bit_length() - 1


def nn(left, right):
    return jnp.dot(left, right, preferred_element_type=F32)


def nt(left, right):
    return lax.dot_general(left, right, (((1,), (1,)), ((), ())), preferred_element_type=F32)


def tn(left, right):
    return lax.dot_general(left, right, (((0,), (0,)), ((), ())), preferred_element_type=F32)


def tt(left, right):
    return lax.dot_general(left, right, (((0,), (1,)), ((), ())), preferred_element_type=F32)


def sigmoid(values):
    return 0.5 + 0.5 * jnp.tanh(0.5 * values)


def layer_norm(values):
    centred = values - jnp.mean(values, axis=-1, keepdims=True)
    variance = jnp.mean(centred * centred, axis=-1, keepdims=True)
    return centred * lax.rsqrt(variance + 1e-05)


def iota(shape, dim):
    return lax.broadcasted_iota(I32, shape, dim)


def one_hot(hits):
    return jnp.where(hits, 1.0, 0.0).astype(BF16)


def greet(axis, count):
    me = lax.axis_index(axis)
    barrier = pltpu.get_barrier_semaphore()

    def signal(k, carry):
        pl.semaphore_signal(
            barrier, inc=1, device_id={axis: lax.rem(me + k, count)}, device_id_type=MESH
        )
        return carry

    lax.fori_loop(1, count, signal, 0)


def chip_steps(chips):
    return sorted(range(1, chips), key=lambda step: -min(step, chips - step))


def each_chip(n_edge, action):
    me = lax.axis_index("edge")
    chips = n_edge // 2
    for step in chip_steps(chips):
        action((me + 2 * step) & (n_edge - 1))


def each_peer(n_edge, action):
    me = lax.axis_index("edge")
    chips = n_edge // 2
    for step in chip_steps(chips):
        peer = (me + 2 * step) & (n_edge - 1)
        action(me, peer)
        action(me, peer ^ 1)
    action(me, me ^ 1)


def embed_kernel(
    n_edge,
    count,
    senders,
    receivers,
    features,
    mesh_senders,
    mesh_receivers,
    mesh_features,
    grid_input,
    first,
    second,
    inner,
    packed_all,
    features_all,
    projected,
    senders_v,
    receivers_v,
    near_senders_v,
    near_receivers_v,
    rows_v,
    first_v,
    second_v,
    inner_v,
    load_sem,
    send_sem,
    recv_sem,
):
    me = lax.axis_index("edge")
    band = lax.axis_index("mesh")
    slots = features.shape[1]
    mesh_slots = mesh_features.shape[1]
    loads = [
        pltpu.make_async_copy(src, dst, load_sem.at[k])
        for k, (src, dst) in enumerate(
            [
                (senders, senders_v),
                (receivers, receivers_v),
                (mesh_senders, near_senders_v),
                (mesh_receivers, near_receivers_v),
                (features, features_all.at[me, :, pl.ds(0, slots)]),
                (mesh_features, features_all.at[me, :, pl.ds(slots, mesh_slots)]),
                (grid_input, rows_v),
                (first, first_v),
                (second, second_v),
                (inner, inner_v),
            ]
        )
    ]
    for load in loads:
        load.start()
    greet("edge", n_edge)
    blocks = senders.shape[0]
    rows = grid_input.shape[1]
    shard = packed_shard(n_edge)
    for load in loads[0:4]:
        load.wait()
    low = senders_v[...] - band * (rows * n_edge)
    near = receivers_v[...] - band * shard
    live = iota((blocks, BLOCK), 0) < count[0]
    packed_all[me, 0:blocks, :] = jnp.where(live, low * shard + near, -1)
    code = near_senders_v[...] * shard + near_receivers_v[...] - band * shard
    code = jnp.concatenate([code, jnp.zeros((8 - code.shape[0], BLOCK), I32)], axis=0)
    packed_all[me, blocks : blocks + 8, :] = code
    for load in loads[4:6]:
        load.wait()
    pl.semaphore_wait(pltpu.get_barrier_semaphore(), n_edge - 1)

    tables = (packed_all, features_all)

    def copy(k, owner, peer):
        return pltpu.make_async_remote_copy(
            src_ref=tables[k].at[owner],
            dst_ref=tables[k].at[owner],
            send_sem=send_sem.at[k, peer],
            recv_sem=recv_sem.at[k, owner],
            device_id={"edge": peer},
            device_id_type=MESH,
        )

    each_peer(n_edge, lambda own, peer: [copy(k, own, peer).start() for k in range(len(tables))])
    loads[6].wait()
    loads[7].wait()
    hidden = tn(rows_v[...], first_v[...])
    hidden = (hidden * sigmoid(hidden)).astype(BF16)
    loads[8].wait()
    latent = layer_norm(nn(hidden, second_v[...])).astype(BF16)
    loads[9].wait()
    projected[...] = tt(inner_v[...], latent).astype(BF16)

    def arrive(own, peer):
        for k in range(len(tables)):
            copy(k, peer, peer).wait_recv()

    def sent(own, peer):
        for k in range(len(tables)):
            copy(k, own, peer).wait_send()

    each_peer(n_edge, arrive)
    each_peer(n_edge, sent)


def packed_shard(n_edge):
    return 16 * n_edge


def encode_kernel(
    n_edge,
    shard,
    packed,
    features,
    projected,
    geometry,
    partial,
    encoded,
    position,
    bounds_v,
    bounds,
    queue,
    geometry_v,
    geometry_w,
    total,
    sem,
    geometry_sem,
):
    me = lax.axis_index("edge")
    load = pltpu.make_async_copy(geometry, geometry_w, geometry_sem)
    load.start()
    per_device = packed.shape[1] - 8
    blocks = per_device * n_edge
    grid_rows = projected.shape[1]
    width = projected.shape[0]
    shift = bits(shard)
    row_bits = bits(grid_rows)
    index = jnp.concatenate([packed[k, 0:per_device, :] for k in range(n_edge)], axis=0)
    encoded[...] = index
    own = (index >> (shift + row_bits)) == me
    own_b = one_hot(own)
    upper = one_hot(iota((BLOCK, BLOCK), 0) < iota((BLOCK, BLOCK), 1))
    before = one_hot(iota((blocks, blocks), 0) < iota((blocks, blocks), 1))
    lower = one_hot(iota((blocks, blocks), 0) > iota((blocks, blocks), 1))
    ones = jnp.ones((BLOCK, BLOCK), BF16)
    rank = nn(own_b, upper)
    per_block = nn(own_b, ones)
    base = nn(lower, per_block.astype(BF16))
    aligned = base.astype(I32) & -BLOCK
    position[...] = jnp.where(own, (rank + base).astype(I32), -1)
    totals = nt(jnp.ones((8, BLOCK), BF16), own_b)
    starts = nn(totals.astype(BF16), before)
    stops = starts + totals
    bounds_v[...] = jnp.where(iota((8, blocks), 0) == 0, starts, stops).astype(I32)
    copy = pltpu.make_async_copy(bounds_v, bounds, sem)
    copy.start()
    queue[...] = jnp.zeros_like(queue)
    total[...] = jnp.zeros_like(total)
    geometry_v[...] = jnp.zeros_like(geometry_v)
    chunk = CHUNK_ROWS * BLOCK
    per_chunk = per_device // CHUNK_ROWS

    def chunk_of(c, device, lane, row):
        code = encoded[pl.ds(row, CHUNK_ROWS), :]
        where = position[pl.ds(row, CHUNK_ROWS), :]
        code_row = jnp.concatenate([code[k : k + 1, :] for k in range(CHUNK_ROWS)], axis=1)
        where_row = jnp.concatenate([where[k : k + 1, :] for k in range(CHUNK_ROWS)], axis=1)
        sender = (code_row >> shift) & (grid_rows - 1)
        parts = features[device, :, pl.ds(lane, chunk)].astype(F32)
        parts = jnp.concatenate([parts, jnp.zeros_like(parts)], axis=0)
        place = iota((8, chunk), 0)
        parts = jnp.where(place == 4, (sender >> 7).astype(F32), parts)
        parts = jnp.where(place == 5, (sender & 127).astype(F32), parts)
        parts = jnp.where(place == 6, ((code_row & (shard - 1)) + 1).astype(F32), parts)
        return parts.astype(BF16), where_row

    def sorted_window(parts, where_row):
        return nt(parts, one_hot(iota((WINDOW, chunk), 0) == where_row))

    def add(offset, window):
        queue[:, pl.ds(pl.multiple_of(offset, BLOCK), WINDOW)] += window

    windows = []
    for device in range(n_edge):
        c = device * per_chunk
        parts, where_row = chunk_of(c, device, 0, c * CHUNK_ROWS)
        from_row = aligned[c * CHUNK_ROWS : c * CHUNK_ROWS + 1, :]
        from_row = jnp.concatenate([from_row] * CHUNK_ROWS, axis=1)
        windows.append(sorted_window(parts, where_row - from_row))
    copy.wait()
    for device, window in enumerate(windows):
        add(bounds[0, device * per_chunk * CHUNK_ROWS] & -BLOCK, window)

    def sort_chunk(c, carry):
        first = bounds[0, c * CHUNK_ROWS]
        last = bounds[1, c * CHUNK_ROWS + CHUNK_ROWS - 1]
        part = c & (per_chunk - 1)
        skip = jnp.where(part == 0, WINDOW, 0)
        start = (first & -BLOCK) + skip

        @pl.when((last > first) & (last > start))
        def _():
            lane = pl.multiple_of(part * chunk, chunk)
            row = pl.multiple_of(c * CHUNK_ROWS, CHUNK_ROWS)
            parts, where_row = chunk_of(c, c >> bits(per_chunk), lane, row)

            def more(w, inner_carry):
                offset = start + w * WINDOW
                add(offset, sorted_window(parts, where_row - offset))
                return inner_carry

            lax.fori_loop(0, (last - start + WINDOW - 1) >> bits(WINDOW), more, 0)

        return carry

    lax.fori_loop(0, n_edge * per_chunk, sort_chunk, 0)
    load.wait()
    geometry_v[0:4, :] = geometry_w[...].astype(F32)
    found = bounds[1, blocks - 1]

    def encode(j, carry):
        offset = pl.multiple_of(j * STEP, STEP)
        parts = queue[:, pl.ds(offset, STEP)]
        sender = (parts[4:5, :] * 128.0 + parts[5:6, :]).astype(I32)
        target = parts[6:7, :].astype(I32)
        picks = one_hot(iota((grid_rows, STEP), 0) == sender)
        goes = one_hot(iota((shard, STEP), 0) + 1 == target)
        pre = nn(projected[...], picks)
        pre = pre + tn(geometry_v[...].astype(BF16), parts.astype(BF16))
        act = (pre * sigmoid(pre)).astype(BF16)
        total[...] += nt(goes, act)
        return carry

    lax.fori_loop(0, lax.div(found + STEP - 1, STEP), encode, 0)
    partial[...] = total[...].astype(BF16)


def step_of(place):
    return jnp.where((place & 1) == 1, (place + 1) >> 1, -(place >> 1))


def place_of(step, n_mesh):
    step = step & (n_mesh - 1)
    return jnp.where(
        step == 0, 0, jnp.where(step <= n_mesh // 2, 2 * step - 1, 2 * (n_mesh - step))
    )


def process_kernel(
    n_mesh,
    n_edge,
    mesh_slots,
    partial,
    mesh_position,
    packed,
    features,
    cotangent,
    node_position,
    geometry,
    w_encoder_outer,
    w_node_first,
    w_node_second,
    w_edge_sender,
    w_edge_receiver,
    w_edge_outer,
    w_update_message,
    w_update_state,
    w_update_outer,
    output,
    gradient,
    encoder_outer,
    node_first,
    node_second,
    edge_sender,
    edge_receiver,
    edge_outer,
    update_message,
    update_state,
    update_outer,
    padded,
    small,
    enc_land,
    latents,
    coarse_own,
    coarse_land,
    coarse,
    send_pick,
    recv_pick,
    recv_drop,
    back_drop,
    edge_term,
    slope,
    cotangents,
    state_term,
    back_out,
    update_act,
    grad_pre,
    back_far,
    back_far_land,
    tail,
    enc_node,
    edge_update,
    load_sem,
    send_sem,
    recv_sem,
    far_send,
    far_recv,
    relay_send,
    relay_recv,
    forward_send,
    final_send,
    final_recv,
    band_ready,
    far_ready,
):
    me = lax.axis_index("edge")
    band = lax.axis_index("mesh")
    own_rows = cotangent.shape[0]
    shard = own_rows * n_edge
    groups = n_mesh * COARSE // own_rows
    per_group = own_rows // COARSE
    mesh_blocks = mesh_slots // BLOCK
    half = mesh_slots
    slots = features.shape[2] - half
    first_row = packed.shape[1] - 8
    edges = 2 * half
    far_rows = n_mesh * COARSE
    loads = [
        pltpu.make_async_copy(src, dst, load_sem.at[k])
        for k, (src, dst) in enumerate(
            [
                (w_encoder_outer, encoder_outer),
                (w_node_first, node_first),
                (w_node_second, node_second),
                (w_edge_sender, edge_sender),
                (w_edge_receiver, edge_receiver),
                (w_edge_outer, edge_outer),
                (w_update_message, update_message),
                (w_update_state, update_state),
                (w_update_outer, update_outer),
            ]
        )
    ]
    for load in loads:
        load.start()
    core = me & 1
    chip = me >> 1
    chips = n_edge // 2
    barrier = pltpu.get_barrier_semaphore()

    def signal_band(k, carry):
        @pl.when((k > 0) | (core == 1))
        def _():
            pl.semaphore_signal(
                barrier,
                inc=1,
                device_id={"edge": 2 * ((chip + k) & (chips - 1))},
                device_id_type=MESH,
            )

        return carry

    def signal_far(k, carry):
        pl.semaphore_signal(
            barrier,
            inc=1,
            device_id={"mesh": (band + k) & (n_mesh - 1), "edge": me | 1},
            device_id_type=MESH,
        )
        return carry

    lax.fori_loop(0, chips, signal_band, 0)
    lax.fori_loop(1, n_mesh, signal_far, 0)

    @pl.when(core == 0)
    def _():
        pl.semaphore_wait(barrier, n_edge - 1)
        pl.semaphore_signal(band_ready, inc=1, device_id={"edge": me ^ 1}, device_id_type=MESH)

    @pl.when(core == 1)
    def _():
        pl.semaphore_wait(band_ready, 1)

    unsent = []

    def to_peer(phase, src, dst, sem, land):
        def copy(peer):
            return pltpu.make_async_remote_copy(
                src_ref=src(peer),
                dst_ref=dst,
                send_sem=send_sem.at[phase, sem(peer)],
                recv_sem=recv_sem.at[phase, land],
                device_id={"edge": peer},
                device_id_type=MESH,
            )

        return copy

    def start_all(phase, src, dst):
        def start(own, peer):
            copy = to_peer(phase, src, dst.at[own], lambda p: p, own)(peer)
            copy.start()
            unsent.append(copy)

        each_peer(n_edge, start)

    def wait_all(phase, src, dst):
        each_peer(
            n_edge,
            lambda own, peer: to_peer(phase, src, dst.at[peer], lambda p: p, peer)(peer).wait_recv(),
        )

    def rows_of(ref):
        return lambda peer: ref.at[pl.ds(pl.multiple_of(peer * own_rows, own_rows), own_rows), :]

    own_slice = pl.ds(pl.multiple_of(me * own_rows, own_rows), own_rows)
    start_all(0, rows_of(partial), enc_land)
    enc_land[me] = partial[own_slice, :]
    start_all(2, lambda peer: cotangent, cotangents)
    cotangents[me] = cotangent[...]

    padded[...] = jnp.zeros_like(padded)
    padded[0:3, 0:own_rows] = mesh_position[...].astype(F32)
    place_columns = padded[...].T
    position_term = jnp.zeros((own_rows, node_position.shape[1]), F32)
    for k in range(3):
        position_term += (
            place_columns[0:own_rows, k : k + 1] * node_position[k : k + 1, :].astype(F32)
        )

    width = geometry.shape[1]
    padded_geometry = jnp.concatenate([geometry[...].astype(F32)] * 2, axis=0)
    padded_geometry = jnp.where(iota((8, width), 0) < 4, padded_geometry, 0.0).astype(BF16)
    small[...] = jnp.zeros_like(small)
    blocks = n_edge // 2
    table_rows = shard + n_edge * far_rows

    def block_rows(block):
        return pl.ds(pl.multiple_of(block * edges, edges), edges)

    def prepare(block, carry):
        span = block_rows(block)
        first, second = 2 * block, 2 * block + 1
        codes = [packed[device, first_row : first_row + 8, :] for device in (first, second)]
        code = jnp.concatenate(
            [rows[k : k + 1, :] for rows in codes for k in range(mesh_blocks)], axis=1
        )
        sender = code >> bits(shard)
        receiver = code & (shard - 1)
        owner_band = sender >> bits(shard)
        near = owner_band == band
        owner_edge = (sender >> bits(own_rows)) & (n_edge - 1)
        far_place = place_of(owner_band - band, n_mesh)
        coarse_row = sender & (COARSE - 1)
        far_slot = ((far_place >> bits(per_group)) * n_edge + owner_edge) * own_rows
        far_slot = far_slot + (far_place & (per_group - 1)) * COARSE + coarse_row
        local = sender - band * shard
        pick = jnp.where(near, local, shard + far_slot)
        mine = owner_edge == me
        drop_far = jnp.where(mine & (owner_band != band), far_place * COARSE + coarse_row, -1)
        drop_near = jnp.where(mine & near, local & (own_rows - 1), -1)
        drop_recv = jnp.where(receiver >> bits(own_rows) == me, receiver & (own_rows - 1), -1)
        back_drop[0:far_rows, span] = one_hot(iota((far_rows, edges), 0) == drop_far)
        base = far_rows + own_rows
        back_drop[far_rows:base, span] = one_hot(iota((own_rows, edges), 0) == drop_near)
        back_drop[base:, span] = one_hot(iota((own_rows, edges), 0) == drop_recv)
        recv_drop[:, span] = one_hot(iota((shard, edges), 0) == receiver)
        pick_columns = jnp.broadcast_to(pick.astype(F32), (128, edges)).T.astype(I32)
        recv_columns = jnp.broadcast_to(receiver.astype(F32), (128, edges)).T.astype(I32)
        lanes = iota((edges, 128), 1)
        for k in range(table_rows // 128):
            send_pick[span, k * 128 : (k + 1) * 128] = one_hot(lanes + k * 128 == pick_columns)
        for k in range(shard // 128):
            recv_pick[span, k * 128 : (k + 1) * 128] = one_hot(lanes + k * 128 == recv_columns)
        small[0:4, 0:half] = features[first, :, slots:].astype(F32)
        small[0:4, half:edges] = features[second, :, slots:].astype(F32)
        edge_term[span, :] = tn(small[...].astype(BF16), padded_geometry)
        return carry

    lax.fori_loop(0, blocks, prepare, 0)
    for load in loads:
        load.wait()
    enc_node[...] = nn(encoder_outer[...], node_first[...]).astype(BF16)

    wait_all(0, rows_of(partial), enc_land)
    enc_sum = jnp.sum(enc_land[...].astype(F32), axis=0)
    hidden = nn(enc_sum.astype(BF16), enc_node[...]) + position_term
    hidden = (hidden * sigmoid(hidden)).astype(BF16)
    latent = layer_norm(nn(hidden, node_second[...])).astype(BF16)
    coarse_own[...] = latent[0:COARSE, :]
    latents[me] = latent

    latent_rows = lambda peer: latents.at[me]
    start_all(1, latent_rows, latents)

    def far_copy(place, land):
        return pltpu.make_async_remote_copy(
            src_ref=coarse_own,
            dst_ref=coarse_land.at[land],
            send_sem=far_send.at[place],
            recv_sem=far_recv.at[land],
            device_id={"mesh": (band + step_of(place) + n_mesh) & (n_mesh - 1)},
            device_id_type=MESH,
        )

    def far_start(k, carry):
        place = n_mesh - k
        far_copy(place, place_of(-step_of(place), n_mesh)).start()
        return carry

    @pl.when(core == 1)
    def _():
        pl.semaphore_wait(barrier, 2 * (n_mesh - 1))
        pl.semaphore_signal(far_ready, inc=1, device_id={"edge": me ^ 1}, device_id_type=MESH)

    @pl.when(core == 0)
    def _():
        pl.semaphore_wait(far_ready, 1)

    lax.fori_loop(1, n_mesh, far_start, 0)
    coarse_land[0] = coarse_own[...]

    def relay(group, owner, peer):
        return pltpu.make_async_remote_copy(
            src_ref=coarse.at[owner, group],
            dst_ref=coarse.at[owner, group],
            send_sem=relay_send.at[group, peer],
            recv_sem=relay_recv.at[group, owner],
            device_id={"edge": peer},
            device_id_type=MESH,
        )

    def forward(group, owner):
        return pltpu.make_async_remote_copy(
            src_ref=coarse.at[owner, group],
            dst_ref=coarse.at[owner, group],
            send_sem=forward_send.at[group, owner],
            recv_sem=relay_recv.at[group, owner],
            device_id={"edge": me ^ 1},
            device_id_type=MESH,
        )

    def pass_on(group):
        def step(owner):
            relay(group, owner, owner).wait_recv()
            copy = forward(group, owner)
            copy.start()
            unsent.append(copy)

        each_chip(n_edge, step)

    def relay_start(group, peer):
        copy = relay(group, me, peer)
        copy.start()
        unsent.append(copy)

    def take_in(group):
        if group == groups - 1:
            each_peer(n_edge, lambda own, peer: relay(group, peer, me).wait_recv())
        else:
            each_chip(n_edge, lambda peer: forward(group, peer ^ 1).wait_recv())
            relay(group, me ^ 1, me).wait_recv()
        table = coarse[:, group].reshape(n_edge * own_rows, width)
        table = nn(table, edge_sender[...]).astype(BF16)
        return pl.ds(shard + group * n_edge * own_rows, n_edge * own_rows), table

    def add_in(group):
        columns, table = take_in(group)

        def add(block, carry):
            span = block_rows(block)
            edge_term[span, :] += nn(send_pick[span, columns], table)
            return carry

        lax.fori_loop(0, blocks, add, 0)

    edge_update[...] = nn(edge_outer[...], update_message[...]).astype(BF16)
    wait_all(1, latent_rows, latents)
    band_latent = latents[...].reshape(shard, width)
    near_table = nn(band_latent, edge_sender[...]).astype(BF16)
    recv_table = nn(band_latent, edge_receiver[...]).astype(BF16)

    def add_near(block, carry):
        span = block_rows(block)
        edge_term[span, :] += nn(send_pick[span, 0:shard], near_table) + nn(
            recv_pick[span, :], recv_table
        )
        return carry

    lax.fori_loop(0, blocks, add_near, 0)
    state_term[...] = nn(band_latent, update_state[...])
    wait_all(2, lambda peer: cotangent, cotangents)
    back_out[...] = nt(cotangents[...].reshape(shard, width), update_outer[...])

    for group in range(groups):
        for k in range(per_group):
            place = group * per_group + k
            if place > 0:
                far_copy(place, place).wait_recv()
        rows = [coarse_land[group * per_group + k].astype(F32) for k in range(per_group)]
        coarse[me, group] = jnp.concatenate(rows, axis=0).astype(BF16)
        if group == groups - 1:
            each_peer(n_edge, lambda own, peer: relay_start(group, peer))
        else:
            each_chip(n_edge, lambda peer: relay_start(group, peer))
            relay_start(group, me ^ 1)
        if group > 0:
            pass_on(group - 1)
        if group > 1:
            add_in(group - 2)
    if groups > 1:
        add_in(groups - 2)
    columns, table = take_in(groups - 1)
    proc_sum = jnp.zeros((shard, width), F32)
    for block in range(blocks):
        span = pl.ds(block * edges, edges)
        pre = edge_term[span, :] + nn(send_pick[span, columns], table)
        sigma = sigmoid(pre)
        slope[span, :] = sigma * (1.0 + pre * (1.0 - sigma))
        proc_sum = proc_sum + nn(recv_drop[:, span], (pre * sigma).astype(BF16))
    update_pre = nn(proc_sum.astype(BF16), edge_update[...]) + state_term[...]
    sigma = sigmoid(update_pre)
    slopes = sigma * (1.0 + update_pre * (1.0 - sigma))
    grad_all = (back_out[...] * slopes).astype(BF16)
    grad_pre[...] = grad_all
    update_act[...] = (update_pre * sigma).astype(BF16)
    band_grads = nt(grad_all, edge_update[...]).astype(BF16)
    back = jnp.zeros((far_rows + 2 * own_rows, width), F32)
    for block in range(blocks):
        span = pl.ds(block * edges, edges)
        grad_edge = (nn(recv_pick[span, :], band_grads) * slope[span, :]).astype(BF16)
        back = back + nn(back_drop[:, span], grad_edge)
    far_total = back[0:far_rows, :]

    def final_copy(place, land):
        return pltpu.make_async_remote_copy(
            src_ref=back_far.at[place],
            dst_ref=back_far_land.at[land],
            send_sem=final_send.at[place],
            recv_sem=final_recv.at[land],
            device_id={"mesh": (band + step_of(place) + n_mesh) & (n_mesh - 1)},
            device_id_type=MESH,
        )

    for place in range(1, n_mesh):
        back_far[place] = far_total[place * COARSE : (place + 1) * COARSE, :].astype(BF16)

    def final_start(k, carry):
        place = n_mesh - k
        final_copy(place, place_of(-step_of(place), n_mesh)).start()
        return carry

    lax.fori_loop(1, n_mesh, final_start, 0)
    mixed = latents[me].astype(F32) + nn(update_act[own_slice, :], update_outer[...])
    output[...] = mixed.astype(BF16)
    grad_node = cotangent[...].astype(F32) + nt(grad_pre[own_slice, :], update_state[...])
    to_receiver = back[far_rows + own_rows :, :].astype(BF16)
    result = grad_node + nt(to_receiver, edge_receiver[...])
    tail[...] = back[far_rows : far_rows + own_rows, :]

    def final_finish(k, carry):
        final_copy(k, k).wait_recv()
        return carry

    lax.fori_loop(1, n_mesh, final_finish, 0)
    arrived = back_far_land[1].astype(F32)
    for place in range(2, n_mesh):
        arrived = arrived + back_far_land[place].astype(F32)
    tail[0:COARSE, :] += arrived
    gradient[...] = result + nt(tail[...].astype(BF16), edge_sender[...])

    def far_sent(k, carry):
        far_copy(k, k).wait_send()
        final_copy(k, k).wait_send()
        return carry

    lax.fori_loop(1, n_mesh, far_sent, 0)
    for copy in unsent:
        copy.wait_send()


def finish_kernel(output, gradient, output_copy, gradient_copy):
    output_copy[...] = output[...]
    gradient_copy[...] = gradient[...]


def vmem():
    return pl.BlockSpec(memory_space=pltpu.VMEM)


def anywhere():
    return pl.BlockSpec(memory_space=pltpu.HBM)


def hbm(value):
    return pltpu.with_memory_space_constraint(value, pltpu.HBM)


def shards(
    n_mesh,
    n_edge,
    grid_input,
    mesh_position,
    encoder_senders,
    encoder_receivers,
    encoder_features,
    encoder_counts,
    mesh_senders,
    mesh_receivers,
    mesh_features,
    cotangent,
    grid_first,
    grid_second,
    encoder_inner,
    encoder_geometry,
    encoder_outer,
    node_first,
    node_position,
    node_second,
    edge_sender,
    edge_receiver,
    edge_geometry,
    edge_outer,
    update_message,
    update_state,
    update_outer,
):
    grid_rows, channels = grid_input.shape
    width = grid_second.shape[1]
    slots = encoder_senders.shape[0]
    blocks = slots // BLOCK
    own_rows = mesh_position.shape[1]
    shard = own_rows * n_edge
    edges = mesh_senders.shape[0]
    dma = pltpu.SemaphoreType.DMA
    packed, features, projected = pl.pallas_call(
        functools.partial(embed_kernel, n_edge),
        out_shape=(
            jax.ShapeDtypeStruct((n_edge, blocks + 8, BLOCK), I32),
            jax.ShapeDtypeStruct((n_edge, 4, slots + edges), BF16),
            jax.ShapeDtypeStruct((width, grid_rows), BF16),
        ),
        in_specs=[pl.BlockSpec(memory_space=pltpu.SMEM)] + [anywhere()] * 10,
        out_specs=(vmem(),) * 3,
        scratch_shapes=[
            pltpu.VMEM((blocks, BLOCK), I32),
            pltpu.VMEM((blocks, BLOCK), I32),
            pltpu.VMEM((edges // BLOCK, BLOCK), I32),
            pltpu.VMEM((edges // BLOCK, BLOCK), I32),
            pltpu.VMEM((channels, grid_rows), BF16),
            pltpu.VMEM((channels, width), BF16),
            pltpu.VMEM((width, width), BF16),
            pltpu.VMEM((width, width), BF16),
            dma((10,)),
            dma((2, n_edge)),
            dma((2, n_edge)),
        ],
        compiler_params=pltpu.CompilerParams(
            collective_id=0, has_side_effects=True, vmem_limit_bytes=12 << 20
        ),
    )(
        encoder_counts,
        hbm(encoder_senders.reshape(blocks, BLOCK)),
        hbm(encoder_receivers.reshape(blocks, BLOCK)),
        hbm(encoder_features),
        hbm(mesh_senders.reshape(edges // BLOCK, BLOCK)),
        hbm(mesh_receivers.reshape(edges // BLOCK, BLOCK)),
        hbm(mesh_features),
        hbm(grid_input.T),
        hbm(grid_first),
        hbm(grid_second),
        hbm(encoder_inner),
    )
    all_blocks = n_edge * blocks
    partial = pl.pallas_call(
        functools.partial(encode_kernel, n_edge, shard),
        out_shape=jax.ShapeDtypeStruct((shard, width), BF16),
        in_specs=[vmem()] * 3 + [anywhere()],
        out_specs=vmem(),
        scratch_shapes=[
            pltpu.VMEM((all_blocks, BLOCK), I32),
            pltpu.VMEM((all_blocks, BLOCK), I32),
            pltpu.VMEM((8, all_blocks), I32),
            pltpu.SMEM((8, all_blocks), I32),
            pltpu.VMEM((8, n_edge * slots + STEP), F32),
            pltpu.VMEM((8, width), F32),
            pltpu.VMEM((4, width), BF16),
            pltpu.VMEM((shard, width), F32),
            dma(()),
            dma(()),
        ],
        compiler_params=pltpu.CompilerParams(vmem_limit_bytes=16 << 20),
    )(packed, features, projected, hbm(encoder_geometry))
    far_rows = n_mesh * COARSE
    groups = far_rows // own_rows
    table_rows = shard + n_edge * far_rows
    weights = [
        encoder_outer,
        node_first,
        node_second,
        edge_sender,
        edge_receiver,
        edge_outer,
        update_message,
        update_state,
        update_outer,
    ]
    output, gradient = pl.pallas_call(
        functools.partial(process_kernel, n_mesh, n_edge, edges),
        out_shape=(
            jax.ShapeDtypeStruct((own_rows, width), BF16),
            jax.ShapeDtypeStruct((own_rows, width), F32),
        ),
        in_specs=[vmem()] * 7 + [anywhere()] * 9,
        out_specs=(vmem(), vmem()),
        scratch_shapes=[pltpu.VMEM((width, width), BF16) for _ in weights]
        + [
            pltpu.VMEM((128, 128), F32),
            pltpu.VMEM((8, 2 * edges), F32),
            pltpu.VMEM((n_edge, own_rows, width), BF16),
            pltpu.VMEM((n_edge, own_rows, width), BF16),
            pltpu.VMEM((COARSE, width), BF16),
            pltpu.VMEM((n_mesh, COARSE, width), BF16),
            pltpu.VMEM((n_edge, groups, own_rows, width), BF16),
            pltpu.VMEM((n_edge * edges, table_rows), BF16),
            pltpu.VMEM((n_edge * edges, shard), BF16),
            pltpu.VMEM((shard, n_edge * edges), BF16),
            pltpu.VMEM((far_rows + 2 * own_rows, n_edge * edges), BF16),
            pltpu.VMEM((n_edge * edges, width), F32),
            pltpu.VMEM((n_edge * edges, width), F32),
            pltpu.VMEM((n_edge, own_rows, width), BF16),
            pltpu.VMEM((shard, width), F32),
            pltpu.VMEM((shard, width), F32),
            pltpu.VMEM((shard, width), BF16),
            pltpu.VMEM((shard, width), BF16),
            pltpu.VMEM((n_mesh, COARSE, width), BF16),
            pltpu.VMEM((n_mesh, COARSE, width), BF16),
            pltpu.VMEM((own_rows, width), F32),
            pltpu.VMEM((width, width), BF16),
            pltpu.VMEM((width, width), BF16),
            dma((9,)),
            dma((3, n_edge)),
            dma((3, n_edge)),
            dma((n_mesh,)),
            dma((n_mesh,)),
            dma((groups, n_edge)),
            dma((groups, n_edge)),
            dma((groups, n_edge)),
            dma((n_mesh,)),
            dma((n_mesh,)),
            pltpu.SemaphoreType.REGULAR,
            pltpu.SemaphoreType.REGULAR,
        ],
        compiler_params=pltpu.CompilerParams(
            collective_id=1, has_side_effects=True, vmem_limit_bytes=36 << 20
        ),
    )(
        partial,
        mesh_position,
        packed,
        features,
        cotangent,
        node_position,
        edge_geometry,
        *[hbm(weight) for weight in weights],
    )
    return pl.pallas_call(
        finish_kernel,
        out_shape=(
            jax.ShapeDtypeStruct((own_rows, width), BF16),
            jax.ShapeDtypeStruct((own_rows, width), F32),
        ),
        in_specs=[vmem()] * 2,
        out_specs=(vmem(), vmem()),
        compiler_params=pltpu.CompilerParams(vmem_limit_bytes=1 << 20),
    )(output, gradient)


def solution(mesh):
    banded = ("mesh", "edge")
    every = ("groups", "mesh", "edge")
    in_specs = (
        P(every, None),
        P(None, banded),
        P(banded),
        P(banded),
        P(None, banded),
        P(banded),
        P(banded),
        P(banded),
        P(None, banded),
        P(every, None),
    ) + (P(),) * 15
    return jax.shard_map(
        functools.partial(shards, mesh.shape["mesh"], mesh.shape["edge"]),
        mesh=mesh,
        in_specs=in_specs,
        out_specs=(P(every, None), P(every, None)),
        check_vma=False,
    )
```
